32 devices in a mesh: dp: 2 (over x), tp: 4 (over z), ep: 4 (over y, core).
Axes of the slice: x: 2, y: 2, z: 4, core: 2. Of those that a mesh axis runs over, the one named last changes fastest.
Arguments:
- hidden: bfloat16 [512, 1536], P(('dp', 'ep')), parts along dimension 0
- seq_lens: int32 [512], P(('dp', 'ep')), parts along dimension 0
- rope_cos: float32 [512, 32], P(('dp', 'ep')), parts along dimension 0
- rope_sin: float32 [512, 32], P(('dp', 'ep')), parts along dimension 0
- ln1_scale: bfloat16 [1536], replicated
- ln1_bias: bfloat16 [1536], replicated
- w_qkv: bfloat16 [1536, 2560], P(None, 'tp')
- b_qkv: bfloat16 [2560], P('tp')
- w_out: bfloat16 [1536, 1536], P('tp')
- b_out: bfloat16 [1536], replicated
- k_cache: bfloat16 [512, 512, 8, 64], P(('dp', 'ep'), None, 'tp'), parts along dimension 0
- v_cache: bfloat16 [512, 512, 8, 64], P(('dp', 'ep'), None, 'tp'), parts along dimension 0
- ln2_scale: bfloat16 [1536], replicated
- ln2_bias: bfloat16 [1536], replicated
- w_router: bfloat16 [1536, 40], replicated
- expert_ids: int32 [512, 8], P(('dp', 'ep')), parts along dimension 0
- w_gate: bfloat16 [40, 1536, 512], P('ep', None, 'tp')
- w_up: bfloat16 [40, 1536, 512], P('ep', None, 'tp')
- w_down: bfloat16 [40, 512, 1536], P('ep', 'tp')
Outputs:
- output 1: bfloat16 [512, 1536], P(('dp', 'ep')), parts along dimension 0
- output 2: bfloat16 [512, 512, 8, 64], P(('dp', 'ep'), None, 'tp'), parts along dimension 0
- output 3: bfloat16 [512, 512, 8, 64], P(('dp', 'ep'), None, 'tp'), parts along dimension 0
There are 2 independent parts. The reference program is written for one: setup_inputs(seed, part) draws one part's arguments, and reference() takes and returns one part's arrays. A program takes and returns all parts, laid end to end along the dimension named above; an argument that names none is the same for every part.
All inputs are finite; a program needn't handle non-finite values.
Results may differ from the reference program's by a relative error of at most 0.01133.
Values are sent between devices in bfloat16 or wider.
A program may use at most 1 GiB of HBM per device.

```python
import jax
import jax.numpy as jnp
from jax import lax

D = 1536
HEADS = 24
KV_HEADS = 8
HEAD = 64
EXPERTS = 40
TOP = 8
FF = 512
BATCH = 64
SMAX = 512
EP_SHARDS = 4

TOKENS = EP_SHARDS * BATCH
Q_PER_GROUP = HEADS // KV_HEADS
QKV_COLS = KV_HEADS * (Q_PER_GROUP + 2) * HEAD
CAP = (2 * TOP * BATCH + EXPERTS - 1) // EXPERTS
EPS = 1e-5
ROPE_BASE = 10000.0


def gaussian(one_key, out_shape):
    return jax.random.normal(one_key, out_shape, jnp.float32)


def draw_routing(route_key):
    hot_key, shard_key = jax.random.split(route_key)
    hot_order = jax.random.permutation(hot_key, EXPERTS)
    n_pairs = TOP * BATCH
    even_total = n_pairs - n_pairs // 2
    even_rows = even_total // EXPERTS + (jnp.arange(EXPERTS) < even_total % EXPERTS).astype(jnp.int32)

    def one_shard(one_key):
        even_key, order_key = jax.random.split(one_key)
        even_order = jax.random.permutation(even_key, EXPERTS)
        counts = jnp.zeros((EXPERTS,), jnp.int32).at[even_order].set(even_rows)
        free_room = CAP - counts[hot_order]
        before = jnp.cumsum(free_room) - free_room
        extra_rows = jnp.minimum(jnp.maximum(n_pairs // 2 - before, 0), free_room)
        counts = counts.at[hot_order].add(extra_rows)
        run_ends = jnp.cumsum(counts)
        slot_expert = jnp.sum((jnp.arange(n_pairs)[:, None] >= run_ends[None, :]).astype(jnp.int32), axis=1)
        choices = slot_expert.reshape(TOP, BATCH).T
        return choices[jax.random.permutation(order_key, BATCH)]

    picked = jax.vmap(one_shard)(jax.random.split(shard_key, EP_SHARDS))
    return picked.reshape(TOKENS, TOP).astype(jnp.int32)


def draw_lengths(len_key):
    draw_key, mark_key = jax.random.split(len_key)
    lengths = jax.random.randint(draw_key, (TOKENS,), SMAX // 16, SMAX)
    mark_order = jax.random.permutation(mark_key, TOKENS)
    lengths = lengths.at[mark_order[0]].set(SMAX - 1).at[mark_order[1]].set(SMAX // 16)
    return lengths.astype(jnp.int32)


def draw_rope(rope_key, lengths, factor_min, factor_max):
    rescale = jax.random.uniform(rope_key, (HEAD // 2,), jnp.float32, factor_min, factor_max)
    inv_freq = ROPE_BASE ** (-jnp.arange(HEAD // 2, dtype=jnp.float32) * 2.0 / HEAD)
    angles = lengths.astype(jnp.float32)[:, None] * inv_freq[None, :] / rescale[None, :]
    return jnp.cos(angles), jnp.sin(angles)


def setup_inputs(seed: int = 0, part: int = 0) -> dict:
    shared_key = jax.random.key(seed)
    part_key = jax.random.fold_in(jax.random.key(seed + 1), part)
    weight_keys = jax.random.split(shared_key, 12)
    part_keys = jax.random.split(part_key, 7)
    bf16 = jnp.bfloat16
    lengths = draw_lengths(part_keys[0])
    rope_cos, rope_sin = draw_rope(part_keys[1], lengths, 1.0, 8.0)
    hidden = gaussian(part_keys[2], (TOKENS, D))
    k_cache = 2.0 * gaussian(part_keys[3], (TOKENS, SMAX, KV_HEADS, HEAD))
    v_cache = 0.5 * gaussian(part_keys[4], (TOKENS, 1, KV_HEADS, HEAD)) + gaussian(part_keys[5], (TOKENS, SMAX, KV_HEADS, HEAD))
    expert_ids = draw_routing(part_keys[6])
    return {
        'hidden': hidden.astype(bf16),
        'seq_lens': lengths,
        'rope_cos': rope_cos,
        'rope_sin': rope_sin,
        'ln1_scale': (1.0 + 0.3 * gaussian(weight_keys[0], (D,))).astype(bf16),
        'ln1_bias': (0.3 * gaussian(weight_keys[1], (D,))).astype(bf16),
        'w_qkv': (gaussian(weight_keys[2], (D, QKV_COLS)) * D ** -0.5).astype(bf16),
        'b_qkv': (0.5 * gaussian(weight_keys[3], (QKV_COLS,))).astype(bf16),
        'w_out': (gaussian(weight_keys[4], (HEADS * HEAD, D)) * (HEADS * HEAD) ** -0.5).astype(bf16),
        'b_out': (0.3 * gaussian(weight_keys[5], (D,))).astype(bf16),
        'k_cache': k_cache.astype(bf16),
        'v_cache': v_cache.astype(bf16),
        'ln2_scale': (1.0 + 0.3 * gaussian(weight_keys[6], (D,))).astype(bf16),
        'ln2_bias': (0.3 * gaussian(weight_keys[7], (D,))).astype(bf16),
        'w_router': (gaussian(weight_keys[8], (D, EXPERTS)) * D ** -0.5).astype(bf16),
        'expert_ids': expert_ids,
        'w_gate': (gaussian(weight_keys[9], (EXPERTS, D, FF)) * D ** -0.5).astype(bf16),
        'w_up': (gaussian(weight_keys[10], (EXPERTS, D, FF)) * D ** -0.5).astype(bf16),
        'w_down': (gaussian(weight_keys[11], (EXPERTS, FF, D)) * FF ** -0.5).astype(bf16),
    }


def layer_norm(values, ln_scale, ln_bias):
    vals_f32 = values.astype(jnp.float32)
    row_mean = jnp.mean(vals_f32, axis=-1, keepdims=True)
    centered = vals_f32 - row_mean
    row_var = jnp.mean(centered * centered, axis=-1, keepdims=True)
    normed = centered * lax.rsqrt(row_var + EPS)
    return (normed * ln_scale.astype(jnp.float32) + ln_bias.astype(jnp.float32)).astype(jnp.bfloat16)


def apply_rope(values, cos_part, sin_part):
    half_dim = values.shape[-1] // 2
    vals_f32 = values.astype(jnp.float32)
    first_half = vals_f32[..., :half_dim]
    second_half = vals_f32[..., half_dim:]
    rotated = jnp.concatenate([first_half * cos_part - second_half * sin_part, second_half * cos_part + first_half * sin_part], axis=-1)
    return rotated.astype(jnp.bfloat16)


def reference(hidden, seq_lens, rope_cos, rope_sin, ln1_scale, ln1_bias, w_qkv, b_qkv, w_out, b_out, k_cache, v_cache, ln2_scale, ln2_bias, w_router, expert_ids, w_gate, w_up, w_down):
    normed = layer_norm(hidden, ln1_scale, ln1_bias)
    qkv_rows = (jnp.dot(normed, w_qkv, preferred_element_type=jnp.float32) + b_qkv.astype(jnp.float32)).astype(jnp.bfloat16)
    qkv_rows = qkv_rows.reshape(TOKENS, KV_HEADS, Q_PER_GROUP + 2, HEAD)
    queries = apply_rope(qkv_rows[:, :, :Q_PER_GROUP], rope_cos[:, None, None, :], rope_sin[:, None, None, :])
    key_new = apply_rope(qkv_rows[:, :, Q_PER_GROUP], rope_cos[:, None, :], rope_sin[:, None, :])
    value_new = qkv_rows[:, :, Q_PER_GROUP + 1]
    positions = jnp.arange(SMAX)
    write_mask = (positions[None, :] == seq_lens[:, None])[:, :, None, None]
    k_cache_out = jnp.where(write_mask, key_new[:, None], k_cache)
    v_cache_out = jnp.where(write_mask, value_new[:, None], v_cache)

    def attend(per_seq):
        q_one, k_one, v_one, len_one = per_seq
        scores = jnp.einsum('gqh,sgh->gqs', q_one.astype(jnp.float32), k_one.astype(jnp.float32)) * HEAD ** -0.5
        scores = jnp.where(positions[None, None, :] <= len_one, scores, -jnp.inf)
        attn_probs = jax.nn.softmax(scores, axis=-1).astype(jnp.bfloat16)
        return jnp.einsum('gqs,sgh->gqh', attn_probs.astype(jnp.float32), v_one.astype(jnp.float32)).astype(jnp.bfloat16)

    context = lax.map(attend, (queries, k_cache_out, v_cache_out, seq_lens))
    attn_full = jnp.dot(context.reshape(TOKENS, HEADS * HEAD), w_out, preferred_element_type=jnp.float32)
    hidden_mid = (hidden.astype(jnp.float32) + attn_full + b_out.astype(jnp.float32)).astype(jnp.bfloat16)
    normed2 = layer_norm(hidden_mid, ln2_scale, ln2_bias)
    logits = jnp.dot(normed2, w_router, preferred_element_type=jnp.float32)
    chosen = jnp.take_along_axis(logits, expert_ids, axis=1)
    gate_probs = jax.nn.softmax(chosen, axis=-1).astype(jnp.bfloat16).astype(jnp.float32)
    mix_weights = jnp.sum(jax.nn.one_hot(expert_ids, EXPERTS, dtype=jnp.float32) * gate_probs[:, :, None], axis=1)

    def expert_step(moe_acc, per_expert):
        gate_w, up_w, down_w, weight = per_expert
        gate_pre = jnp.dot(normed2, gate_w, preferred_element_type=jnp.float32)
        up_pre = jnp.dot(normed2, up_w, preferred_element_type=jnp.float32)
        hidden_act = (jax.nn.silu(gate_pre) * up_pre).astype(jnp.bfloat16)
        expert_out = jnp.dot(hidden_act, down_w, preferred_element_type=jnp.float32).astype(jnp.bfloat16)
        return moe_acc + weight[:, None] * expert_out.astype(jnp.float32), None

    moe_sum, _ = lax.scan(expert_step, jnp.zeros((TOKENS, D), jnp.float32), (w_gate, w_up, w_down, mix_weights.T))
    hidden_out = (hidden_mid.astype(jnp.float32) + moe_sum).astype(jnp.bfloat16)
    return (hidden_out, k_cache_out, v_cache_out)
```

```python
import functools

import jax
import jax.numpy as jnp
from jax import lax
from jax.experimental import pallas as pl
from jax.experimental.pallas import tpu as pltpu
from jax.sharding import PartitionSpec as P

EPS = 1e-5
F32 = jnp.float32
BF16 = jnp.bfloat16
MESH = pl.DeviceIdType.MESH
VMEM_LIMIT = 60 * 1024 * 1024
NT = (((1,), (1,)), ((), ()))
BB = 8
COLS = 3


def normalize(vals_f32, ln_scale, ln_bias):
    row_mean = jnp.mean(vals_f32, axis=-1, keepdims=True)
    centered = vals_f32 - row_mean
    row_var = jnp.mean(centered * centered, axis=-1, keepdims=True)
    normed = centered * lax.rsqrt(row_var + EPS)
    return (normed * ln_scale + ln_bias).astype(BF16)


def row_of(vec_ref):
    return vec_ref[...].astype(F32)[None, :]


def attention_kernel(lens_ref, hid_ref, cos_ref, sin_ref, scale_ref, bias_ref, bqkv_ref, wqkv_hbm, k_hbm, v_hbm,
                     ctx_ref, ko_hbm, vo_hbm, k_buf, v_buf, w_buf, q_buf, kn_buf, vn_buf, c_buf, w_sem, k_sem, v_sem, ko_sem, vo_sem):
    n_rows = hid_ref.shape[0]
    n_blocks = n_rows // BB
    s_max = k_buf.shape[2]
    w_copy = pltpu.make_async_copy(wqkv_hbm, w_buf, w_sem)
    w_copy.start()

    def fetch(i):
        rows = pl.ds(i * BB, BB)
        return (pltpu.make_async_copy(k_hbm.at[rows], k_buf.at[rows], k_sem.at[i]),
                pltpu.make_async_copy(v_hbm.at[rows], v_buf.at[rows], v_sem.at[i]))

    def flush(i):
        rows = pl.ds(i * BB, BB)
        return (pltpu.make_async_copy(k_buf.at[rows], ko_hbm.at[rows], ko_sem.at[i]),
                pltpu.make_async_copy(v_buf.at[rows], vo_hbm.at[rows], vo_sem.at[i]))

    for i in range(n_blocks):
        for copy in fetch(i):
            copy.start()

    normed = normalize(hid_ref[...].astype(F32), row_of(scale_ref), row_of(bias_ref))
    w_copy.wait()
    qkv = jnp.dot(normed, w_buf[...], preferred_element_type=F32) + row_of(bqkv_ref)
    qkv = qkv.astype(BF16).astype(F32)
    qkv = jnp.concatenate([qkv, jnp.zeros((128 - n_rows, qkv.shape[1]), F32)], axis=0)
    feats = qkv.T
    cos_t = jnp.concatenate([cos_ref[...], jnp.zeros((32, 128 - n_rows), F32)], axis=1)
    sin_t = jnp.concatenate([sin_ref[...], jnp.zeros((32, 128 - n_rows), F32)], axis=1)

    def rotate(base):
        u, w = feats[base:base + 32], feats[base + 32:base + 64]
        return jnp.concatenate([u * cos_t - w * sin_t, w * cos_t + u * sin_t], axis=0).astype(BF16).astype(F32)

    zeros = jnp.zeros((64, 128), F32)
    for g in range(2):
        for j in range(3):
            q_rot = rotate(g * 320 + j * 64)
            both = jnp.concatenate([q_rot, zeros] if g == 0 else [zeros, q_rot], axis=0)
            q_buf[pl.ds(g * 3 + j, n_rows, stride=8), :] = both.T[:n_rows]
    for r in (6, 7):
        q_buf[pl.ds(r, n_rows, stride=8), :] = jnp.zeros((n_rows, 128), F32)
    k_new = jnp.concatenate([rotate(192), rotate(320 + 192)], axis=0)
    v_new = jnp.concatenate([feats[256:320], feats[320 + 256:320 + 320]], axis=0)
    for i in range(n_blocks):
        kn_buf[i] = k_new if i == 0 else pltpu.roll(k_new, 128 - i * BB, 1)
        vn_buf[i] = v_new if i == 0 else pltpu.roll(v_new, 128 - i * BB, 1)

    def block(i, carry):
        for copy in fetch(i):
            copy.wait()
        k_cols, v_cols = kn_buf[i], vn_buf[i]
        lane = lax.broadcasted_iota(jnp.int32, (128, 128), 1)
        position = lax.broadcasted_iota(jnp.int32, (8, s_max), 1)
        scores = []
        for j in range(BB):
            b = i * BB + j
            pos = lens_ref[b]
            first = pl.multiple_of((pos // 128) * 128, 128)
            hit = lane == pos - first
            window = pl.ds(first, 128)
            k_buf[b, :, window] = jnp.where(hit, k_cols[:, j:j + 1], k_buf[b, :, window].astype(F32)).astype(BF16)
            v_buf[b, :, window] = jnp.where(hit, v_cols[:, j:j + 1], v_buf[b, :, window].astype(F32)).astype(BF16)
            rows = pl.ds(pl.multiple_of(b * 8, 8), 8)
            one = jnp.dot(q_buf[rows, :].astype(BF16), k_buf[b], preferred_element_type=F32) * 0.125
            scores.append(jnp.where(position <= pos, one, -jnp.inf))
        scores = jnp.concatenate(scores, axis=0)
        top = jnp.max(scores, axis=1, keepdims=True)
        weights = jnp.exp(scores - top)
        probs = weights * (1.0 / jnp.sum(weights, axis=1, keepdims=True))
        for j in range(BB):
            b = i * BB + j
            rows = pl.ds(pl.multiple_of(b * 8, 8), 8)
            c_buf[rows, :] = lax.dot_general(probs[j * 8:j * 8 + 8].astype(BF16), v_buf[b], NT, preferred_element_type=F32)
        for copy in flush(i):
            copy.start()
        return carry

    lax.fori_loop(0, n_blocks, block, 0)
    heads = [c_buf[pl.ds(r, n_rows, stride=8), :] for r in range(6)]
    low = lax.broadcasted_iota(jnp.int32, (n_rows, 128), 1) < 64
    ctx_ref[:, 0:128] = jnp.where(low, heads[0], pltpu.roll(heads[1], 64, 1)).astype(BF16)
    ctx_ref[:, 128:256] = jnp.where(low, heads[2], heads[3]).astype(BF16)
    ctx_ref[:, 256:384] = jnp.where(low, pltpu.roll(heads[4], 64, 1), heads[5]).astype(BF16)
    for i in range(n_blocks):
        for copy in flush(i):
            copy.wait()


def moe_kernel(hid_ref, ctx_ref, bout_ref, scale_ref, bias_ref, wr_ref, ids_ref, wout_hbm, wg_hbm, wu_hbm, wd_hbm, out_ref,
               wout, wgu, wd, wr, part_f, part_b, rs_recv, x1_buf, h2, ids_buf, act, lo, hi, d_recv, y_send, y_recv, t_f, t_b, z_recv, o_buf,
               wsem, ssem, rsem):
    z, ep = lax.axis_index("tp"), lax.axis_index("ep")
    n_rows, d_model = hid_ref.shape
    n_exp = wgu.shape[0]
    width = d_model // COLS
    z_peers = [lax.rem(z + dz, 4) for dz in (1, 2, 3)]
    y_peer = lax.rem(ep + 2, 4)
    partner = ep + 1 - 2 * lax.rem(ep, 2)
    diagonal = 3 - ep
    barrier = pltpu.get_barrier_semaphore()
    for peer in z_peers:
        pl.semaphore_signal(barrier, inc=1, device_id={"tp": peer}, device_id_type=MESH)
    for peer in (y_peer, partner, diagonal):
        pl.semaphore_signal(barrier, inc=1, device_id={"ep": peer}, device_id_type=MESH)

    loads = [pltpu.make_async_copy(wout_hbm, wout, wsem.at[0])]
    for e in range(n_exp):
        loads.append(pltpu.make_async_copy(wg_hbm.at[e], wgu.at[e, :, 0:128], wsem.at[1 + 2 * e]))
        loads.append(pltpu.make_async_copy(wu_hbm.at[e], wgu.at[e, :, 128:256], wsem.at[2 + 2 * e]))
    loads.append(pltpu.make_async_copy(wd_hbm, wd, wsem.at[1 + 2 * n_exp]))
    for load in loads:
        load.start()

    sent = []

    def send(src, dst, slot, device):
        copy = pltpu.make_async_remote_copy(src_ref=src, dst_ref=dst, send_sem=ssem.at[slot], recv_sem=rsem.at[slot],
                                            device_id=device, device_id_type=MESH)
        copy.start()
        sent.append(copy)
        return copy

    loads[0].wait()
    part = jnp.dot(ctx_ref[...], wout[...], preferred_element_type=F32)
    part_f[...] = part
    part_b[...] = part.astype(BF16)
    wr[...] = jnp.concatenate([wr_ref[...], jnp.zeros((128 - wr_ref.shape[0], d_model), BF16)], axis=0)
    ids_buf[0] = ids_ref[...]
    pl.semaphore_wait(barrier, 6)

    def rows_of(index):
        return pl.ds(pl.multiple_of(index * 16, 16), 16)

    mine = rows_of(z)
    slot = 0
    rs = []
    for dz in range(3):
        rs.append(send(part_b.at[rows_of(z_peers[dz])], rs_recv.at[dz], slot, {"tp": z_peers[dz]}))
        slot += 1
    id_copies = []
    for shard, peer in ((1, y_peer), (2, partner), (3, diagonal)):
        id_copies.append(send(ids_ref, ids_buf.at[shard], slot, {"ep": peer}))
        slot += 1
    for copy in rs:
        copy.wait_recv()
    total = part_f[mine, :] + rs_recv[0].astype(F32) + rs_recv[1].astype(F32) + rs_recv[2].astype(F32)
    x1 = (hid_ref[mine, :].astype(F32) + total + row_of(bout_ref)).astype(BF16).astype(F32)
    x1_buf[...] = x1
    h2[mine, :] = normalize(x1, row_of(scale_ref), row_of(bias_ref))

    def piece(shard, index):
        return h2.at[pl.ds(pl.multiple_of(shard * n_rows + index * 16, 16), 16)]

    from_z, from_y, from_p = [], [], []
    for dz in range(3):
        from_z.append(send(piece(0, z), piece(0, z), slot, {"tp": z_peers[dz]}))
        slot += 1

    def pass_on(index):
        nonlocal slot
        from_y.append(send(piece(0, index), piece(1, index), slot, {"ep": y_peer}))
        slot += 1
        from_p.append(send(piece(0, index), piece(2, index), slot, {"ep": partner}))
        slot += 1

    z_order = [z] + [lax.rem(z + 4 - dz, 4) for dz in (1, 2, 3)]
    pass_on(z)
    for dz in range(3):
        from_z[dz].wait_recv()
        pass_on(z_order[dz + 1])

    def masks(shard):
        picks = ids_buf[shard]
        expert = lax.broadcasted_iota(jnp.int32, (128, n_rows), 0)
        hit = jnp.zeros((128, n_rows), F32)
        for k in range(picks.shape[0]):
            hit = jnp.where(expert == picks[k:k + 1, :], 1.0, hit)
        return hit.T

    def up(shard):
        rows = h2[shard * n_rows:(shard + 1) * n_rows, :]
        logits = lax.dot_general(rows, wr[...], NT, preferred_element_type=F32)
        picked = masks(shard) > 0.5
        logits = jnp.where(picked, logits, -jnp.inf)
        shifted = jnp.exp(logits - jnp.max(logits, axis=1, keepdims=True))
        gates = (shifted / jnp.sum(shifted, axis=1, keepdims=True)).astype(BF16).astype(F32)
        gates = pltpu.roll(gates, lax.rem(128 - ep * n_exp, 128), 1)
        for e in range(n_exp):
            if shard == 0:
                loads[1 + 2 * e].wait()
                loads[2 + 2 * e].wait()
            pre = jnp.dot(rows, wgu[e], preferred_element_type=F32)
            gate_pre, up_pre = pre[:, :128], pre[:, 128:]
            hidden = (gate_pre * jax.nn.sigmoid(gate_pre) * up_pre).astype(BF16).astype(F32)
            act[shard * n_rows:(shard + 1) * n_rows, e * 128:(e + 1) * 128] = (hidden * gates[:, e:e + 1]).astype(BF16)

    up(0)
    from_pp = []
    for k in range(4):
        from_y[k].wait_recv()
        index = z_order[k]
        from_pp.append(send(piece(1, index), piece(3, index), slot, {"ep": partner}))
        slot += 1
    for k in range(4):
        from_p[k].wait_recv()
    for copy in id_copies:
        copy.wait_recv()
    up(2)
    up(1)
    for k in range(4):
        from_pp[k].wait_recv()
    up(3)
    loads[-1].wait()

    def cols(n):
        return pl.ds(n * width, width)

    from_d, from_yy, from_zz, from_o = [], [], [], []

    def reduce_pair(n):
        nonlocal slot
        from_d[n].wait_recv()
        y_send[:, cols(n)] = (lo[64:128, cols(n)] + d_recv[64:128, cols(n)].astype(F32)).astype(BF16)
        from_yy.append(send(y_send.at[:, cols(n)], y_recv.at[:, cols(n)], slot, {"ep": y_peer}))
        slot += 1

    for n in range(COLS):
        hi[:, cols(n)] = jnp.dot(act[128:256, :], wd[:, cols(n)], preferred_element_type=F32).astype(BF16)
        from_d.append(send(hi.at[:, cols(n)], d_recv.at[:, cols(n)], slot, {"ep": partner}))
        slot += 1
        if n > 0:
            reduce_pair(n - 1)
        lo[:, cols(n)] = jnp.dot(act[0:128, :], wd[:, cols(n)], preferred_element_type=F32)
    reduce_pair(COLS - 1)
    for n in range(COLS):
        from_yy[n].wait_recv()
        t = lo[0:64, cols(n)] + d_recv[0:64, cols(n)].astype(F32) + y_recv[:, cols(n)].astype(F32)
        t_f[:, cols(n)] = t
        t_b[:, cols(n)] = t.astype(BF16)
        group = []
        for dz in range(3):
            group.append(send(t_b.at[rows_of(z_peers[dz]), cols(n)], z_recv.at[dz, :, cols(n)], slot, {"tp": z_peers[dz]}))
            slot += 1
        from_zz.append(group)
    for n in range(COLS):
        for copy in from_zz[n]:
            copy.wait_recv()
        moe = t_f[mine, cols(n)] + z_recv[0, :, cols(n)].astype(F32) + z_recv[1, :, cols(n)].astype(F32) + z_recv[2, :, cols(n)].astype(F32)
        o_buf[mine, cols(n)] = (x1_buf[:, cols(n)] + moe).astype(BF16)
        for dz in range(3):
            from_o.append(send(o_buf.at[mine, cols(n)], o_buf.at[mine, cols(n)], slot, {"tp": z_peers[dz]}))
            slot += 1
    for copy in from_o:
        copy.wait_recv()
    out_ref[...] = o_buf[...]
    for copy in sent:
        copy.wait_send()


N_SLOTS = 3 + 3 + 3 + 8 + 4 + COLS * 2 + COLS * 6


def solution(mesh):
    token_rows = P(('dp', 'ep'), None)
    token_vec = P(('dp', 'ep'))
    cache_spec = P(('dp', 'ep'), None, 'tp', None)
    expert_in = P('ep', None, 'tp')
    expert_down = P('ep', 'tp', None)
    vm = pl.BlockSpec(memory_space=pltpu.VMEM)
    sm = pl.BlockSpec(memory_space=pltpu.SMEM)
    anyspace = pl.BlockSpec(memory_space=pl.ANY)

    def device_step(hidden, seq_lens, rope_cos, rope_sin, ln1_scale, ln1_bias, w_qkv, b_qkv, w_out, b_out, k_cache, v_cache, ln2_scale, ln2_bias, w_router, expert_ids, w_gate, w_up, w_down):
        n, d = hidden.shape
        _, s_max, groups, head = k_cache.shape
        feat = groups * head
        n_exp = w_gate.shape[0]
        k_in = k_cache.transpose(0, 2, 3, 1).reshape(n, feat, s_max)
        v_in = v_cache.transpose(0, 2, 3, 1).reshape(n, feat, s_max)
        ctx, k_out, v_out = pl.pallas_call(
            attention_kernel,
            out_shape=(jax.ShapeDtypeStruct((n, 384), BF16), jax.ShapeDtypeStruct(k_in.shape, BF16), jax.ShapeDtypeStruct(v_in.shape, BF16)),
            in_specs=[sm, vm, vm, vm, vm, vm, vm, anyspace, anyspace, anyspace],
            out_specs=(vm, anyspace, anyspace),
            scratch_shapes=[
                pltpu.VMEM(k_in.shape, BF16), pltpu.VMEM(v_in.shape, BF16), pltpu.VMEM(w_qkv.shape, BF16),
                pltpu.VMEM((n * 8, 128), F32), pltpu.VMEM((n // BB, 128, 128), F32), pltpu.VMEM((n // BB, 128, 128), F32), pltpu.VMEM((n * 8, 128), F32),
                pltpu.SemaphoreType.DMA, pltpu.SemaphoreType.DMA((n // BB,)), pltpu.SemaphoreType.DMA((n // BB,)),
                pltpu.SemaphoreType.DMA((n // BB,)), pltpu.SemaphoreType.DMA((n // BB,)),
            ],
            compiler_params=pltpu.CompilerParams(vmem_limit_bytes=VMEM_LIMIT),
            name="attention",
        )(seq_lens, hidden, rope_cos.T, rope_sin.T, ln1_scale, ln1_bias, b_qkv, w_qkv, k_in, v_in)
        rows = lambda r, t: pltpu.VMEM((r, d), t)
        hidden_out = pl.pallas_call(
            moe_kernel,
            out_shape=jax.ShapeDtypeStruct((n, d), BF16),
            in_specs=[vm] * 7 + [anyspace] * 4,
            out_specs=vm,
            scratch_shapes=[
                pltpu.VMEM(w_out.shape, BF16), pltpu.VMEM((n_exp, d, 256), BF16), pltpu.VMEM((n_exp * 128, d), BF16), rows(128, BF16),
                rows(64, F32), rows(64, BF16), pltpu.VMEM((3, 16, d), BF16), rows(16, F32), rows(256, BF16), pltpu.VMEM((4, 8, n), jnp.int32),
                pltpu.VMEM((256, n_exp * 128), BF16), rows(128, F32), rows(128, BF16), rows(128, BF16), rows(64, BF16), rows(64, BF16),
                rows(64, F32), rows(64, BF16), pltpu.VMEM((3, 16, d), BF16), rows(64, BF16),
                pltpu.SemaphoreType.DMA((2 * n_exp + 2,)), pltpu.SemaphoreType.DMA((N_SLOTS,)), pltpu.SemaphoreType.DMA((N_SLOTS,)),
            ],
            compiler_params=pltpu.CompilerParams(vmem_limit_bytes=VMEM_LIMIT, collective_id=0, has_side_effects=True),
            name="moe",
        )(hidden, ctx, b_out, ln2_scale, ln2_bias, w_router.T, expert_ids.T, w_out, w_gate, w_up, w_down.reshape(n_exp * 128, d))
        unfold = lambda c: c.reshape(n, groups, head, s_max).transpose(0, 3, 1, 2)
        return hidden_out, unfold(k_out), unfold(v_out)

    in_specs = (token_rows, token_vec, token_rows, token_rows, P(), P(), P(None, 'tp'), P('tp'), P('tp', None), P(), cache_spec, cache_spec, P(), P(), P(), token_rows, expert_in, expert_in, expert_down)
    return jax.shard_map(device_step, mesh=mesh, in_specs=in_specs, out_specs=(token_rows, cache_spec, cache_spec), check_vma=False)
```

```python
import functools

import jax
import jax.numpy as jnp
from jax import lax
from jax.experimental import pallas as pl
from jax.experimental.pallas import tpu as pltpu
from jax.sharding import PartitionSpec as P

EPS = 1e-5
F32 = jnp.float32
BF16 = jnp.bfloat16
MESH = pl.DeviceIdType.MESH
VMEM_LIMIT = 66_600_000
MOE_LIMIT = 66_200_000
NT = (((1,), (1,)), ((), ()))
BB = 8
COLS = 3


def normalize(vals_f32, ln_scale, ln_bias):
    row_mean = jnp.mean(vals_f32, axis=-1, keepdims=True)
    centered = vals_f32 - row_mean
    row_var = jnp.mean(centered * centered, axis=-1, keepdims=True)
    normed = centered * lax.rsqrt(row_var + EPS)
    return (normed * ln_scale + ln_bias).astype(BF16)


def row_of(vec_ref):
    return vec_ref[...].astype(F32)[None, :]


def attention_kernel(lens_hbm, hid_hbm, cos_hbm, sin_hbm, scale_hbm, bias_hbm, bqkv_hbm, wqkv_hbm, k_hbm, v_hbm,
                     ctx_ref, ko_hbm, vo_hbm, lens_ref, hid_ref, cos_ref, sin_ref, scale_ref, bias_ref, bqkv_ref,
                     k_buf, v_buf, w_buf, q_buf, kn_buf, vn_buf, c_buf, in_sem, w_sem, k_sem, v_sem, ko_sem, vo_sem):
    n_rows = hid_ref.shape[0]
    n_blocks = n_rows // BB
    s_max = k_buf.shape[2]
    smalls = ((hid_hbm, hid_ref), (scale_hbm, scale_ref), (bias_hbm, bias_ref), (bqkv_hbm, bqkv_ref), (cos_hbm, cos_ref), (sin_hbm, sin_ref),
              (lens_hbm, lens_ref))
    small_copies = [pltpu.make_async_copy(src, dst, in_sem.at[i]) for i, (src, dst) in enumerate(smalls)]
    w_copy = pltpu.make_async_copy(wqkv_hbm, w_buf, w_sem)
    for copy in small_copies[:3] + [w_copy] + small_copies[3:]:
        copy.start()

    def fetch(i):
        rows = pl.ds(i * BB, BB)
        return (pltpu.make_async_copy(k_hbm.at[rows], k_buf.at[rows], k_sem.at[i]),
                pltpu.make_async_copy(v_hbm.at[rows], v_buf.at[rows], v_sem.at[i]))

    def flush(i):
        rows = pl.ds(i * BB, BB)
        return (pltpu.make_async_copy(k_buf.at[rows], ko_hbm.at[rows], ko_sem.at[i]),
                pltpu.make_async_copy(v_buf.at[rows], vo_hbm.at[rows], vo_sem.at[i]))

    for i in range(n_blocks):
        for copy in fetch(i):
            copy.start()

    for copy in small_copies:
        copy.wait()
    normed = normalize(hid_ref[...].astype(F32), row_of(scale_ref), row_of(bias_ref))
    w_copy.wait()
    qkv = jnp.dot(normed, w_buf[...], preferred_element_type=F32) + row_of(bqkv_ref)
    qkv = qkv.astype(BF16).astype(F32)
    qkv = jnp.concatenate([qkv, jnp.zeros((128 - n_rows, qkv.shape[1]), F32)], axis=0)
    feats = qkv.T
    cos_t = jnp.concatenate([cos_ref[...], jnp.zeros((32, 128 - n_rows), F32)], axis=1)
    sin_t = jnp.concatenate([sin_ref[...], jnp.zeros((32, 128 - n_rows), F32)], axis=1)

    def rotate(base):
        u, w = feats[base:base + 32], feats[base + 32:base + 64]
        return jnp.concatenate([u * cos_t - w * sin_t, w * cos_t + u * sin_t], axis=0).astype(BF16).astype(F32)

    zeros = jnp.zeros((64, 128), F32)
    for g in range(2):
        for j in range(3):
            q_rot = rotate(g * 320 + j * 64)
            both = jnp.concatenate([q_rot, zeros] if g == 0 else [zeros, q_rot], axis=0)
            q_buf[pl.ds(g * 3 + j, n_rows, stride=8), :] = both.T[:n_rows]
    for r in (6, 7):
        q_buf[pl.ds(r, n_rows, stride=8), :] = jnp.zeros((n_rows, 128), F32)
    k_new = jnp.concatenate([rotate(192), rotate(320 + 192)], axis=0)
    v_new = jnp.concatenate([feats[256:320], feats[320 + 256:320 + 320]], axis=0)
    for i in range(n_blocks):
        kn_buf[i] = k_new if i == 0 else pltpu.roll(k_new, 128 - i * BB, 1)
        vn_buf[i] = v_new if i == 0 else pltpu.roll(v_new, 128 - i * BB, 1)

    def block(i, carry):
        for copy in fetch(i):
            copy.wait()
        k_cols, v_cols = kn_buf[i], vn_buf[i]
        lane = lax.broadcasted_iota(jnp.int32, (128, 128), 1)
        position = lax.broadcasted_iota(jnp.int32, (8, s_max), 1)
        scores = []
        for j in range(BB):
            b = i * BB + j
            pos = lens_ref[b]
            first = pl.multiple_of((pos // 128) * 128, 128)
            hit = lane == pos - first
            window = pl.ds(first, 128)
            k_buf[b, :, window] = jnp.where(hit, k_cols[:, j:j + 1], k_buf[b, :, window].astype(F32)).astype(BF16)
            v_buf[b, :, window] = jnp.where(hit, v_cols[:, j:j + 1], v_buf[b, :, window].astype(F32)).astype(BF16)
            rows = pl.ds(pl.multiple_of(b * 8, 8), 8)
            one = jnp.dot(q_buf[rows, :].astype(BF16), k_buf[b], preferred_element_type=F32) * 0.125
            scores.append(jnp.where(position <= pos, one, -jnp.inf))
        scores = jnp.concatenate(scores, axis=0)
        top = jnp.max(scores, axis=1, keepdims=True)
        weights = jnp.exp(scores - top)
        probs = weights * (1.0 / jnp.sum(weights, axis=1, keepdims=True))
        for j in range(BB):
            b = i * BB + j
            rows = pl.ds(pl.multiple_of(b * 8, 8), 8)
            c_buf[rows, :] = lax.dot_general(probs[j * 8:j * 8 + 8].astype(BF16), v_buf[b], NT, preferred_element_type=F32)
        return carry

    lax.fori_loop(0, n_blocks, block, 0)
    for i in range(n_blocks):
        for copy in flush(i):
            copy.start()
    heads = [c_buf[pl.ds(r, n_rows, stride=8), :] for r in range(6)]
    low = lax.broadcasted_iota(jnp.int32, (n_rows, 128), 1) < 64
    ctx_ref[:, 0:128] = jnp.where(low, heads[0], pltpu.roll(heads[1], 64, 1)).astype(BF16)
    ctx_ref[:, 128:256] = jnp.where(low, heads[2], heads[3]).astype(BF16)
    ctx_ref[:, 256:384] = jnp.where(low, pltpu.roll(heads[4], 64, 1), heads[5]).astype(BF16)
    for i in range(n_blocks):
        for copy in flush(i):
            copy.wait()


def moe_kernel(hid_ref, ctx_ref, bout_ref, scale_ref, bias_ref, wr_ref, ids_ref, wout_hbm, wg_hbm, wu_hbm, wd_hbm, out_ref,
               wout, wgu, wd, wr, part_f, part_b, rs_recv, x1_buf, h2, ids_buf, act, lo, hi, d_recv, y_send, y_recv, t_f, t_b, z_recv, o_buf,
               wsem, ssem, rsem):
    z, ep = lax.axis_index("tp"), lax.axis_index("ep")
    n_rows, d_model = hid_ref.shape
    n_exp = wgu.shape[0]
    width = d_model // COLS
    z_peers = [lax.rem(z + dz, 4) for dz in (1, 2, 3)]
    y_peer = lax.rem(ep + 2, 4)
    partner = ep + 1 - 2 * lax.rem(ep, 2)
    diagonal = 3 - ep
    barrier = pltpu.get_barrier_semaphore()
    for peer in z_peers:
        pl.semaphore_signal(barrier, inc=1, device_id={"tp": peer}, device_id_type=MESH)
    for peer in (y_peer, partner, diagonal):
        pl.semaphore_signal(barrier, inc=1, device_id={"ep": peer}, device_id_type=MESH)

    loads = [pltpu.make_async_copy(wout_hbm, wout, wsem.at[0])]
    for e in range(n_exp):
        loads.append(pltpu.make_async_copy(wg_hbm.at[e], wgu.at[e, :, 0:128], wsem.at[1 + 2 * e]))
        loads.append(pltpu.make_async_copy(wu_hbm.at[e], wgu.at[e, :, 128:256], wsem.at[2 + 2 * e]))
    loads.append(pltpu.make_async_copy(wd_hbm, wd, wsem.at[1 + 2 * n_exp]))
    for load in loads:
        load.start()

    sent = []

    def send(src, dst, slot, device):
        copy = pltpu.make_async_remote_copy(src_ref=src, dst_ref=dst, send_sem=ssem.at[slot], recv_sem=rsem.at[slot],
                                            device_id=device, device_id_type=MESH)
        copy.start()
        sent.append(copy)
        return copy

    loads[0].wait()
    part = jnp.dot(ctx_ref[...], wout[...], preferred_element_type=F32)
    part_f[...] = part
    part_b[...] = part.astype(BF16)
    wr[...] = jnp.concatenate([wr_ref[...], jnp.zeros((128 - wr_ref.shape[0], d_model), BF16)], axis=0)
    ids_buf[0] = ids_ref[...]
    pl.semaphore_wait(barrier, 6)

    def rows_of(index):
        return pl.ds(pl.multiple_of(index * 16, 16), 16)

    mine = rows_of(z)
    slot = 0
    rs = []
    for dz in range(3):
        rs.append(send(part_b.at[rows_of(z_peers[dz])], rs_recv.at[dz], slot, {"tp": z_peers[dz]}))
        slot += 1
    id_copies = []
    for shard, peer in ((1, y_peer), (2, partner), (3, diagonal)):
        id_copies.append(send(ids_ref, ids_buf.at[shard], slot, {"ep": peer}))
        slot += 1
    for copy in rs:
        copy.wait_recv()
    total = part_f[mine, :] + rs_recv[0].astype(F32) + rs_recv[1].astype(F32) + rs_recv[2].astype(F32)
    x1 = (hid_ref[mine, :].astype(F32) + total + row_of(bout_ref)).astype(BF16).astype(F32)
    x1_buf[...] = x1
    h2[mine, :] = normalize(x1, row_of(scale_ref), row_of(bias_ref))

    def piece(shard, index):
        return h2.at[pl.ds(pl.multiple_of(shard * n_rows + index * 16, 16), 16)]

    from_z, from_y, from_p = [], [], []
    for dz in range(3):
        from_z.append(send(piece(0, z), piece(0, z), slot, {"tp": z_peers[dz]}))
        slot += 1

    def pass_on(index):
        nonlocal slot
        from_y.append(send(piece(0, index), piece(1, index), slot, {"ep": y_peer}))
        slot += 1
        from_p.append(send(piece(0, index), piece(2, index), slot, {"ep": partner}))
        slot += 1

    z_order = [z] + [lax.rem(z + 4 - dz, 4) for dz in (1, 2, 3)]
    pass_on(z)
    for dz in range(3):
        from_z[dz].wait_recv()
        pass_on(z_order[dz + 1])

    def masks(shard):
        picks = ids_buf[shard]
        expert = lax.broadcasted_iota(jnp.int32, (128, n_rows), 0)
        hit = jnp.zeros((128, n_rows), F32)
        for k in range(picks.shape[0]):
            hit = jnp.where(expert == picks[k:k + 1, :], 1.0, hit)
        return hit.T

    def up(shard):
        rows = h2[shard * n_rows:(shard + 1) * n_rows, :]
        logits = lax.dot_general(rows, wr[...], NT, preferred_element_type=F32)
        picked = masks(shard) > 0.5
        logits = jnp.where(picked, logits, -jnp.inf)
        shifted = jnp.exp(logits - jnp.max(logits, axis=1, keepdims=True))
        gates = (shifted / jnp.sum(shifted, axis=1, keepdims=True)).astype(BF16).astype(F32)
        gates = pltpu.roll(gates, lax.rem(128 - ep * n_exp, 128), 1)
        for e in range(n_exp):
            if shard == 0:
                loads[1 + 2 * e].wait()
                loads[2 + 2 * e].wait()
            pre = jnp.dot(rows, wgu[e], preferred_element_type=F32)
            gate_pre, up_pre = pre[:, :128], pre[:, 128:]
            hidden = (gate_pre * jax.nn.sigmoid(gate_pre) * up_pre).astype(BF16).astype(F32)
            act[shard * n_rows:(shard + 1) * n_rows, e * 128:(e + 1) * 128] = (hidden * gates[:, e:e + 1]).astype(BF16)

    up(0)
    from_pp = []
    for k in range(4):
        from_y[k].wait_recv()
        index = z_order[k]
        from_pp.append(send(piece(1, index), piece(3, index), slot, {"ep": partner}))
        slot += 1
    for k in range(4):
        from_p[k].wait_recv()
    for copy in id_copies:
        copy.wait_recv()
    up(2)
    up(1)
    for k in range(4):
        from_pp[k].wait_recv()
    up(3)
    loads[-1].wait()

    def cols(n):
        return pl.ds(n * width, width)

    from_d, from_yy, from_zz, from_o = [], [], [], []

    def reduce_pair(n):
        nonlocal slot
        from_d[n].wait_recv()
        y_send[:, cols(n)] = (lo[64:128, cols(n)] + d_recv[64:128, cols(n)].astype(F32)).astype(BF16)
        from_yy.append(send(y_send.at[:, cols(n)], y_recv.at[:, cols(n)], slot, {"ep": y_peer}))
        slot += 1

    for n in range(COLS):
        hi[:, cols(n)] = jnp.dot(act[128:256, :], wd[:, cols(n)], preferred_element_type=F32).astype(BF16)
        from_d.append(send(hi.at[:, cols(n)], d_recv.at[:, cols(n)], slot, {"ep": partner}))
        slot += 1
        if n > 0:
            reduce_pair(n - 1)
        lo[:, cols(n)] = jnp.dot(act[0:128, :], wd[:, cols(n)], preferred_element_type=F32)
    reduce_pair(COLS - 1)
    for n in range(COLS):
        from_yy[n].wait_recv()
        t = lo[0:64, cols(n)] + d_recv[0:64, cols(n)].astype(F32) + y_recv[:, cols(n)].astype(F32)
        t_f[:, cols(n)] = t
        t_b[:, cols(n)] = t.astype(BF16)
        group = []
        for dz in range(3):
            group.append(send(t_b.at[rows_of(z_peers[dz]), cols(n)], z_recv.at[dz, :, cols(n)], slot, {"tp": z_peers[dz]}))
            slot += 1
        from_zz.append(group)
    for n in range(COLS):
        for copy in from_zz[n]:
            copy.wait_recv()
        moe = t_f[mine, cols(n)] + z_recv[0, :, cols(n)].astype(F32) + z_recv[1, :, cols(n)].astype(F32) + z_recv[2, :, cols(n)].astype(F32)
        o_buf[mine, cols(n)] = (x1_buf[:, cols(n)] + moe).astype(BF16)
        for dz in range(3):
            from_o.append(send(o_buf.at[mine, cols(n)], o_buf.at[mine, cols(n)], slot, {"tp": z_peers[dz]}))
            slot += 1
    for copy in from_o:
        copy.wait_recv()
    out_ref[...] = o_buf[...]
    for copy in sent:
        copy.wait_send()


N_SLOTS = 3 + 3 + 3 + 8 + 4 + COLS * 2 + COLS * 6


def solution(mesh):
    token_rows = P(('dp', 'ep'), None)
    token_vec = P(('dp', 'ep'))
    cache_spec = P(('dp', 'ep'), None, 'tp', None)
    expert_in = P('ep', None, 'tp')
    expert_down = P('ep', 'tp', None)
    vm = pl.BlockSpec(memory_space=pltpu.VMEM)
    anyspace = pl.BlockSpec(memory_space=pl.ANY)

    def device_step(hidden, seq_lens, rope_cos, rope_sin, ln1_scale, ln1_bias, w_qkv, b_qkv, w_out, b_out, k_cache, v_cache, ln2_scale, ln2_bias, w_router, expert_ids, w_gate, w_up, w_down):
        n, d = hidden.shape
        _, s_max, groups, head = k_cache.shape
        feat = groups * head
        n_exp = w_gate.shape[0]
        k_in = k_cache.transpose(0, 2, 3, 1).reshape(n, feat, s_max)
        v_in = v_cache.transpose(0, 2, 3, 1).reshape(n, feat, s_max)
        ctx, k_out, v_out = pl.pallas_call(
            attention_kernel,
            out_shape=(pltpu.VMEM((n, 384), BF16), jax.ShapeDtypeStruct(k_in.shape, BF16), jax.ShapeDtypeStruct(v_in.shape, BF16)),
            in_specs=[anyspace] * 10,
            out_specs=(vm, anyspace, anyspace),
            scratch_shapes=[
                pltpu.SMEM((n,), jnp.int32), pltpu.VMEM((n, d), BF16), pltpu.VMEM((32, n), F32), pltpu.VMEM((32, n), F32),
                pltpu.VMEM((d,), BF16), pltpu.VMEM((d,), BF16), pltpu.VMEM(b_qkv.shape, BF16),
                pltpu.VMEM(k_in.shape, BF16), pltpu.VMEM(v_in.shape, BF16), pltpu.VMEM(w_qkv.shape, BF16),
                pltpu.VMEM((n * 8, 128), F32), pltpu.VMEM((n // BB, 128, 128), F32), pltpu.VMEM((n // BB, 128, 128), F32), pltpu.VMEM((n * 8, 128), F32),
                pltpu.SemaphoreType.DMA((7,)), pltpu.SemaphoreType.DMA, pltpu.SemaphoreType.DMA((n // BB,)), pltpu.SemaphoreType.DMA((n // BB,)),
                pltpu.SemaphoreType.DMA((n // BB,)), pltpu.SemaphoreType.DMA((n // BB,)),
            ],
            compiler_params=pltpu.CompilerParams(vmem_limit_bytes=VMEM_LIMIT),
            name="attention",
        )(seq_lens, hidden, rope_cos.T, rope_sin.T, ln1_scale, ln1_bias, b_qkv, w_qkv, k_in, v_in)
        rows = lambda r, t: pltpu.VMEM((r, d), t)
        hidden_out = pl.pallas_call(
            moe_kernel,
            out_shape=pltpu.VMEM((n, d), BF16),
            in_specs=[vm] * 7 + [anyspace] * 4,
            out_specs=vm,
            scratch_shapes=[
                pltpu.VMEM(w_out.shape, BF16), pltpu.VMEM((n_exp, d, 256), BF16), pltpu.VMEM((n_exp * 128, d), BF16), rows(128, BF16),
                rows(64, F32), rows(64, BF16), pltpu.VMEM((3, 16, d), BF16), rows(16, F32), rows(256, BF16), pltpu.VMEM((4, 8, n), jnp.int32),
                pltpu.VMEM((256, n_exp * 128), BF16), rows(128, F32), rows(128, BF16), rows(128, BF16), rows(64, BF16), rows(64, BF16),
                rows(64, F32), rows(64, BF16), pltpu.VMEM((3, 16, d), BF16), rows(64, BF16),
                pltpu.SemaphoreType.DMA((2 * n_exp + 2,)), pltpu.SemaphoreType.DMA((N_SLOTS,)), pltpu.SemaphoreType.DMA((N_SLOTS,)),
            ],
            compiler_params=pltpu.CompilerParams(vmem_limit_bytes=MOE_LIMIT, collective_id=0, has_side_effects=True),
            name="moe",
        )(hidden, ctx, b_out, ln2_scale, ln2_bias, w_router.T, expert_ids.T, w_out, w_gate, w_up, w_down.reshape(n_exp * 128, d))
        unfold = lambda c: c.reshape(n, groups, head, s_max).transpose(0, 3, 1, 2)
        return hidden_out, unfold(k_out), unfold(v_out)

    in_specs = (token_rows, token_vec, token_rows, token_rows, P(), P(), P(None, 'tp'), P('tp'), P('tp', None), P(), cache_spec, cache_spec, P(), P(), P(), token_rows, expert_in, expert_in, expert_down)
    return jax.shard_map(device_step, mesh=mesh, in_specs=in_specs, out_specs=(token_rows, cache_spec, cache_spec), check_vma=False)
```

```python
import functools

import jax
import jax.numpy as jnp
from jax import lax
from jax.experimental import pallas as pl
from jax.experimental.pallas import tpu as pltpu
from jax.sharding import PartitionSpec as P

EPS = 1e-5
F32 = jnp.float32
BF16 = jnp.bfloat16
MESH = pl.DeviceIdType.MESH
VMEM_LIMIT = 66_400_000
MOE_LIMIT = 65_900_000
NT = (((1,), (1,)), ((), ()))
BB = 8
COLS = 6
LAG = 3
AHEAD = 3
W_PARTS = 4


def normalize(vals_f32, ln_scale, ln_bias):
    row_mean = jnp.mean(vals_f32, axis=-1, keepdims=True)
    centered = vals_f32 - row_mean
    row_var = jnp.mean(centered * centered, axis=-1, keepdims=True)
    normed = centered * lax.rsqrt(row_var + EPS)
    return (normed * ln_scale + ln_bias).astype(BF16)


def row_of(vec_ref):
    return vec_ref[...].astype(F32)[None, :]


def attention_kernel(lens_hbm, hid_hbm, cos_hbm, sin_hbm, scale_hbm, bias_hbm, bqkv_hbm, wqkv_hbm, wout_hbm, k_hbm, v_hbm,
                     part_ref, ko_hbm, vo_hbm, lens_ref, hid_ref, cos_ref, sin_ref, scale_ref, bias_ref, bqkv_ref,
                     k_buf, v_buf, w_buf, wo_buf, q_buf, kn_buf, vn_buf, c_buf, in_sem, w_sem, wo_sem, k_sem, v_sem, ko_sem, vo_sem):
    n_rows = hid_ref.shape[0]
    n_blocks = n_rows // BB
    s_max = k_buf.shape[2]
    smalls = ((hid_hbm, hid_ref), (scale_hbm, scale_ref), (bias_hbm, bias_ref), (bqkv_hbm, bqkv_ref), (cos_hbm, cos_ref), (sin_hbm, sin_ref),
              (lens_hbm, lens_ref))
    small_copies = [pltpu.make_async_copy(src, dst, in_sem.at[i]) for i, (src, dst) in enumerate(smalls)]
    w_rows = w_buf.shape[0] // W_PARTS
    w_copies = [pltpu.make_async_copy(wqkv_hbm.at[pl.ds(i * w_rows, w_rows)], w_buf.at[pl.ds(i * w_rows, w_rows)], w_sem.at[i]) for i in range(W_PARTS)]
    wo_copy = pltpu.make_async_copy(wout_hbm, wo_buf, wo_sem)
    for copy in small_copies[:3] + w_copies + small_copies[3:]:
        copy.start()

    def fetch(i):
        rows = pl.ds(i * BB, BB)
        return (pltpu.make_async_copy(k_hbm.at[rows], k_buf.at[rows], k_sem.at[i]),
                pltpu.make_async_copy(v_hbm.at[rows], v_buf.at[rows], v_sem.at[i]))

    def flush(i):
        rows = pl.ds(i * BB, BB)
        return (pltpu.make_async_copy(k_buf.at[rows], ko_hbm.at[rows], ko_sem.at[i]),
                pltpu.make_async_copy(v_buf.at[rows], vo_hbm.at[rows], vo_sem.at[i]))

    def fetch_start(i):
        for copy in fetch(i):
            copy.start()

    for i in range(AHEAD):
        fetch_start(i)

    for copy in small_copies:
        copy.wait()
    normed = normalize(hid_ref[...].astype(F32), row_of(scale_ref), row_of(bias_ref))
    for copy in w_copies:
        copy.wait()
    fetch_start(AHEAD)
    qkv = jnp.dot(normed, w_buf[...], preferred_element_type=F32) + row_of(bqkv_ref)
    qkv = qkv.astype(BF16).astype(F32)
    qkv = jnp.concatenate([qkv, jnp.zeros((128 - n_rows, qkv.shape[1]), F32)], axis=0)
    feats = qkv.T
    cos_t = jnp.concatenate([cos_ref[...], jnp.zeros((32, 128 - n_rows), F32)], axis=1)
    sin_t = jnp.concatenate([sin_ref[...], jnp.zeros((32, 128 - n_rows), F32)], axis=1)

    def rotate(base):
        u, w = feats[base:base + 32], feats[base + 32:base + 64]
        return jnp.concatenate([u * cos_t - w * sin_t, w * cos_t + u * sin_t], axis=0).astype(BF16).astype(F32)

    zeros = jnp.zeros((64, 128), F32)
    for g in range(2):
        for j in range(3):
            q_rot = rotate(g * 320 + j * 64)
            both = jnp.concatenate([q_rot, zeros] if g == 0 else [zeros, q_rot], axis=0)
            q_buf[pl.ds(g * 3 + j, n_rows, stride=8), :] = both.T[:n_rows]
    for r in (6, 7):
        q_buf[pl.ds(r, n_rows, stride=8), :] = jnp.zeros((n_rows, 128), F32)
    k_new = jnp.concatenate([rotate(192), rotate(320 + 192)], axis=0)
    v_new = jnp.concatenate([feats[256:320], feats[320 + 256:320 + 320]], axis=0)
    for i in range(n_blocks):
        kn_buf[i] = k_new if i == 0 else pltpu.roll(k_new, 128 - i * BB, 1)
        vn_buf[i] = v_new if i == 0 else pltpu.roll(v_new, 128 - i * BB, 1)

    def block(i, carry):
        for copy in fetch(i):
            copy.wait()

        @pl.when(i + AHEAD + 1 < n_blocks)
        def _():
            fetch_start(i + AHEAD + 1)

        @pl.when(i == n_blocks - AHEAD - 1)
        def _():
            wo_copy.start()

        k_cols, v_cols = kn_buf[i], vn_buf[i]
        lane = lax.broadcasted_iota(jnp.int32, (128, 128), 1)
        position = lax.broadcasted_iota(jnp.int32, (8, s_max), 1)
        scores = []
        for j in range(BB):
            b = i * BB + j
            pos = lens_ref[b]
            first = pl.multiple_of((pos // 128) * 128, 128)
            hit = lane == pos - first
            window = pl.ds(first, 128)
            k_buf[b, :, window] = jnp.where(hit, k_cols[:, j:j + 1], k_buf[b, :, window].astype(F32)).astype(BF16)
            v_buf[b, :, window] = jnp.where(hit, v_cols[:, j:j + 1], v_buf[b, :, window].astype(F32)).astype(BF16)
            rows = pl.ds(pl.multiple_of(b * 8, 8), 8)
            one = jnp.dot(q_buf[rows, :].astype(BF16), k_buf[b], preferred_element_type=F32) * 0.125
            scores.append(jnp.where(position <= pos, one, -jnp.inf))
        scores = jnp.concatenate(scores, axis=0)
        top = jnp.max(scores, axis=1, keepdims=True)
        weights = jnp.exp(scores - top)
        probs = weights * (1.0 / jnp.sum(weights, axis=1, keepdims=True))
        for j in range(BB):
            b = i * BB + j
            rows = pl.ds(pl.multiple_of(b * 8, 8), 8)
            c_buf[rows, :] = lax.dot_general(probs[j * 8:j * 8 + 8].astype(BF16), v_buf[b], NT, preferred_element_type=F32)
        for copy in flush(i):
            copy.start()
        return carry

    lax.fori_loop(0, n_blocks, block, 0)
    heads = [c_buf[pl.ds(r, n_rows, stride=8), :] for r in range(6)]
    low = lax.broadcasted_iota(jnp.int32, (n_rows, 128), 1) < 64
    ctx = jnp.concatenate([
        jnp.where(low, heads[0], pltpu.roll(heads[1], 64, 1)),
        jnp.where(low, heads[2], heads[3]),
        jnp.where(low, pltpu.roll(heads[4], 64, 1), heads[5]),
    ], axis=1).astype(BF16)
    wo_copy.wait()
    part_ref[...] = jnp.dot(ctx, wo_buf[...], preferred_element_type=F32).astype(BF16)
    for i in range(n_blocks):
        for copy in flush(i):
            copy.wait()


def moe_kernel(hid_ref, part_ref, bout_ref, scale_ref, bias_ref, wr_ref, ids_ref, wg_hbm, wu_hbm, wd_hbm, out_ref,
               wgu, wd, wr, part, from_end, pair, across_in, x1, h2, ids_buf, act, lo, hi, d_recv, y_send, y_recv,
               t_part, t_end, t_pair, t_across, o_buf, wsem, ssem, rsem):
    z, ep = lax.axis_index("tp"), lax.axis_index("ep")
    n_rows, d_model = hid_ref.shape
    n_exp = wgu.shape[0]
    width = d_model // COLS
    n_pieces = n_rows // 16
    near = z + 1 - 2 * lax.rem(z, 2)
    across = 3 - z
    y_peer = lax.rem(ep + 2, 4)
    partner = ep + 1 - 2 * lax.rem(ep, 2)
    diagonal = 3 - ep
    is_mid = jnp.logical_or(z == 1, z == 2)
    is_end = jnp.logical_or(z == 0, z == 3)
    barrier = pltpu.get_barrier_semaphore()
    pl.semaphore_signal(barrier, inc=1, device_id={"tp": near}, device_id_type=MESH)
    for peer in (y_peer, partner, diagonal):
        pl.semaphore_signal(barrier, inc=1, device_id={"ep": peer}, device_id_type=MESH)

    @pl.when(is_mid)
    def _():
        pl.semaphore_signal(barrier, inc=1, device_id={"tp": across}, device_id_type=MESH)

    loads = []
    for e in range(n_exp):
        loads.append(pltpu.make_async_copy(wg_hbm.at[e], wgu.at[e, :, 0:128], wsem.at[2 * e]))
        loads.append(pltpu.make_async_copy(wu_hbm.at[e], wgu.at[e, :, 128:256], wsem.at[2 * e + 1]))
    loads.append(pltpu.make_async_copy(wd_hbm, wd, wsem.at[2 * n_exp]))
    for load in loads:
        load.start()

    part[...] = part_ref[...]
    ids_buf[0] = ids_ref[...]
    wr[...] = jnp.concatenate([wr_ref[...], jnp.zeros((128 - wr_ref.shape[0], d_model), BF16)], axis=0)

    count = [0]

    def slots(n):
        count[0] += n
        return list(range(count[0] - n, count[0]))

    def remote(src, dst, slot, device):
        return pltpu.make_async_remote_copy(src_ref=src, dst_ref=dst, send_sem=ssem.at[slot], recv_sem=rsem.at[slot],
                                            device_id=device, device_id_type=MESH)

    def rows(k, shard=0):
        return pl.ds(shard * n_rows + k * 16, 16)

    def cols(n):
        return pl.ds(n * width, width)

    s_a, s_b, s_c, s_y, s_p, s_pp = (slots(n_pieces) for _ in range(6))
    s_ids = slots(3)
    s_d, s_yy, s_e, s_f, s_g = (slots(COLS) for _ in range(5))
    pieces = range(n_pieces)
    a = [remote(part.at[rows(k)], from_end.at[rows(k)], s_a[k], {"tp": near}) for k in pieces]
    b = [remote(pair.at[rows(k)], across_in.at[rows(k)], s_b[k], {"tp": across}) for k in pieces]
    c = [remote(x1.at[rows(k)], x1.at[rows(k)], s_c[k], {"tp": near}) for k in pieces]
    to_y = [remote(h2.at[rows(k)], h2.at[rows(k, 1)], s_y[k], {"ep": y_peer}) for k in pieces]
    to_p = [remote(h2.at[rows(k)], h2.at[rows(k, 2)], s_p[k], {"ep": partner}) for k in pieces]
    y_to_p = [remote(h2.at[rows(k, 1)], h2.at[rows(k, 3)], s_pp[k], {"ep": partner}) for k in pieces]
    to_ids = [remote(ids_ref, ids_buf.at[i + 1], s_ids[i], {"ep": peer}) for i, peer in enumerate((y_peer, partner, diagonal))]
    chunks = range(COLS)
    to_d = [remote(hi.at[:, cols(n)], d_recv.at[:, cols(n)], s_d[n], {"ep": partner}) for n in chunks]
    to_yy = [remote(y_send.at[:, cols(n)], y_recv.at[:, cols(n)], s_yy[n], {"ep": y_peer}) for n in chunks]
    to_mid = [remote(t_part.at[:, cols(n)], t_end.at[:, cols(n)], s_e[n], {"tp": near}) for n in chunks]
    to_mate = [remote(t_pair.at[:, cols(n)], t_across.at[:, cols(n)], s_f[n], {"tp": across}) for n in chunks]
    to_end = [remote(o_buf.at[:, cols(n)], o_buf.at[:, cols(n)], s_g[n], {"tp": near}) for n in chunks]

    @pl.when(is_end)
    def _():
        pl.semaphore_wait(barrier, 4)
        for k in pieces:
            a[k].start()

    @pl.when(is_mid)
    def _():
        pl.semaphore_wait(barrier, 5)

    for copy in to_ids:
        copy.start()

    @pl.when(is_mid)
    def _():
        for k in pieces:
            a[k].wait_recv()
            pair[rows(k), :] = (part[rows(k), :].astype(F32) + from_end[rows(k), :].astype(F32)).astype(BF16)
            b[k].start()

    scale, bias, bout = row_of(scale_ref), row_of(bias_ref), row_of(bout_ref)
    for k in pieces:
        @pl.when(is_mid)
        def _():
            b[k].wait_recv()
            total = pair[rows(k), :].astype(F32) + across_in[rows(k), :].astype(F32)
            x1[rows(k), :] = (hid_ref[rows(k), :].astype(F32) + total + bout).astype(BF16)
            c[k].start()

        @pl.when(is_end)
        def _():
            c[k].wait_recv()

        h2[rows(k), :] = normalize(x1[rows(k), :].astype(F32), scale, bias)
        to_y[k].start()
        to_p[k].start()

    def masks(shard):
        picks = ids_buf[shard]
        expert = lax.broadcasted_iota(jnp.int32, (128, n_rows), 0)
        hit = jnp.zeros((128, n_rows), F32)
        for k in range(picks.shape[0]):
            hit = jnp.where(expert == picks[k:k + 1, :], 1.0, hit)
        return hit.T

    def up(shard):
        toks = h2[shard * n_rows:(shard + 1) * n_rows, :]
        logits = lax.dot_general(toks, wr[...], NT, preferred_element_type=F32)
        logits = jnp.where(masks(shard) > 0.5, logits, -jnp.inf)
        shifted = jnp.exp(logits - jnp.max(logits, axis=1, keepdims=True))
        gates = (shifted / jnp.sum(shifted, axis=1, keepdims=True)).astype(BF16).astype(F32)
        gates = pltpu.roll(gates, lax.rem(128 - ep * n_exp, 128), 1)
        for e in range(n_exp):
            if shard == 0:
                loads[2 * e].wait()
                loads[2 * e + 1].wait()
            pre = jnp.dot(toks, wgu[e], preferred_element_type=F32)
            gate_pre, up_pre = pre[:, :128], pre[:, 128:]
            hidden = (gate_pre * jax.nn.sigmoid(gate_pre) * up_pre).astype(BF16).astype(F32)
            act[shard * n_rows:(shard + 1) * n_rows, e * 128:(e + 1) * 128] = (hidden * gates[:, e:e + 1]).astype(BF16)

    def relay(k):
        to_y[k].wait_recv()
        y_to_p[k].start()

    for k in (0, 1):
        relay(k)
    up(0)
    for k in (2, 3):
        relay(k)
    for copy in to_p + to_ids:
        copy.wait_recv()
    up(2)
    up(1)
    for copy in y_to_p:
        copy.wait_recv()
    up(3)
    loads[-1].wait()

    def reduce_pair(n):
        to_d[n].wait_recv()
        y_send[:, cols(n)] = (lo[64:128, cols(n)] + d_recv[64:128, cols(n)].astype(F32)).astype(BF16)
        to_yy[n].start()

    for n in chunks:
        hi[:, cols(n)] = jnp.dot(act[128:256, :], wd[:, cols(n)], preferred_element_type=F32).astype(BF16)
        to_d[n].start()
        lo[:, cols(n)] = jnp.dot(act[0:128, :], wd[:, cols(n)], preferred_element_type=F32)
        if n >= LAG:
            reduce_pair(n - LAG)
    for n in range(COLS - LAG, COLS):
        reduce_pair(n)

    def own_sum(n):
        to_yy[n].wait_recv()
        return lo[0:64, cols(n)] + d_recv[0:64, cols(n)].astype(F32) + y_recv[:, cols(n)].astype(F32)

    @pl.when(is_end)
    def _():
        for n in chunks:
            t_part[:, cols(n)] = own_sum(n).astype(BF16)
            to_mid[n].start()
        for n in chunks:
            to_end[n].wait_recv()

    @pl.when(is_mid)
    def _():
        for n in chunks:
            mine = own_sum(n)
            to_mid[n].wait_recv()
            t_pair[:, cols(n)] = (mine + t_end[:, cols(n)].astype(F32)).astype(BF16)
            to_mate[n].start()
        for n in chunks:
            to_mate[n].wait_recv()
            moe = t_pair[:, cols(n)].astype(F32) + t_across[:, cols(n)].astype(F32)
            o_buf[:, cols(n)] = (x1[:, cols(n)].astype(F32) + moe).astype(BF16)
            to_end[n].start()

    out_ref[...] = o_buf[...]
    for copy in to_y + to_p + y_to_p + to_ids + to_d + to_yy:
        copy.wait_send()

    @pl.when(is_end)
    def _():
        for copy in a + to_mid:
            copy.wait_send()

    @pl.when(is_mid)
    def _():
        for copy in b + c + to_mate + to_end:
            copy.wait_send()


N_SLOTS = 6 * 4 + 3 + 5 * COLS


def solution(mesh):
    token_rows = P(('dp', 'ep'), None)
    token_vec = P(('dp', 'ep'))
    cache_spec = P(('dp', 'ep'), None, 'tp', None)
    expert_in = P('ep', None, 'tp')
    expert_down = P('ep', 'tp', None)
    vm = pl.BlockSpec(memory_space=pltpu.VMEM)
    anyspace = pl.BlockSpec(memory_space=pl.ANY)

    def device_step(hidden, seq_lens, rope_cos, rope_sin, ln1_scale, ln1_bias, w_qkv, b_qkv, w_out, b_out, k_cache, v_cache, ln2_scale, ln2_bias, w_router, expert_ids, w_gate, w_up, w_down):
        n, d = hidden.shape
        _, s_max, groups, head = k_cache.shape
        feat = groups * head
        n_exp = w_gate.shape[0]
        k_in = k_cache.transpose(0, 2, 3, 1).reshape(n, feat, s_max)
        v_in = v_cache.transpose(0, 2, 3, 1).reshape(n, feat, s_max)
        part, k_out, v_out = pl.pallas_call(
            attention_kernel,
            out_shape=(pltpu.VMEM((n, d), BF16), jax.ShapeDtypeStruct(k_in.shape, BF16), jax.ShapeDtypeStruct(v_in.shape, BF16)),
            in_specs=[anyspace] * 11,
            out_specs=(vm, anyspace, anyspace),
            scratch_shapes=[
                pltpu.SMEM((n,), jnp.int32), pltpu.VMEM((n, d), BF16), pltpu.VMEM((32, n), F32), pltpu.VMEM((32, n), F32),
                pltpu.VMEM((d,), BF16), pltpu.VMEM((d,), BF16), pltpu.VMEM(b_qkv.shape, BF16),
                pltpu.VMEM(k_in.shape, BF16), pltpu.VMEM(v_in.shape, BF16), pltpu.VMEM(w_qkv.shape, BF16), pltpu.VMEM(w_out.shape, BF16),
                pltpu.VMEM((n * 8, 128), F32), pltpu.VMEM((n // BB, 128, 128), F32), pltpu.VMEM((n // BB, 128, 128), F32), pltpu.VMEM((n * 8, 128), F32),
                pltpu.SemaphoreType.DMA((7,)), pltpu.SemaphoreType.DMA((W_PARTS,)), pltpu.SemaphoreType.DMA, pltpu.SemaphoreType.DMA((n // BB,)), pltpu.SemaphoreType.DMA((n // BB,)),
                pltpu.SemaphoreType.DMA((n // BB,)), pltpu.SemaphoreType.DMA((n // BB,)),
            ],
            compiler_params=pltpu.CompilerParams(vmem_limit_bytes=VMEM_LIMIT),
            name="attention",
        )(seq_lens, hidden, rope_cos.T, rope_sin.T, ln1_scale, ln1_bias, b_qkv, w_qkv, w_out, k_in, v_in)
        part = pltpu.with_memory_space_constraint(part, pltpu.VMEM)
        rows = lambda r, t: pltpu.VMEM((r, d), t)
        hidden_out = pl.pallas_call(
            moe_kernel,
            out_shape=pltpu.VMEM((n, d), BF16),
            in_specs=[vm] * 7 + [anyspace] * 3,
            out_specs=vm,
            scratch_shapes=[
                pltpu.VMEM((n_exp, d, 256), BF16), pltpu.VMEM((n_exp * 128, d), BF16), rows(128, BF16),
                rows(64, BF16), rows(64, BF16), rows(64, BF16), rows(64, BF16), rows(64, BF16), rows(256, BF16), pltpu.VMEM((4, 8, n), jnp.int32),
                pltpu.VMEM((256, n_exp * 128), BF16), rows(128, F32), rows(128, BF16), rows(128, BF16), rows(64, BF16), rows(64, BF16),
                rows(64, BF16), rows(64, BF16), rows(64, BF16), rows(64, BF16), rows(64, BF16),
                pltpu.SemaphoreType.DMA((2 * n_exp + 1,)), pltpu.SemaphoreType.DMA((N_SLOTS,)), pltpu.SemaphoreType.DMA((N_SLOTS,)),
            ],
            compiler_params=pltpu.CompilerParams(vmem_limit_bytes=MOE_LIMIT, collective_id=0, has_side_effects=True),
            name="moe",
        )(hidden, part, b_out, ln2_scale, ln2_bias, w_router.T, expert_ids.T, w_gate, w_up, w_down.reshape(n_exp * 128, d))
        unfold = lambda c: c.reshape(n, groups, head, s_max).transpose(0, 3, 1, 2)
        return hidden_out, unfold(k_out), unfold(v_out)

    in_specs = (token_rows, token_vec, token_rows, token_rows, P(), P(), P(None, 'tp'), P('tp'), P('tp', None), P(), cache_spec, cache_spec, P(), P(), P(), token_rows, expert_in, expert_in, expert_down)
    return jax.shard_map(device_step, mesh=mesh, in_specs=in_specs, out_specs=(token_rows, cache_spec, cache_spec), check_vma=False)
```

```python
import functools

import jax
import jax.numpy as jnp
from jax import lax
from jax.experimental import pallas as pl
from jax.experimental.pallas import tpu as pltpu
from jax.sharding import PartitionSpec as P

EPS = 1e-5
F32 = jnp.float32
BF16 = jnp.bfloat16
MESH = pl.DeviceIdType.MESH
VMEM_LIMIT = 66_400_000
MOE_LIMIT = 64_500_000
NT = (((1,), (1,)), ((), ()))
BB = 8
COLS = 3
AHEAD = 3
W_PARTS = 4


def normalize(vals_f32, ln_scale, ln_bias):
    row_mean = jnp.mean(vals_f32, axis=-1, keepdims=True)
    centered = vals_f32 - row_mean
    row_var = jnp.mean(centered * centered, axis=-1, keepdims=True)
    normed = centered * lax.rsqrt(row_var + EPS)
    return (normed * ln_scale + ln_bias).astype(BF16)


def row_of(vec_ref):
    return vec_ref[...].astype(F32)[None, :]


def attention_kernel(lens_hbm, hid_hbm, cos_hbm, sin_hbm, scale_hbm, bias_hbm, bqkv_hbm, wqkv_hbm, wout_hbm, k_hbm, v_hbm,
                     part_ref, ko_hbm, vo_hbm, lens_ref, hid_ref, cos_ref, sin_ref, scale_ref, bias_ref, bqkv_ref,
                     k_buf, v_buf, w_buf, wo_buf, q_buf, kn_buf, vn_buf, c_buf, in_sem, w_sem, wo_sem, k_sem, v_sem, ko_sem, vo_sem):
    n_rows = hid_ref.shape[0]
    n_blocks = n_rows // BB
    s_max = k_buf.shape[2]
    smalls = ((hid_hbm, hid_ref), (scale_hbm, scale_ref), (bias_hbm, bias_ref), (bqkv_hbm, bqkv_ref), (cos_hbm, cos_ref), (sin_hbm, sin_ref),
              (lens_hbm, lens_ref))
    small_copies = [pltpu.make_async_copy(src, dst, in_sem.at[i]) for i, (src, dst) in enumerate(smalls)]
    w_rows = w_buf.shape[0] // W_PARTS
    w_copies = [pltpu.make_async_copy(wqkv_hbm.at[pl.ds(i * w_rows, w_rows)], w_buf.at[pl.ds(i * w_rows, w_rows)], w_sem.at[i]) for i in range(W_PARTS)]
    wo_copy = pltpu.make_async_copy(wout_hbm, wo_buf, wo_sem)
    for copy in small_copies[:3] + w_copies + small_copies[3:]:
        copy.start()

    def fetch(i):
        rows = pl.ds(i * BB, BB)
        return (pltpu.make_async_copy(k_hbm.at[rows], k_buf.at[rows], k_sem.at[i]),
                pltpu.make_async_copy(v_hbm.at[rows], v_buf.at[rows], v_sem.at[i]))

    def flush(i):
        rows = pl.ds(i * BB, BB)
        return (pltpu.make_async_copy(k_buf.at[rows], ko_hbm.at[rows], ko_sem.at[i]),
                pltpu.make_async_copy(v_buf.at[rows], vo_hbm.at[rows], vo_sem.at[i]))

    def fetch_start(i):
        for copy in fetch(i):
            copy.start()

    for i in range(AHEAD):
        fetch_start(i)

    for copy in small_copies:
        copy.wait()
    normed = normalize(hid_ref[...].astype(F32), row_of(scale_ref), row_of(bias_ref))
    for copy in w_copies:
        copy.wait()
    fetch_start(AHEAD)
    qkv = jnp.dot(normed, w_buf[...], preferred_element_type=F32) + row_of(bqkv_ref)
    qkv = qkv.astype(BF16).astype(F32)
    qkv = jnp.concatenate([qkv, jnp.zeros((128 - n_rows, qkv.shape[1]), F32)], axis=0)
    feats = qkv.T
    cos_t = jnp.concatenate([cos_ref[...], jnp.zeros((32, 128 - n_rows), F32)], axis=1)
    sin_t = jnp.concatenate([sin_ref[...], jnp.zeros((32, 128 - n_rows), F32)], axis=1)

    def rotate(base):
        u, w = feats[base:base + 32], feats[base + 32:base + 64]
        return jnp.concatenate([u * cos_t - w * sin_t, w * cos_t + u * sin_t], axis=0).astype(BF16).astype(F32)

    zeros = jnp.zeros((64, 128), F32)
    for g in range(2):
        for j in range(3):
            q_rot = rotate(g * 320 + j * 64)
            both = jnp.concatenate([q_rot, zeros] if g == 0 else [zeros, q_rot], axis=0)
            q_buf[pl.ds(g * 3 + j, n_rows, stride=8), :] = both.T[:n_rows]
    for r in (6, 7):
        q_buf[pl.ds(r, n_rows, stride=8), :] = jnp.zeros((n_rows, 128), F32)
    k_new = jnp.concatenate([rotate(192), rotate(320 + 192)], axis=0)
    v_new = jnp.concatenate([feats[256:320], feats[320 + 256:320 + 320]], axis=0)
    for i in range(n_blocks):
        kn_buf[i] = k_new if i == 0 else pltpu.roll(k_new, 128 - i * BB, 1)
        vn_buf[i] = v_new if i == 0 else pltpu.roll(v_new, 128 - i * BB, 1)

    def block(i, carry):
        for copy in fetch(i):
            copy.wait()

        @pl.when(i + AHEAD + 1 < n_blocks)
        def _():
            fetch_start(i + AHEAD + 1)

        @pl.when(i == n_blocks - AHEAD - 1)
        def _():
            wo_copy.start()

        k_cols, v_cols = kn_buf[i], vn_buf[i]
        lane = lax.broadcasted_iota(jnp.int32, (128, 128), 1)
        position = lax.broadcasted_iota(jnp.int32, (8, s_max), 1)
        scores = []
        for j in range(BB):
            b = i * BB + j
            pos = lens_ref[b]
            first = pl.multiple_of((pos // 128) * 128, 128)
            hit = lane == pos - first
            window = pl.ds(first, 128)
            k_buf[b, :, window] = jnp.where(hit, k_cols[:, j:j + 1], k_buf[b, :, window].astype(F32)).astype(BF16)
            v_buf[b, :, window] = jnp.where(hit, v_cols[:, j:j + 1], v_buf[b, :, window].astype(F32)).astype(BF16)
            rows = pl.ds(pl.multiple_of(b * 8, 8), 8)
            one = jnp.dot(q_buf[rows, :].astype(BF16), k_buf[b], preferred_element_type=F32) * 0.125
            scores.append(jnp.where(position <= pos, one, -jnp.inf))
        scores = jnp.concatenate(scores, axis=0)
        top = jnp.max(scores, axis=1, keepdims=True)
        weights = jnp.exp(scores - top)
        probs = weights * (1.0 / jnp.sum(weights, axis=1, keepdims=True))
        for j in range(BB):
            b = i * BB + j
            rows = pl.ds(pl.multiple_of(b * 8, 8), 8)
            c_buf[rows, :] = lax.dot_general(probs[j * 8:j * 8 + 8].astype(BF16), v_buf[b], NT, preferred_element_type=F32)
        for copy in flush(i):
            copy.start()
        return carry

    lax.fori_loop(0, n_blocks, block, 0)
    heads = [c_buf[pl.ds(r, n_rows, stride=8), :] for r in range(6)]
    low = lax.broadcasted_iota(jnp.int32, (n_rows, 128), 1) < 64
    ctx = jnp.concatenate([
        jnp.where(low, heads[0], pltpu.roll(heads[1], 64, 1)),
        jnp.where(low, heads[2], heads[3]),
        jnp.where(low, pltpu.roll(heads[4], 64, 1), heads[5]),
    ], axis=1).astype(BF16)
    wo_copy.wait()
    part_ref[...] = jnp.dot(ctx, wo_buf[...], preferred_element_type=F32).astype(BF16)
    for i in range(n_blocks):
        for copy in flush(i):
            copy.wait()


def moe_kernel(hid_ref, part_ref, bout_ref, scale_ref, bias_ref, wr_ref, ids_ref, wg_hbm, wu_hbm, wd_hbm, out_ref,
               wgu, wd, wr, rs_recv, x1_buf, h2, ids_buf, act, lo, hi, d_recv, y_send, y_recv, t_f, t_b, z_recv, o_buf,
               wsem, ssem, rsem):
    z, ep = lax.axis_index("tp"), lax.axis_index("ep")
    n_rows, d_model = hid_ref.shape
    n_exp = wgu.shape[0]
    width = d_model // COLS
    z_peers = [lax.rem(z + dz, 4) for dz in (1, 2, 3)]
    y_peer = lax.rem(ep + 2, 4)
    partner = ep + 1 - 2 * lax.rem(ep, 2)
    diagonal = 3 - ep
    barrier = pltpu.get_barrier_semaphore()
    for peer in z_peers:
        pl.semaphore_signal(barrier, inc=1, device_id={"tp": peer}, device_id_type=MESH)
    for peer in (y_peer, partner, diagonal):
        pl.semaphore_signal(barrier, inc=1, device_id={"ep": peer}, device_id_type=MESH)

    loads = [None]
    for e in range(n_exp):
        loads.append(pltpu.make_async_copy(wg_hbm.at[e], wgu.at[e, :, 0:128], wsem.at[1 + 2 * e]))
        loads.append(pltpu.make_async_copy(wu_hbm.at[e], wgu.at[e, :, 128:256], wsem.at[2 + 2 * e]))
    loads.append(pltpu.make_async_copy(wd_hbm, wd, wsem.at[1 + 2 * n_exp]))
    for load in loads[1:]:
        load.start()

    sent = []

    def send(src, dst, slot, device):
        copy = pltpu.make_async_remote_copy(src_ref=src, dst_ref=dst, send_sem=ssem.at[slot], recv_sem=rsem.at[slot],
                                            device_id=device, device_id_type=MESH)
        copy.start()
        sent.append(copy)
        return copy

    wr[...] = jnp.concatenate([wr_ref[...], jnp.zeros((128 - wr_ref.shape[0], d_model), BF16)], axis=0)
    ids_buf[0] = ids_ref[...]
    pl.semaphore_wait(barrier, 6)

    def rows_of(index):
        return pl.ds(pl.multiple_of(index * 16, 16), 16)

    mine = rows_of(z)
    slot = 0
    rs = []
    for dz in range(3):
        rs.append(send(part_ref.at[rows_of(z_peers[dz])], rs_recv.at[dz], slot, {"tp": z_peers[dz]}))
        slot += 1
    id_copies = []
    for shard, peer in ((1, y_peer), (2, partner), (3, diagonal)):
        id_copies.append(send(ids_ref, ids_buf.at[shard], slot, {"ep": peer}))
        slot += 1
    for copy in rs:
        copy.wait_recv()
    total = part_ref[mine, :].astype(F32) + rs_recv[0].astype(F32) + rs_recv[1].astype(F32) + rs_recv[2].astype(F32)
    x1 = (hid_ref[mine, :].astype(F32) + total + row_of(bout_ref)).astype(BF16).astype(F32)
    x1_buf[...] = x1
    h2[mine, :] = normalize(x1, row_of(scale_ref), row_of(bias_ref))

    def piece(shard, index):
        return h2.at[pl.ds(pl.multiple_of(shard * n_rows + index * 16, 16), 16)]

    from_z, from_y, from_p = [], [], []
    for dz in range(3):
        from_z.append(send(piece(0, z), piece(0, z), slot, {"tp": z_peers[dz]}))
        slot += 1

    def pass_on(index):
        nonlocal slot
        from_y.append(send(piece(0, index), piece(1, index), slot, {"ep": y_peer}))
        slot += 1
        from_p.append(send(piece(0, index), piece(2, index), slot, {"ep": partner}))
        slot += 1

    z_order = [z] + [lax.rem(z + 4 - dz, 4) for dz in (1, 2, 3)]
    pass_on(z)
    for dz in range(3):
        from_z[dz].wait_recv()
        pass_on(z_order[dz + 1])

    def masks(shard):
        picks = ids_buf[shard]
        expert = lax.broadcasted_iota(jnp.int32, (128, n_rows), 0)
        hit = jnp.zeros((128, n_rows), F32)
        for k in range(picks.shape[0]):
            hit = jnp.where(expert == picks[k:k + 1, :], 1.0, hit)
        return hit.T

    def up(shard):
        rows = h2[shard * n_rows:(shard + 1) * n_rows, :]
        logits = lax.dot_general(rows, wr[...], NT, preferred_element_type=F32)
        picked = masks(shard) > 0.5
        logits = jnp.where(picked, logits, -jnp.inf)
        shifted = jnp.exp(logits - jnp.max(logits, axis=1, keepdims=True))
        gates = (shifted / jnp.sum(shifted, axis=1, keepdims=True)).astype(BF16).astype(F32)
        gates = pltpu.roll(gates, lax.rem(128 - ep * n_exp, 128), 1)
        for e in range(n_exp):
            if shard == 0:
                loads[1 + 2 * e].wait()
                loads[2 + 2 * e].wait()
            pre = jnp.dot(rows, wgu[e], preferred_element_type=F32)
            gate_pre, up_pre = pre[:, :128], pre[:, 128:]
            hidden = (gate_pre * jax.nn.sigmoid(gate_pre) * up_pre).astype(BF16).astype(F32)
            act[shard * n_rows:(shard + 1) * n_rows, e * 128:(e + 1) * 128] = (hidden * gates[:, e:e + 1]).astype(BF16)

    up(0)
    from_pp = []
    for k in range(4):
        from_y[k].wait_recv()
        index = z_order[k]
        from_pp.append(send(piece(1, index), piece(3, index), slot, {"ep": partner}))
        slot += 1
    for k in range(4):
        from_p[k].wait_recv()
    for copy in id_copies:
        copy.wait_recv()
    up(2)
    up(1)
    for k in range(4):
        from_pp[k].wait_recv()
    up(3)
    loads[-1].wait()

    def cols(n):
        return pl.ds(n * width, width)

    from_d, from_yy, from_zz, from_o = [], [], [], []

    def reduce_pair(n):
        nonlocal slot
        from_d[n].wait_recv()
        y_send[:, cols(n)] = (lo[64:128, cols(n)] + d_recv[64:128, cols(n)].astype(F32)).astype(BF16)
        from_yy.append(send(y_send.at[:, cols(n)], y_recv.at[:, cols(n)], slot, {"ep": y_peer}))
        slot += 1

    for n in range(COLS):
        hi[:, cols(n)] = jnp.dot(act[128:256, :], wd[:, cols(n)], preferred_element_type=F32).astype(BF16)
        from_d.append(send(hi.at[:, cols(n)], d_recv.at[:, cols(n)], slot, {"ep": partner}))
        slot += 1
        if n > 0:
            reduce_pair(n - 1)
        lo[:, cols(n)] = jnp.dot(act[0:128, :], wd[:, cols(n)], preferred_element_type=F32)
    reduce_pair(COLS - 1)
    for n in range(COLS):
        from_yy[n].wait_recv()
        t = lo[0:64, cols(n)] + d_recv[0:64, cols(n)].astype(F32) + y_recv[:, cols(n)].astype(F32)
        t_f[:, cols(n)] = t
        t_b[:, cols(n)] = t.astype(BF16)
        group = []
        for dz in range(3):
            group.append(send(t_b.at[rows_of(z_peers[dz]), cols(n)], z_recv.at[dz, :, cols(n)], slot, {"tp": z_peers[dz]}))
            slot += 1
        from_zz.append(group)
    for n in range(COLS):
        for copy in from_zz[n]:
            copy.wait_recv()
        moe = t_f[mine, cols(n)] + z_recv[0, :, cols(n)].astype(F32) + z_recv[1, :, cols(n)].astype(F32) + z_recv[2, :, cols(n)].astype(F32)
        o_buf[mine, cols(n)] = (x1_buf[:, cols(n)] + moe).astype(BF16)
        for dz in range(3):
            from_o.append(send(o_buf.at[mine, cols(n)], o_buf.at[mine, cols(n)], slot, {"tp": z_peers[dz]}))
            slot += 1
    for copy in from_o:
        copy.wait_recv()
    out_ref[...] = o_buf[...]
    for copy in sent:
        copy.wait_send()


N_SLOTS = 3 + 3 + 3 + 8 + 4 + COLS * 2 + COLS * 6


def solution(mesh):
    token_rows = P(('dp', 'ep'), None)
    token_vec = P(('dp', 'ep'))
    cache_spec = P(('dp', 'ep'), None, 'tp', None)
    expert_in = P('ep', None, 'tp')
    expert_down = P('ep', 'tp', None)
    vm = pl.BlockSpec(memory_space=pltpu.VMEM)
    anyspace = pl.BlockSpec(memory_space=pl.ANY)

    def device_step(hidden, seq_lens, rope_cos, rope_sin, ln1_scale, ln1_bias, w_qkv, b_qkv, w_out, b_out, k_cache, v_cache, ln2_scale, ln2_bias, w_router, expert_ids, w_gate, w_up, w_down):
        n, d = hidden.shape
        _, s_max, groups, head = k_cache.shape
        feat = groups * head
        n_exp = w_gate.shape[0]
        k_in = k_cache.transpose(0, 2, 3, 1).reshape(n, feat, s_max)
        v_in = v_cache.transpose(0, 2, 3, 1).reshape(n, feat, s_max)
        part, k_out, v_out = pl.pallas_call(
            attention_kernel,
            out_shape=(pltpu.VMEM((n, d), BF16), jax.ShapeDtypeStruct(k_in.shape, BF16), jax.ShapeDtypeStruct(v_in.shape, BF16)),
            in_specs=[anyspace] * 11,
            out_specs=(vm, anyspace, anyspace),
            scratch_shapes=[
                pltpu.SMEM((n,), jnp.int32), pltpu.VMEM((n, d), BF16), pltpu.VMEM((32, n), F32), pltpu.VMEM((32, n), F32),
                pltpu.VMEM((d,), BF16), pltpu.VMEM((d,), BF16), pltpu.VMEM(b_qkv.shape, BF16),
                pltpu.VMEM(k_in.shape, BF16), pltpu.VMEM(v_in.shape, BF16), pltpu.VMEM(w_qkv.shape, BF16), pltpu.VMEM(w_out.shape, BF16),
                pltpu.VMEM((n * 8, 128), F32), pltpu.VMEM((n // BB, 128, 128), F32), pltpu.VMEM((n // BB, 128, 128), F32), pltpu.VMEM((n * 8, 128), F32),
                pltpu.SemaphoreType.DMA((7,)), pltpu.SemaphoreType.DMA((W_PARTS,)), pltpu.SemaphoreType.DMA, pltpu.SemaphoreType.DMA((n // BB,)), pltpu.SemaphoreType.DMA((n // BB,)),
                pltpu.SemaphoreType.DMA((n // BB,)), pltpu.SemaphoreType.DMA((n // BB,)),
            ],
            compiler_params=pltpu.CompilerParams(vmem_limit_bytes=VMEM_LIMIT),
            name="attention",
        )(seq_lens, hidden, rope_cos.T, rope_sin.T, ln1_scale, ln1_bias, b_qkv, w_qkv, w_out, k_in, v_in)
        part = pltpu.with_memory_space_constraint(part, pltpu.VMEM)
        rows = lambda r, t: pltpu.VMEM((r, d), t)
        hidden_out = pl.pallas_call(
            moe_kernel,
            out_shape=pltpu.VMEM((n, d), BF16),
            in_specs=[vm] * 7 + [anyspace] * 3,
            out_specs=vm,
            scratch_shapes=[
                pltpu.VMEM((n_exp, d, 256), BF16), pltpu.VMEM((n_exp * 128, d), BF16), rows(128, BF16),
                pltpu.VMEM((3, 16, d), BF16), rows(16, F32), rows(256, BF16), pltpu.VMEM((4, 8, n), jnp.int32),
                pltpu.VMEM((256, n_exp * 128), BF16), rows(128, F32), rows(128, BF16), rows(128, BF16), rows(64, BF16), rows(64, BF16),
                rows(64, F32), rows(64, BF16), pltpu.VMEM((3, 16, d), BF16), rows(64, BF16),
                pltpu.SemaphoreType.DMA((2 * n_exp + 2,)), pltpu.SemaphoreType.DMA((N_SLOTS,)), pltpu.SemaphoreType.DMA((N_SLOTS,)),
            ],
            compiler_params=pltpu.CompilerParams(vmem_limit_bytes=MOE_LIMIT, collective_id=0, has_side_effects=True),
            name="moe",
        )(hidden, part, b_out, ln2_scale, ln2_bias, w_router.T, expert_ids.T, w_gate, w_up, w_down.reshape(n_exp * 128, d))
        unfold = lambda c: c.reshape(n, groups, head, s_max).transpose(0, 3, 1, 2)
        return hidden_out, unfold(k_out), unfold(v_out)

    in_specs = (token_rows, token_vec, token_rows, token_rows, P(), P(), P(None, 'tp'), P('tp'), P('tp', None), P(), cache_spec, cache_spec, P(), P(), P(), token_rows, expert_in, expert_in, expert_down)
    return jax.shard_map(device_step, mesh=mesh, in_specs=in_specs, out_specs=(token_rows, cache_spec, cache_spec), check_vma=False)
```

```python
import functools

import jax
import jax.numpy as jnp
from jax import lax
from jax.experimental import pallas as pl
from jax.experimental.pallas import tpu as pltpu
from jax.sharding import PartitionSpec as P

EPS = 1e-5
F32 = jnp.float32
BF16 = jnp.bfloat16
MESH = pl.DeviceIdType.MESH
VMEM_LIMIT = 66_400_000
MOE_LIMIT = 64_500_000
NT = (((1,), (1,)), ((), ()))
BB = 8
COLS = 6
PIECE = 8
AHEAD = 3
W_PARTS = 4


def normalize(vals_f32, ln_scale, ln_bias):
    row_mean = jnp.mean(vals_f32, axis=-1, keepdims=True)
    centered = vals_f32 - row_mean
    row_var = jnp.mean(centered * centered, axis=-1, keepdims=True)
    normed = centered * lax.rsqrt(row_var + EPS)
    return (normed * ln_scale + ln_bias).astype(BF16)


def row_of(vec_ref):
    return vec_ref[...].astype(F32)[None, :]


def attention_kernel(lens_hbm, hid_hbm, cos_hbm, sin_hbm, scale_hbm, bias_hbm, bqkv_hbm, wqkv_hbm, wout_hbm, k_hbm, v_hbm,
                     part_ref, ko_hbm, vo_hbm, lens_ref, hid_ref, cos_ref, sin_ref, scale_ref, bias_ref, bqkv_ref,
                     k_buf, v_buf, w_buf, wo_buf, q_buf, kn_buf, vn_buf, c_buf, in_sem, w_sem, wo_sem, k_sem, v_sem, ko_sem, vo_sem):
    n_rows = hid_ref.shape[0]
    n_blocks = n_rows // BB
    s_max = k_buf.shape[2]
    smalls = ((hid_hbm, hid_ref), (scale_hbm, scale_ref), (bias_hbm, bias_ref), (bqkv_hbm, bqkv_ref), (cos_hbm, cos_ref), (sin_hbm, sin_ref),
              (lens_hbm, lens_ref))
    small_copies = [pltpu.make_async_copy(src, dst, in_sem.at[i]) for i, (src, dst) in enumerate(smalls)]
    w_rows = w_buf.shape[0] // W_PARTS
    w_copies = [pltpu.make_async_copy(wqkv_hbm.at[pl.ds(i * w_rows, w_rows)], w_buf.at[pl.ds(i * w_rows, w_rows)], w_sem.at[i]) for i in range(W_PARTS)]
    wo_copy = pltpu.make_async_copy(wout_hbm, wo_buf, wo_sem)
    for copy in small_copies[:3] + w_copies + small_copies[3:]:
        copy.start()

    def fetch(i):
        rows = pl.ds(i * BB, BB)
        return (pltpu.make_async_copy(k_hbm.at[rows], k_buf.at[rows], k_sem.at[i]),
                pltpu.make_async_copy(v_hbm.at[rows], v_buf.at[rows], v_sem.at[i]))

    def flush(i):
        rows = pl.ds(i * BB, BB)
        return (pltpu.make_async_copy(k_buf.at[rows], ko_hbm.at[rows], ko_sem.at[i]),
                pltpu.make_async_copy(v_buf.at[rows], vo_hbm.at[rows], vo_sem.at[i]))

    def fetch_start(i):
        for copy in fetch(i):
            copy.start()

    for i in range(AHEAD):
        fetch_start(i)

    for copy in small_copies:
        copy.wait()
    normed = normalize(hid_ref[...].astype(F32), row_of(scale_ref), row_of(bias_ref))
    for copy in w_copies:
        copy.wait()
    fetch_start(AHEAD)
    qkv = jnp.dot(normed, w_buf[...], preferred_element_type=F32) + row_of(bqkv_ref)
    qkv = qkv.astype(BF16).astype(F32)
    qkv = jnp.concatenate([qkv, jnp.zeros((128 - n_rows, qkv.shape[1]), F32)], axis=0)
    feats = qkv.T
    cos_t = jnp.concatenate([cos_ref[...], jnp.zeros((32, 128 - n_rows), F32)], axis=1)
    sin_t = jnp.concatenate([sin_ref[...], jnp.zeros((32, 128 - n_rows), F32)], axis=1)

    def rotate(base):
        u, w = feats[base:base + 32], feats[base + 32:base + 64]
        return jnp.concatenate([u * cos_t - w * sin_t, w * cos_t + u * sin_t], axis=0).astype(BF16).astype(F32)

    zeros = jnp.zeros((64, 128), F32)
    for g in range(2):
        for j in range(3):
            q_rot = rotate(g * 320 + j * 64)
            both = jnp.concatenate([q_rot, zeros] if g == 0 else [zeros, q_rot], axis=0)
            q_buf[pl.ds(g * 3 + j, n_rows, stride=8), :] = both.T[:n_rows]
    for r in (6, 7):
        q_buf[pl.ds(r, n_rows, stride=8), :] = jnp.zeros((n_rows, 128), F32)
    k_new = jnp.concatenate([rotate(192), rotate(320 + 192)], axis=0)
    v_new = jnp.concatenate([feats[256:320], feats[320 + 256:320 + 320]], axis=0)
    for i in range(n_blocks):
        kn_buf[i] = k_new if i == 0 else pltpu.roll(k_new, 128 - i * BB, 1)
        vn_buf[i] = v_new if i == 0 else pltpu.roll(v_new, 128 - i * BB, 1)

    def block(i, carry):
        for copy in fetch(i):
            copy.wait()

        @pl.when(i + AHEAD + 1 < n_blocks)
        def _():
            fetch_start(i + AHEAD + 1)

        @pl.when(i == n_blocks - AHEAD - 1)
        def _():
            wo_copy.start()

        k_cols, v_cols = kn_buf[i], vn_buf[i]
        lane = lax.broadcasted_iota(jnp.int32, (128, 128), 1)
        position = lax.broadcasted_iota(jnp.int32, (8, s_max), 1)
        scores = []
        for j in range(BB):
            b = i * BB + j
            pos = lens_ref[b]
            first = pl.multiple_of((pos // 128) * 128, 128)
            hit = lane == pos - first
            window = pl.ds(first, 128)
            k_buf[b, :, window] = jnp.where(hit, k_cols[:, j:j + 1], k_buf[b, :, window].astype(F32)).astype(BF16)
            v_buf[b, :, window] = jnp.where(hit, v_cols[:, j:j + 1], v_buf[b, :, window].astype(F32)).astype(BF16)
            rows = pl.ds(pl.multiple_of(b * 8, 8), 8)
            one = jnp.dot(q_buf[rows, :].astype(BF16), k_buf[b], preferred_element_type=F32) * 0.125
            scores.append(jnp.where(position <= pos, one, -jnp.inf))
        scores = jnp.concatenate(scores, axis=0)
        top = jnp.max(scores, axis=1, keepdims=True)
        weights = jnp.exp(scores - top)
        probs = weights * (1.0 / jnp.sum(weights, axis=1, keepdims=True))
        for j in range(BB):
            b = i * BB + j
            rows = pl.ds(pl.multiple_of(b * 8, 8), 8)
            c_buf[rows, :] = lax.dot_general(probs[j * 8:j * 8 + 8].astype(BF16), v_buf[b], NT, preferred_element_type=F32)
        for copy in flush(i):
            copy.start()
        return carry

    lax.fori_loop(0, n_blocks, block, 0)
    heads = [c_buf[pl.ds(r, n_rows, stride=8), :] for r in range(6)]
    low = lax.broadcasted_iota(jnp.int32, (n_rows, 128), 1) < 64
    ctx = jnp.concatenate([
        jnp.where(low, heads[0], pltpu.roll(heads[1], 64, 1)),
        jnp.where(low, heads[2], heads[3]),
        jnp.where(low, pltpu.roll(heads[4], 64, 1), heads[5]),
    ], axis=1).astype(BF16)
    wo_copy.wait()
    part_ref[...] = jnp.dot(ctx, wo_buf[...], preferred_element_type=F32).astype(BF16)
    for i in range(n_blocks):
        for copy in flush(i):
            copy.wait()


def moe_kernel(hid_ref, part_ref, bout_ref, scale_ref, bias_ref, wr_ref, ids_ref, wg_hbm, wu_hbm, wd_hbm, out_ref,
               wgu, wd, wr, rs_recv, x1, h2, ids_buf, act, own_p, y_p, hi0, hi1, d0, d1, y_send, y_recv,
               t_part, t_end, t_pair, t_across, o_buf, wsem, ssem, rsem):
    z, ep = lax.axis_index("tp"), lax.axis_index("ep")
    n_rows, d_model = hid_ref.shape
    n_exp = wgu.shape[0]
    width = d_model // COLS
    z_peers = [lax.rem(z + dz, 4) for dz in (1, 2, 3)]
    near, across = z + 1 - 2 * lax.rem(z, 2), 3 - z
    y_peer = lax.rem(ep + 2, 4)
    partner = ep + 1 - 2 * lax.rem(ep, 2)
    diagonal = 3 - ep
    is_mid = jnp.logical_or(z == 1, z == 2)
    is_end = jnp.logical_or(z == 0, z == 3)
    barrier = pltpu.get_barrier_semaphore()
    for peer in z_peers:
        pl.semaphore_signal(barrier, inc=1, device_id={"tp": peer}, device_id_type=MESH)
    for peer in (y_peer, partner, diagonal):
        pl.semaphore_signal(barrier, inc=1, device_id={"ep": peer}, device_id_type=MESH)

    loads = []
    for e in range(n_exp):
        loads.append(pltpu.make_async_copy(wg_hbm.at[e], wgu.at[e, :, 0:128], wsem.at[2 * e]))
        loads.append(pltpu.make_async_copy(wu_hbm.at[e], wgu.at[e, :, 128:256], wsem.at[2 * e + 1]))
    loads.append(pltpu.make_async_copy(wd_hbm, wd, wsem.at[2 * n_exp]))
    for load in loads:
        load.start()

    count = [0]

    def remote(src, dst, device):
        slot = count[0]
        count[0] += 1
        return pltpu.make_async_remote_copy(src_ref=src, dst_ref=dst, send_sem=ssem.at[slot], recv_sem=rsem.at[slot],
                                            device_id=device, device_id_type=MESH)

    def at(index, h, shard=0):
        return pl.ds(pl.multiple_of(shard * n_rows + index * 16 + h * PIECE, PIECE), PIECE)

    def cols(n):
        return pl.ds(n * width, width)

    halves = range(16 // PIECE)
    z_order = [z] + [lax.rem(z + 4 - dz, 4) for dz in (1, 2, 3)]
    rs = [[remote(part_ref.at[at(z_peers[dz], h)], rs_recv.at[dz, pl.ds(h * PIECE, PIECE)], {"tp": z_peers[dz]}) for dz in range(3)] for h in halves]
    to_z = [[remote(h2.at[at(z, h)], h2.at[at(z, h)], {"tp": z_peers[dz]}) for dz in range(3)] for h in halves]
    to_p = [[remote(h2.at[at(z_order[k], h)], h2.at[at(z_order[k], h, 1)], {"ep": partner}) for k in range(4)] for h in halves]
    to_y = [[remote(h2.at[at(z_order[k], h)], h2.at[at(z_order[k], h, 2)], {"ep": y_peer}) for k in range(4)] for h in halves]
    y_to_p = [[remote(h2.at[at(z_order[k], h, 2)], h2.at[at(z_order[k], h, 3)], {"ep": partner}) for k in range(4)] for h in halves]
    mine = pl.ds(pl.multiple_of(z * 16, 16), 16)
    x1_z = [remote(x1.at[mine], x1.at[mine], {"tp": z_peers[dz]}) for dz in range(3)]
    to_ids = [remote(ids_ref, ids_buf.at[i + 1], {"ep": peer}) for i, peer in enumerate((partner, y_peer, diagonal))]
    chunks = range(COLS)
    to_d0 = remote(hi0, d0, {"ep": partner})
    to_d = [remote(hi1.at[:, cols(n)], d1.at[:, cols(n)], {"ep": partner}) for n in chunks]
    to_yy = [remote(y_send.at[:, cols(n)], y_recv.at[:, cols(n)], {"ep": y_peer}) for n in chunks]
    to_mid = [remote(t_part.at[:, cols(n)], t_end.at[:, cols(n)], {"tp": near}) for n in chunks]
    to_mate = [remote(t_pair.at[:, cols(n)], t_across.at[:, cols(n)], {"tp": across}) for n in chunks]
    to_end = [remote(o_buf.at[:, cols(n)], o_buf.at[:, cols(n)], {"tp": near}) for n in chunks]

    scale, bias, bout = row_of(scale_ref), row_of(bias_ref), row_of(bout_ref)
    ids_buf[0] = ids_ref[...]
    wr[...] = jnp.concatenate([wr_ref[...], jnp.zeros((128 - wr_ref.shape[0], d_model), BF16)], axis=0)
    pl.semaphore_wait(barrier, 6)

    for h in halves:
        for dz in range(3):
            rs[h][dz].start()
    for copy in to_ids:
        copy.start()
    for h in halves:
        for dz in range(3):
            rs[h][dz].wait_recv()
        got = pl.ds(h * PIECE, PIECE)
        total = part_ref[at(z, h), :].astype(F32) + rs_recv[0, got].astype(F32) + rs_recv[1, got].astype(F32) + rs_recv[2, got].astype(F32)
        row = (hid_ref[at(z, h), :].astype(F32) + total + bout).astype(BF16)
        x1[at(z, h), :] = row
        h2[at(z, h), :] = normalize(row.astype(F32), scale, bias)
        for dz in range(3):
            to_z[h][dz].start()
        to_y[h][0].start()
        to_p[h][0].start()
    for copy in x1_z:
        copy.start()

    def relay(h, k):
        to_y[h][k].wait_recv()
        y_to_p[h][k].start()

    for h in halves:
        for dz in range(3):
            to_z[h][dz].wait_recv()
            to_y[h][dz + 1].start()
            to_p[h][dz + 1].start()
        relay(h, 0)

    def masks(shard):
        picks = ids_buf[shard]
        expert = lax.broadcasted_iota(jnp.int32, (128, n_rows), 0)
        hit = jnp.zeros((128, n_rows), F32)
        for k in range(picks.shape[0]):
            hit = jnp.where(expert == picks[k:k + 1, :], 1.0, hit)
        return hit.T

    def toks(shard):
        return h2[shard * n_rows:(shard + 1) * n_rows, :]

    def gates_of(shard):
        logits = lax.dot_general(toks(shard), wr[...], NT, preferred_element_type=F32)
        logits = jnp.where(masks(shard) > 0.5, logits, -jnp.inf)
        shifted = jnp.exp(logits - jnp.max(logits, axis=1, keepdims=True))
        gates = (shifted / jnp.sum(shifted, axis=1, keepdims=True)).astype(BF16).astype(F32)
        return pltpu.roll(gates, lax.rem(128 - ep * n_exp, 128), 1)

    def up(shard, gates, first, last):
        rows = toks(shard)
        for e in range(first, last):
            if shard == 0:
                loads[2 * e].wait()
                loads[2 * e + 1].wait()
            pre = jnp.dot(rows, wgu[e], preferred_element_type=F32)
            gate_pre, up_pre = pre[:, :128], pre[:, 128:]
            hidden = (gate_pre * jax.nn.sigmoid(gate_pre) * up_pre).astype(BF16).astype(F32)
            act[shard * n_rows:(shard + 1) * n_rows, e * 128:(e + 1) * 128] = (hidden * gates[:, e:e + 1]).astype(BF16)

    for copy in to_ids:
        copy.wait_recv()
    gates = gates_of(0)
    split = n_exp // len(halves)
    for h in halves:
        up(0, gates, h * split, (h + 1) * split)
        for k in (1, 2, 3):
            relay(h, k)
    for h in halves:
        for copy in to_p[h]:
            copy.wait_recv()
    up(1, gates_of(1), 0, n_exp)
    loads[-1].wait()
    for n in range(3):
        third = pl.ds(n * 512, 512)
        both = jnp.dot(act[0:128, :], wd[:, third], preferred_element_type=F32)
        own_p[:, third] = both[0:64]
        hi0[:, third] = both[64:128].astype(BF16)
    to_d0.start()
    up(2, gates_of(2), 0, n_exp)
    for h in halves:
        for copy in y_to_p[h]:
            copy.wait_recv()
    up(3, gates_of(3), 0, n_exp)

    def reduce_pair(n):
        to_d[n].wait_recv()
        y_send[:, cols(n)] = (y_p[:, cols(n)] + d1[:, cols(n)].astype(F32)).astype(BF16)
        to_yy[n].start()

    for n in chunks:
        both = jnp.dot(act[128:256, :], wd[:, cols(n)], preferred_element_type=F32)
        y_p[:, cols(n)] = both[0:64]
        hi1[:, cols(n)] = both[64:128].astype(BF16)
        to_d[n].start()
    to_d0.wait_recv()
    for n in chunks:
        reduce_pair(n)
    for copy in x1_z:
        copy.wait_recv()

    def own_sum(n):
        to_yy[n].wait_recv()
        return own_p[:, cols(n)] + d0[:, cols(n)].astype(F32) + y_recv[:, cols(n)].astype(F32)

    @pl.when(is_end)
    def _():
        for n in chunks:
            t_part[:, cols(n)] = own_sum(n).astype(BF16)
            to_mid[n].start()
        for n in chunks:
            to_end[n].wait_recv()

    @pl.when(is_mid)
    def _():
        for n in chunks:
            part_sum = own_sum(n)
            to_mid[n].wait_recv()
            t_pair[:, cols(n)] = (part_sum + t_end[:, cols(n)].astype(F32)).astype(BF16)
            to_mate[n].start()
        for n in chunks:
            to_mate[n].wait_recv()
            moe = t_pair[:, cols(n)].astype(F32) + t_across[:, cols(n)].astype(F32)
            o_buf[:, cols(n)] = (x1[:, cols(n)].astype(F32) + moe).astype(BF16)
            to_end[n].start()

    out_ref[...] = o_buf[...]
    for group in rs + to_z + to_p + to_y + y_to_p + [x1_z, to_ids, [to_d0], to_d, to_yy]:
        for copy in group:
            copy.wait_send()

    @pl.when(is_end)
    def _():
        for copy in to_mid:
            copy.wait_send()

    @pl.when(is_mid)
    def _():
        for copy in to_mate + to_end:
            copy.wait_send()


N_SLOTS = (16 // PIECE) * 18 + 3 + 3 + 1 + 5 * COLS


def solution(mesh):
    token_rows = P(('dp', 'ep'), None)
    token_vec = P(('dp', 'ep'))
    cache_spec = P(('dp', 'ep'), None, 'tp', None)
    expert_in = P('ep', None, 'tp')
    expert_down = P('ep', 'tp', None)
    vm = pl.BlockSpec(memory_space=pltpu.VMEM)
    anyspace = pl.BlockSpec(memory_space=pl.ANY)

    def device_step(hidden, seq_lens, rope_cos, rope_sin, ln1_scale, ln1_bias, w_qkv, b_qkv, w_out, b_out, k_cache, v_cache, ln2_scale, ln2_bias, w_router, expert_ids, w_gate, w_up, w_down):
        n, d = hidden.shape
        _, s_max, groups, head = k_cache.shape
        feat = groups * head
        n_exp = w_gate.shape[0]
        k_in = k_cache.transpose(0, 2, 3, 1).reshape(n, feat, s_max)
        v_in = v_cache.transpose(0, 2, 3, 1).reshape(n, feat, s_max)
        part, k_out, v_out = pl.pallas_call(
            attention_kernel,
            out_shape=(pltpu.VMEM((n, d), BF16), jax.ShapeDtypeStruct(k_in.shape, BF16), jax.ShapeDtypeStruct(v_in.shape, BF16)),
            in_specs=[anyspace] * 11,
            out_specs=(vm, anyspace, anyspace),
            scratch_shapes=[
                pltpu.SMEM((n,), jnp.int32), pltpu.VMEM((n, d), BF16), pltpu.VMEM((32, n), F32), pltpu.VMEM((32, n), F32),
                pltpu.VMEM((d,), BF16), pltpu.VMEM((d,), BF16), pltpu.VMEM(b_qkv.shape, BF16),
                pltpu.VMEM(k_in.shape, BF16), pltpu.VMEM(v_in.shape, BF16), pltpu.VMEM(w_qkv.shape, BF16), pltpu.VMEM(w_out.shape, BF16),
                pltpu.VMEM((n * 8, 128), F32), pltpu.VMEM((n // BB, 128, 128), F32), pltpu.VMEM((n // BB, 128, 128), F32), pltpu.VMEM((n * 8, 128), F32),
                pltpu.SemaphoreType.DMA((7,)), pltpu.SemaphoreType.DMA((W_PARTS,)), pltpu.SemaphoreType.DMA, pltpu.SemaphoreType.DMA((n // BB,)), pltpu.SemaphoreType.DMA((n // BB,)),
                pltpu.SemaphoreType.DMA((n // BB,)), pltpu.SemaphoreType.DMA((n // BB,)),
            ],
            compiler_params=pltpu.CompilerParams(vmem_limit_bytes=VMEM_LIMIT),
            name="attention",
        )(seq_lens, hidden, rope_cos.T, rope_sin.T, ln1_scale, ln1_bias, b_qkv, w_qkv, w_out, k_in, v_in)
        part = pltpu.with_memory_space_constraint(part, pltpu.VMEM)
        rows = lambda r, t: pltpu.VMEM((r, d), t)
        hidden_out = pl.pallas_call(
            moe_kernel,
            out_shape=pltpu.VMEM((n, d), BF16),
            in_specs=[vm] * 7 + [anyspace] * 3,
            out_specs=vm,
            scratch_shapes=[
                pltpu.VMEM((n_exp, d, 256), BF16), pltpu.VMEM((n_exp * 128, d), BF16), rows(128, BF16),
                pltpu.VMEM((3, 16, d), BF16), rows(64, BF16), rows(256, BF16), pltpu.VMEM((4, 8, n), jnp.int32),
                pltpu.VMEM((256, n_exp * 128), BF16), rows(64, F32), rows(64, F32), rows(64, BF16), rows(64, BF16), rows(64, BF16), rows(64, BF16),
                rows(64, BF16), rows(64, BF16), rows(64, BF16), rows(64, BF16), rows(64, BF16), rows(64, BF16), rows(64, BF16),
                pltpu.SemaphoreType.DMA((2 * n_exp + 1,)), pltpu.SemaphoreType.DMA((N_SLOTS,)), pltpu.SemaphoreType.DMA((N_SLOTS,)),
            ],
            compiler_params=pltpu.CompilerParams(vmem_limit_bytes=MOE_LIMIT, collective_id=0, has_side_effects=True),
            name="moe",
        )(hidden, part, b_out, ln2_scale, ln2_bias, w_router.T, expert_ids.T, w_gate, w_up, w_down.reshape(n_exp * 128, d))
        unfold = lambda c: c.reshape(n, groups, head, s_max).transpose(0, 3, 1, 2)
        return hidden_out, unfold(k_out), unfold(v_out)

    in_specs = (token_rows, token_vec, token_rows, token_rows, P(), P(), P(None, 'tp'), P('tp'), P('tp', None), P(), cache_spec, cache_spec, P(), P(), P(), token_rows, expert_in, expert_in, expert_down)
    return jax.shard_map(device_step, mesh=mesh, in_specs=in_specs, out_specs=(token_rows, cache_spec, cache_spec), check_vma=False)
```

```python
import functools

import jax
import jax.numpy as jnp
from jax import lax
from jax.experimental import pallas as pl
from jax.experimental.pallas import tpu as pltpu
from jax.sharding import PartitionSpec as P

EPS = 1e-5
F32 = jnp.float32
BF16 = jnp.bfloat16
MESH = pl.DeviceIdType.MESH
VMEM_LIMIT = 66_400_000
MOE_LIMIT = 40_000_000
NT = (((1,), (1,)), ((), ()))
BB = 4
COLS = 3
PIECE = 16
AHEAD = 6
W_PARTS = 4


def normalize(vals_f32, ln_scale, ln_bias):
    row_mean = jnp.mean(vals_f32, axis=-1, keepdims=True)
    centered = vals_f32 - row_mean
    row_var = jnp.mean(centered * centered, axis=-1, keepdims=True)
    normed = centered * lax.rsqrt(row_var + EPS)
    return (normed * ln_scale + ln_bias).astype(BF16)


def row_of(vec_ref):
    return vec_ref[...].astype(F32)[None, :]


def attention_kernel(lens_hbm, hid_hbm, cos_hbm, sin_hbm, scale_hbm, bias_hbm, bqkv_hbm, wqkv_hbm, wout_hbm, k_hbm, v_hbm,
                     part_ref, ko_hbm, vo_hbm, lens_ref, hid_ref, cos_ref, sin_ref, scale_ref, bias_ref, bqkv_ref,
                     k_buf, v_buf, w_buf, wo_buf, q_buf, kn_buf, vn_buf, c_buf, in_sem, w_sem, wo_sem, k_sem, v_sem, ko_sem, vo_sem):
    n_rows = hid_ref.shape[0]
    n_blocks = n_rows // BB
    s_max = k_buf.shape[2]
    smalls = ((hid_hbm, hid_ref), (scale_hbm, scale_ref), (bias_hbm, bias_ref), (bqkv_hbm, bqkv_ref), (cos_hbm, cos_ref), (sin_hbm, sin_ref),
              (lens_hbm, lens_ref))
    small_copies = [pltpu.make_async_copy(src, dst, in_sem.at[i]) for i, (src, dst) in enumerate(smalls)]
    w_rows = w_buf.shape[0] // W_PARTS
    w_copies = [pltpu.make_async_copy(wqkv_hbm.at[pl.ds(i * w_rows, w_rows)], w_buf.at[pl.ds(i * w_rows, w_rows)], w_sem.at[i]) for i in range(W_PARTS)]
    wo_copy = pltpu.make_async_copy(wout_hbm, wo_buf, wo_sem)
    for copy in small_copies[:3] + w_copies + small_copies[3:]:
        copy.start()

    def fetch(i):
        rows = pl.ds(i * BB, BB)
        return (pltpu.make_async_copy(k_hbm.at[rows], k_buf.at[rows], k_sem.at[i]),
                pltpu.make_async_copy(v_hbm.at[rows], v_buf.at[rows], v_sem.at[i]))

    def flush(i):
        rows = pl.ds(i * BB, BB)
        return (pltpu.make_async_copy(k_buf.at[rows], ko_hbm.at[rows], ko_sem.at[i]),
                pltpu.make_async_copy(v_buf.at[rows], vo_hbm.at[rows], vo_sem.at[i]))

    def fetch_start(i):
        for copy in fetch(i):
            copy.start()

    for i in range(AHEAD):
        fetch_start(i)

    for copy in small_copies:
        copy.wait()
    normed = normalize(hid_ref[...].astype(F32), row_of(scale_ref), row_of(bias_ref))
    for copy in w_copies:
        copy.wait()
    fetch_start(AHEAD)
    qkv = jnp.dot(normed, w_buf[...], preferred_element_type=F32) + row_of(bqkv_ref)
    qkv = qkv.astype(BF16).astype(F32)
    qkv = jnp.concatenate([qkv, jnp.zeros((128 - n_rows, qkv.shape[1]), F32)], axis=0)
    feats = qkv.T
    cos_t = jnp.concatenate([cos_ref[...], jnp.zeros((32, 128 - n_rows), F32)], axis=1)
    sin_t = jnp.concatenate([sin_ref[...], jnp.zeros((32, 128 - n_rows), F32)], axis=1)

    def rotate(base):
        u, w = feats[base:base + 32], feats[base + 32:base + 64]
        return jnp.concatenate([u * cos_t - w * sin_t, w * cos_t + u * sin_t], axis=0).astype(BF16).astype(F32)

    zeros = jnp.zeros((64, 128), F32)
    for g in range(2):
        for j in range(3):
            q_rot = rotate(g * 320 + j * 64)
            both = jnp.concatenate([q_rot, zeros] if g == 0 else [zeros, q_rot], axis=0)
            q_buf[pl.ds(g * 3 + j, n_rows, stride=8), :] = both.T[:n_rows]
    for r in (6, 7):
        q_buf[pl.ds(r, n_rows, stride=8), :] = jnp.zeros((n_rows, 128), F32)
    k_new = jnp.concatenate([rotate(192), rotate(320 + 192)], axis=0)
    v_new = jnp.concatenate([feats[256:320], feats[320 + 256:320 + 320]], axis=0)
    for i in range(n_blocks):
        kn_buf[i] = k_new if i == 0 else pltpu.roll(k_new, 128 - i * BB, 1)
        vn_buf[i] = v_new if i == 0 else pltpu.roll(v_new, 128 - i * BB, 1)

    def block(i, carry):
        for copy in fetch(i):
            copy.wait()

        @pl.when(i + AHEAD + 1 < n_blocks)
        def _():
            fetch_start(i + AHEAD + 1)

        @pl.when(i == n_blocks - AHEAD - 1)
        def _():
            wo_copy.start()

        k_cols, v_cols = kn_buf[i], vn_buf[i]
        lane = lax.broadcasted_iota(jnp.int32, (128, 128), 1)
        position = lax.broadcasted_iota(jnp.int32, (8, s_max), 1)
        scores = []
        for j in range(BB):
            b = i * BB + j
            pos = lens_ref[b]
            first = pl.multiple_of((pos // 128) * 128, 128)
            hit = lane == pos - first
            window = pl.ds(first, 128)
            k_buf[b, :, window] = jnp.where(hit, k_cols[:, j:j + 1], k_buf[b, :, window].astype(F32)).astype(BF16)
            v_buf[b, :, window] = jnp.where(hit, v_cols[:, j:j + 1], v_buf[b, :, window].astype(F32)).astype(BF16)
            rows = pl.ds(pl.multiple_of(b * 8, 8), 8)
            one = jnp.dot(q_buf[rows, :].astype(BF16), k_buf[b], preferred_element_type=F32) * 0.125
            scores.append(jnp.where(position <= pos, one, -jnp.inf))
        scores = jnp.concatenate(scores, axis=0)
        top = jnp.max(scores, axis=1, keepdims=True)
        weights = jnp.exp(scores - top)
        probs = weights * (1.0 / jnp.sum(weights, axis=1, keepdims=True))
        for j in range(BB):
            b = i * BB + j
            rows = pl.ds(pl.multiple_of(b * 8, 8), 8)
            c_buf[rows, :] = lax.dot_general(probs[j * 8:j * 8 + 8].astype(BF16), v_buf[b], NT, preferred_element_type=F32)
        for copy in flush(i):
            copy.start()
        return carry

    lax.fori_loop(0, n_blocks, block, 0)
    heads = [c_buf[pl.ds(r, n_rows, stride=8), :] for r in range(6)]
    low = lax.broadcasted_iota(jnp.int32, (n_rows, 128), 1) < 64
    ctx = jnp.concatenate([
        jnp.where(low, heads[0], pltpu.roll(heads[1], 64, 1)),
        jnp.where(low, heads[2], heads[3]),
        jnp.where(low, pltpu.roll(heads[4], 64, 1), heads[5]),
    ], axis=1).astype(BF16)
    wo_copy.wait()
    part_ref[...] = jnp.dot(ctx, wo_buf[...], preferred_element_type=F32).astype(BF16)
    for i in range(n_blocks):
        for copy in flush(i):
            copy.wait()


def moe_kernel(hid_ref, part_ref, bout_ref, scale_ref, bias_ref, wr_ref, ids_ref, wg_hbm, wu_hbm, wd_hbm, out_ref,
               wgu, wd, wr, rs_recv, x1, h2, ids_buf, act, own_p, y_p, hi0, hi1, d0, d1, y_send, y_recv,
               t_f, t_b, z_recv, o_buf, wsem, ssem, rsem):
    z, ep = lax.axis_index("tp"), lax.axis_index("ep")
    n_rows, d_model = hid_ref.shape
    n_exp = wgu.shape[0]
    width = d_model // COLS
    z_peers = [lax.rem(z + dz, 4) for dz in (1, 2, 3)]
    y_peer = lax.rem(ep + 2, 4)
    partner = ep + 1 - 2 * lax.rem(ep, 2)
    diagonal = 3 - ep
    barrier = pltpu.get_barrier_semaphore()
    for peer in z_peers:
        pl.semaphore_signal(barrier, inc=1, device_id={"tp": peer}, device_id_type=MESH)
    for peer in (y_peer, partner, diagonal):
        pl.semaphore_signal(barrier, inc=1, device_id={"ep": peer}, device_id_type=MESH)

    loads = []
    for e in range(n_exp):
        loads.append(pltpu.make_async_copy(wg_hbm.at[e], wgu.at[e, :, 0:128], wsem.at[2 * e]))
        loads.append(pltpu.make_async_copy(wu_hbm.at[e], wgu.at[e, :, 128:256], wsem.at[2 * e + 1]))
    loads.append(pltpu.make_async_copy(wd_hbm, wd, wsem.at[2 * n_exp]))
    for load in loads:
        load.start()

    count = [0]

    def remote(src, dst, device):
        slot = count[0]
        count[0] += 1
        return pltpu.make_async_remote_copy(src_ref=src, dst_ref=dst, send_sem=ssem.at[slot], recv_sem=rsem.at[slot],
                                            device_id=device, device_id_type=MESH)

    def at(index, h, shard=0):
        return pl.ds(pl.multiple_of(shard * n_rows + index * 16 + h * PIECE, PIECE), PIECE)

    def rows_at(index):
        return pl.ds(pl.multiple_of(index * 16, 16), 16)

    def cols(n):
        return pl.ds(n * width, width)

    halves = range(16 // PIECE)
    z_order = [z] + [lax.rem(z + 4 - dz, 4) for dz in (1, 2, 3)]
    rs = [[remote(part_ref.at[at(z_peers[dz], h)], rs_recv.at[dz, pl.ds(h * PIECE, PIECE)], {"tp": z_peers[dz]}) for dz in range(3)] for h in halves]
    to_z = [[remote(h2.at[at(z, h)], h2.at[at(z, h)], {"tp": z_peers[dz]}) for dz in range(3)] for h in halves]
    to_p = [[remote(h2.at[at(z_order[k], h)], h2.at[at(z_order[k], h, 1)], {"ep": partner}) for k in range(4)] for h in halves]
    to_y = [[remote(h2.at[at(z_order[k], h)], h2.at[at(z_order[k], h, 2)], {"ep": y_peer}) for k in range(4)] for h in halves]
    y_to_p = [[remote(h2.at[at(z_order[k], h, 2)], h2.at[at(z_order[k], h, 3)], {"ep": partner}) for k in range(4)] for h in halves]
    mine = rows_at(z)
    to_ids = [remote(ids_ref, ids_buf.at[i + 1], {"ep": peer}) for i, peer in enumerate((partner, y_peer, diagonal))]
    chunks = range(COLS)
    to_d0 = [remote(hi0.at[n], d0.at[n], {"ep": partner}) for n in chunks]
    to_d = [remote(hi1.at[n], d1.at[n], {"ep": partner}) for n in chunks]
    to_yy = [remote(y_send.at[n], y_recv.at[n], {"ep": y_peer}) for n in chunks]
    to_zz = [[remote(t_b.at[n, rows_at(z_peers[dz])], z_recv.at[n, dz], {"tp": z_peers[dz]}) for dz in range(3)] for n in chunks]
    to_o = [[remote(o_buf.at[n, mine], o_buf.at[n, mine], {"tp": z_peers[dz]}) for dz in range(3)] for n in chunks]

    scale, bias, bout = row_of(scale_ref), row_of(bias_ref), row_of(bout_ref)
    ids_buf[0] = ids_ref[...]
    wr[...] = jnp.concatenate([wr_ref[...], jnp.zeros((128 - wr_ref.shape[0], d_model), BF16)], axis=0)
    pl.semaphore_wait(barrier, 6)

    for h in halves:
        for dz in range(3):
            rs[h][dz].start()
    for copy in to_ids:
        copy.start()
    for h in halves:
        for dz in range(3):
            rs[h][dz].wait_recv()
        got = pl.ds(h * PIECE, PIECE)
        total = part_ref[at(z, h), :].astype(F32) + rs_recv[0, got].astype(F32) + rs_recv[1, got].astype(F32) + rs_recv[2, got].astype(F32)
        row = (hid_ref[at(z, h), :].astype(F32) + total + bout).astype(BF16)
        x1[got, :] = row.astype(F32)
        h2[at(z, h), :] = normalize(row.astype(F32), scale, bias)
        for dz in range(3):
            to_z[h][dz].start()
        to_y[h][0].start()
        to_p[h][0].start()

    def relay(h, k):
        to_y[h][k].wait_recv()
        y_to_p[h][k].start()

    for h in halves:
        for dz in range(3):
            to_z[h][dz].wait_recv()
            to_y[h][dz + 1].start()
            to_p[h][dz + 1].start()
        relay(h, 0)

    def masks(shard):
        picks = ids_buf[shard]
        expert = lax.broadcasted_iota(jnp.int32, (128, n_rows), 0)
        hit = jnp.zeros((128, n_rows), F32)
        for k in range(picks.shape[0]):
            hit = jnp.where(expert == picks[k:k + 1, :], 1.0, hit)
        return hit.T

    def toks(shard):
        return h2[shard * n_rows:(shard + 1) * n_rows, :]

    def gates_of(shard):
        logits = lax.dot_general(toks(shard), wr[...], NT, preferred_element_type=F32)
        logits = jnp.where(masks(shard) > 0.5, logits, -jnp.inf)
        shifted = jnp.exp(logits - jnp.max(logits, axis=1, keepdims=True))
        gates = (shifted / jnp.sum(shifted, axis=1, keepdims=True)).astype(BF16).astype(F32)
        return pltpu.roll(gates, lax.rem(128 - ep * n_exp, 128), 1)

    def up(shard, gates, first, last):
        rows = toks(shard)
        for e in range(first, last):
            if shard == 0:
                loads[2 * e].wait()
                loads[2 * e + 1].wait()
            pre = jnp.dot(rows, wgu[e], preferred_element_type=F32)
            gate_pre, up_pre = pre[:, :128], pre[:, 128:]
            hidden = (gate_pre * jax.nn.sigmoid(gate_pre) * up_pre).astype(BF16).astype(F32)
            act[shard * n_rows:(shard + 1) * n_rows, e * 128:(e + 1) * 128] = (hidden * gates[:, e:e + 1]).astype(BF16)

    for copy in to_ids:
        copy.wait_recv()
    up(0, gates_of(0), 0, n_exp)
    for h in halves:
        for k in (1, 2, 3):
            relay(h, k)
    for h in halves:
        for copy in to_p[h]:
            copy.wait_recv()
    up(1, gates_of(1), 0, n_exp)
    up(2, gates_of(2), 0, n_exp)
    for h in halves:
        for copy in y_to_p[h]:
            copy.wait_recv()
    up(3, gates_of(3), 0, n_exp)
    loads[-1].wait()

    def reduce_pair(n):
        to_d[n].wait_recv()
        y_send[n] = (y_p[n] + d1[n].astype(F32)).astype(BF16)
        to_yy[n].start()

    for n in chunks:
        both = jnp.dot(act[128:256, :], wd[:, cols(n)], preferred_element_type=F32)
        y_p[n] = both[0:64]
        hi1[n] = both[64:128].astype(BF16)
        to_d[n].start()
        if n > 0:
            reduce_pair(n - 1)
        both = jnp.dot(act[0:128, :], wd[:, cols(n)], preferred_element_type=F32)
        own_p[n] = both[0:64]
        hi0[n] = both[64:128].astype(BF16)
        to_d0[n].start()
    reduce_pair(COLS - 1)
    for n in chunks:
        to_d0[n].wait_recv()
        to_yy[n].wait_recv()
        t = own_p[n] + d0[n].astype(F32) + y_recv[n].astype(F32)
        t_f[n] = t
        t_b[n] = t.astype(BF16)
        for copy in to_zz[n]:
            copy.start()
    for n in chunks:
        for copy in to_zz[n]:
            copy.wait_recv()
        moe = t_f[n, mine, :] + z_recv[n, 0].astype(F32) + z_recv[n, 1].astype(F32) + z_recv[n, 2].astype(F32)
        o_buf[n, mine, :] = (x1[:, cols(n)] + moe).astype(BF16)
        for copy in to_o[n]:
            copy.start()
    for n in chunks:
        for copy in to_o[n]:
            copy.wait_recv()
        out_ref[:, cols(n)] = o_buf[n]
    for group in rs + to_z + to_p + to_y + y_to_p + [to_ids, to_d0, to_d, to_yy] + to_zz + to_o:
        for copy in group:
            copy.wait_send()


N_SLOTS = (16 // PIECE) * 18 + 3 + 9 * COLS


def solution(mesh):
    token_rows = P(('dp', 'ep'), None)
    token_vec = P(('dp', 'ep'))
    cache_spec = P(('dp', 'ep'), None, 'tp', None)
    expert_in = P('ep', None, 'tp')
    expert_down = P('ep', 'tp', None)
    vm = pl.BlockSpec(memory_space=pltpu.VMEM)
    anyspace = pl.BlockSpec(memory_space=pl.ANY)

    def device_step(hidden, seq_lens, rope_cos, rope_sin, ln1_scale, ln1_bias, w_qkv, b_qkv, w_out, b_out, k_cache, v_cache, ln2_scale, ln2_bias, w_router, expert_ids, w_gate, w_up, w_down):
        n, d = hidden.shape
        _, s_max, groups, head = k_cache.shape
        feat = groups * head
        n_exp = w_gate.shape[0]
        k_in = k_cache.transpose(0, 2, 3, 1).reshape(n, feat, s_max)
        v_in = v_cache.transpose(0, 2, 3, 1).reshape(n, feat, s_max)
        part, k_out, v_out = pl.pallas_call(
            attention_kernel,
            out_shape=(pltpu.VMEM((n, d), BF16), jax.ShapeDtypeStruct(k_in.shape, BF16), jax.ShapeDtypeStruct(v_in.shape, BF16)),
            in_specs=[anyspace] * 11,
            out_specs=(vm, anyspace, anyspace),
            scratch_shapes=[
                pltpu.SMEM((n,), jnp.int32), pltpu.VMEM((n, d), BF16), pltpu.VMEM((32, n), F32), pltpu.VMEM((32, n), F32),
                pltpu.VMEM((d,), BF16), pltpu.VMEM((d,), BF16), pltpu.VMEM(b_qkv.shape, BF16),
                pltpu.VMEM(k_in.shape, BF16), pltpu.VMEM(v_in.shape, BF16), pltpu.VMEM(w_qkv.shape, BF16), pltpu.VMEM(w_out.shape, BF16),
                pltpu.VMEM((n * 8, 128), F32), pltpu.VMEM((n // BB, 128, 128), F32), pltpu.VMEM((n // BB, 128, 128), F32), pltpu.VMEM((n * 8, 128), F32),
                pltpu.SemaphoreType.DMA((7,)), pltpu.SemaphoreType.DMA((W_PARTS,)), pltpu.SemaphoreType.DMA, pltpu.SemaphoreType.DMA((n // BB,)), pltpu.SemaphoreType.DMA((n // BB,)),
                pltpu.SemaphoreType.DMA((n // BB,)), pltpu.SemaphoreType.DMA((n // BB,)),
            ],
            compiler_params=pltpu.CompilerParams(vmem_limit_bytes=VMEM_LIMIT),
            name="attention",
        )(seq_lens, hidden, rope_cos.T, rope_sin.T, ln1_scale, ln1_bias, b_qkv, w_qkv, w_out, k_in, v_in)
        part = pltpu.with_memory_space_constraint(part, pltpu.VMEM)
        in_hbm = lambda w: pltpu.with_memory_space_constraint(w, pltpu.HBM)
        rows = lambda r, t: pltpu.VMEM((r, d), t)
        cut = lambda r, t: pltpu.VMEM((COLS, r, d // COLS), t)
        hidden_out = pl.pallas_call(
            moe_kernel,
            out_shape=pltpu.VMEM((n, d), BF16),
            in_specs=[vm] * 7 + [anyspace] * 3,
            out_specs=vm,
            scratch_shapes=[
                pltpu.VMEM((n_exp, d, 256), BF16), pltpu.VMEM((n_exp * 128, d), BF16), rows(128, BF16),
                pltpu.VMEM((3, 16, d), BF16), rows(16, F32), rows(256, BF16), pltpu.VMEM((4, 8, n), jnp.int32), pltpu.VMEM((256, n_exp * 128), BF16),
                cut(64, F32), cut(64, F32), cut(64, BF16), cut(64, BF16), cut(64, BF16), cut(64, BF16), cut(64, BF16), cut(64, BF16),
                cut(64, F32), cut(64, BF16), pltpu.VMEM((COLS, 3, 16, d // COLS), BF16), cut(64, BF16),
                pltpu.SemaphoreType.DMA((2 * n_exp + 1,)), pltpu.SemaphoreType.DMA((N_SLOTS,)), pltpu.SemaphoreType.DMA((N_SLOTS,)),
            ],
            compiler_params=pltpu.CompilerParams(vmem_limit_bytes=MOE_LIMIT, collective_id=0, has_side_effects=True),
            name="moe",
        )(hidden, part, b_out, ln2_scale, ln2_bias, w_router.T, expert_ids.T, in_hbm(w_gate), in_hbm(w_up), in_hbm(w_down.reshape(n_exp * 128, d)))
        unfold = lambda c: c.reshape(n, groups, head, s_max).transpose(0, 3, 1, 2)
        return hidden_out, unfold(k_out), unfold(v_out)

    in_specs = (token_rows, token_vec, token_rows, token_rows, P(), P(), P(None, 'tp'), P('tp'), P('tp', None), P(), cache_spec, cache_spec, P(), P(), P(), token_rows, expert_in, expert_in, expert_down)
    return jax.shard_map(device_step, mesh=mesh, in_specs=in_specs, out_specs=(token_rows, cache_spec, cache_spec), check_vma=False)
```

```python
import functools

import jax
import jax.numpy as jnp
from jax import lax
from jax.experimental import pallas as pl
from jax.experimental.pallas import tpu as pltpu
from jax.sharding import PartitionSpec as P

EPS = 1e-5
F32 = jnp.float32
BF16 = jnp.bfloat16
MESH = pl.DeviceIdType.MESH
VMEM_LIMIT = 66_400_000
MOE_LIMIT = 40_000_000
NT = (((1,), (1,)), ((), ()))
BB = 8
COLS = 6
PIECE = 16
AHEAD = 3
W_PARTS = 4


def normalize(vals_f32, ln_scale, ln_bias):
    row_mean = jnp.mean(vals_f32, axis=-1, keepdims=True)
    centered = vals_f32 - row_mean
    row_var = jnp.mean(centered * centered, axis=-1, keepdims=True)
    normed = centered * lax.rsqrt(row_var + EPS)
    return (normed * ln_scale + ln_bias).astype(BF16)


def row_of(vec_ref):
    return vec_ref[...].astype(F32)[None, :]


def attention_kernel(lens_hbm, hid_hbm, cos_hbm, sin_hbm, scale_hbm, bias_hbm, bqkv_hbm, wqkv_hbm, wout_hbm, k_hbm, v_hbm,
                     part_ref, ko_hbm, vo_hbm, lens_ref, hid_ref, cos_ref, sin_ref, scale_ref, bias_ref, bqkv_ref,
                     k_buf, v_buf, w_buf, wo_buf, q_buf, kn_buf, vn_buf, c_buf, in_sem, w_sem, wo_sem, k_sem, v_sem, ko_sem, vo_sem):
    n_rows = hid_ref.shape[0]
    n_blocks = n_rows // BB
    s_max = k_buf.shape[2]
    smalls = ((hid_hbm, hid_ref), (scale_hbm, scale_ref), (bias_hbm, bias_ref), (bqkv_hbm, bqkv_ref), (cos_hbm, cos_ref), (sin_hbm, sin_ref),
              (lens_hbm, lens_ref))
    small_copies = [pltpu.make_async_copy(src, dst, in_sem.at[i]) for i, (src, dst) in enumerate(smalls)]
    w_rows = w_buf.shape[0] // W_PARTS
    w_copies = [pltpu.make_async_copy(wqkv_hbm.at[pl.ds(i * w_rows, w_rows)], w_buf.at[pl.ds(i * w_rows, w_rows)], w_sem.at[i]) for i in range(W_PARTS)]
    wo_copy = pltpu.make_async_copy(wout_hbm, wo_buf, wo_sem)
    for copy in small_copies[:3] + w_copies + small_copies[3:]:
        copy.start()

    def fetch(i):
        rows = pl.ds(i * BB, BB)
        return (pltpu.make_async_copy(k_hbm.at[rows], k_buf.at[rows], k_sem.at[i]),
                pltpu.make_async_copy(v_hbm.at[rows], v_buf.at[rows], v_sem.at[i]))

    def flush(i):
        rows = pl.ds(i * BB, BB)
        return (pltpu.make_async_copy(k_buf.at[rows], ko_hbm.at[rows], ko_sem.at[i]),
                pltpu.make_async_copy(v_buf.at[rows], vo_hbm.at[rows], vo_sem.at[i]))

    def fetch_start(i):
        for copy in fetch(i):
            copy.start()

    for i in range(AHEAD):
        fetch_start(i)

    for copy in small_copies:
        copy.wait()
    normed = normalize(hid_ref[...].astype(F32), row_of(scale_ref), row_of(bias_ref))
    for copy in w_copies:
        copy.wait()
    fetch_start(AHEAD)
    qkv = jnp.dot(normed, w_buf[...], preferred_element_type=F32) + row_of(bqkv_ref)
    qkv = qkv.astype(BF16).astype(F32)
    qkv = jnp.concatenate([qkv, jnp.zeros((128 - n_rows, qkv.shape[1]), F32)], axis=0)
    feats = qkv.T
    cos_t = jnp.concatenate([cos_ref[...], jnp.zeros((32, 128 - n_rows), F32)], axis=1)
    sin_t = jnp.concatenate([sin_ref[...], jnp.zeros((32, 128 - n_rows), F32)], axis=1)

    def rotate(base):
        u, w = feats[base:base + 32], feats[base + 32:base + 64]
        return jnp.concatenate([u * cos_t - w * sin_t, w * cos_t + u * sin_t], axis=0).astype(BF16).astype(F32)

    zeros = jnp.zeros((64, 128), F32)
    for g in range(2):
        for j in range(3):
            q_rot = rotate(g * 320 + j * 64)
            both = jnp.concatenate([q_rot, zeros] if g == 0 else [zeros, q_rot], axis=0)
            q_buf[pl.ds(g * 3 + j, n_rows, stride=8), :] = both.T[:n_rows]
    for r in (6, 7):
        q_buf[pl.ds(r, n_rows, stride=8), :] = jnp.zeros((n_rows, 128), F32)
    k_new = jnp.concatenate([rotate(192), rotate(320 + 192)], axis=0)
    v_new = jnp.concatenate([feats[256:320], feats[320 + 256:320 + 320]], axis=0)
    for i in range(n_blocks):
        kn_buf[i] = k_new if i == 0 else pltpu.roll(k_new, 128 - i * BB, 1)
        vn_buf[i] = v_new if i == 0 else pltpu.roll(v_new, 128 - i * BB, 1)

    def block(i, carry):
        for copy in fetch(i):
            copy.wait()

        @pl.when(i + AHEAD + 1 < n_blocks)
        def _():
            fetch_start(i + AHEAD + 1)

        @pl.when(i == n_blocks - AHEAD - 1)
        def _():
            wo_copy.start()

        k_cols, v_cols = kn_buf[i], vn_buf[i]
        lane = lax.broadcasted_iota(jnp.int32, (128, 128), 1)
        position = lax.broadcasted_iota(jnp.int32, (8, s_max), 1)
        scores = []
        for j in range(BB):
            b = i * BB + j
            pos = lens_ref[b]
            first = pl.multiple_of((pos // 128) * 128, 128)
            hit = lane == pos - first
            window = pl.ds(first, 128)
            k_buf[b, :, window] = jnp.where(hit, k_cols[:, j:j + 1], k_buf[b, :, window].astype(F32)).astype(BF16)
            v_buf[b, :, window] = jnp.where(hit, v_cols[:, j:j + 1], v_buf[b, :, window].astype(F32)).astype(BF16)
            rows = pl.ds(pl.multiple_of(b * 8, 8), 8)
            one = jnp.dot(q_buf[rows, :].astype(BF16), k_buf[b], preferred_element_type=F32) * 0.125
            scores.append(jnp.where(position <= pos, one, -jnp.inf))
        scores = jnp.concatenate(scores, axis=0)
        top = jnp.max(scores, axis=1, keepdims=True)
        weights = jnp.exp(scores - top)
        probs = weights * (1.0 / jnp.sum(weights, axis=1, keepdims=True))
        for j in range(BB):
            b = i * BB + j
            rows = pl.ds(pl.multiple_of(b * 8, 8), 8)
            c_buf[rows, :] = lax.dot_general(probs[j * 8:j * 8 + 8].astype(BF16), v_buf[b], NT, preferred_element_type=F32)
        for copy in flush(i):
            copy.start()
        return carry

    lax.fori_loop(0, n_blocks, block, 0)
    heads = [c_buf[pl.ds(r, n_rows, stride=8), :] for r in range(6)]
    low = lax.broadcasted_iota(jnp.int32, (n_rows, 128), 1) < 64
    ctx = jnp.concatenate([
        jnp.where(low, heads[0], pltpu.roll(heads[1], 64, 1)),
        jnp.where(low, heads[2], heads[3]),
        jnp.where(low, pltpu.roll(heads[4], 64, 1), heads[5]),
    ], axis=1).astype(BF16)
    wo_copy.wait()
    part_ref[...] = jnp.dot(ctx, wo_buf[...], preferred_element_type=F32).astype(BF16)
    for i in range(n_blocks):
        for copy in flush(i):
            copy.wait()


def moe_kernel(hid_ref, part_ref, bout_ref, scale_ref, bias_ref, wr_ref, ids_ref, wg_hbm, wu_hbm, wd_hbm, out_ref,
               wgu, wd, wr, rs_recv, x1, h2, ids_buf, act, own_p, y_p, hi0, hi1, d0, d1, y_send, y_recv,
               t_f, t_b, z_recv, o_buf, wsem, ssem, rsem):
    z, ep = lax.axis_index("tp"), lax.axis_index("ep")
    n_rows, d_model = hid_ref.shape
    n_exp = wgu.shape[0]
    width = d_model // COLS
    z_peers = [lax.rem(z + dz, 4) for dz in (1, 2, 3)]
    y_peer = lax.rem(ep + 2, 4)
    partner = ep + 1 - 2 * lax.rem(ep, 2)
    diagonal = 3 - ep
    barrier = pltpu.get_barrier_semaphore()
    for peer in z_peers:
        pl.semaphore_signal(barrier, inc=1, device_id={"tp": peer}, device_id_type=MESH)
    for peer in (y_peer, partner, diagonal):
        pl.semaphore_signal(barrier, inc=1, device_id={"ep": peer}, device_id_type=MESH)

    loads = []
    for e in range(n_exp):
        loads.append(pltpu.make_async_copy(wg_hbm.at[e], wgu.at[e, :, 0:128], wsem.at[2 * e]))
        loads.append(pltpu.make_async_copy(wu_hbm.at[e], wgu.at[e, :, 128:256], wsem.at[2 * e + 1]))
    loads.append(pltpu.make_async_copy(wd_hbm, wd, wsem.at[2 * n_exp]))
    for load in loads:
        load.start()

    count = [0]

    def remote(src, dst, device):
        slot = count[0]
        count[0] += 1
        return pltpu.make_async_remote_copy(src_ref=src, dst_ref=dst, send_sem=ssem.at[slot], recv_sem=rsem.at[slot],
                                            device_id=device, device_id_type=MESH)

    def at(index, h, shard=0):
        return pl.ds(pl.multiple_of(shard * n_rows + index * 16 + h * PIECE, PIECE), PIECE)

    def rows_at(index):
        return pl.ds(pl.multiple_of(index * 16, 16), 16)

    def cols(n):
        return pl.ds(n * width, width)

    halves = range(16 // PIECE)
    z_order = [z] + [lax.rem(z + 4 - dz, 4) for dz in (1, 2, 3)]
    rs = [[remote(part_ref.at[at(z_peers[dz], h)], rs_recv.at[dz, pl.ds(h * PIECE, PIECE)], {"tp": z_peers[dz]}) for dz in range(3)] for h in halves]
    to_z = [[remote(h2.at[at(z, h)], h2.at[at(z, h)], {"tp": z_peers[dz]}) for dz in range(3)] for h in halves]
    to_p = [[remote(h2.at[at(z_order[k], h)], h2.at[at(z_order[k], h, 1)], {"ep": partner}) for k in range(4)] for h in halves]
    to_y = [[remote(h2.at[at(z_order[k], h)], h2.at[at(z_order[k], h, 2)], {"ep": y_peer}) for k in range(4)] for h in halves]
    y_to_p = [[remote(h2.at[at(z_order[k], h, 2)], h2.at[at(z_order[k], h, 3)], {"ep": partner}) for k in range(4)] for h in halves]
    mine = rows_at(z)
    to_ids = [remote(ids_ref, ids_buf.at[i + 1], {"ep": peer}) for i, peer in enumerate((partner, y_peer, diagonal))]
    chunks = range(COLS)
    to_d0 = [remote(hi0.at[n], d0.at[n], {"ep": partner}) for n in chunks]
    to_d = [remote(hi1.at[n], d1.at[n], {"ep": partner}) for n in chunks]
    to_yy = [remote(y_send.at[n], y_recv.at[n], {"ep": y_peer}) for n in chunks]
    to_zz = [[remote(t_b.at[n, rows_at(z_peers[dz])], z_recv.at[n, dz], {"tp": z_peers[dz]}) for dz in range(3)] for n in chunks]
    to_o = [[remote(o_buf.at[n, mine], o_buf.at[n, mine], {"tp": z_peers[dz]}) for dz in range(3)] for n in chunks]

    scale, bias, bout = row_of(scale_ref), row_of(bias_ref), row_of(bout_ref)
    ids_buf[0] = ids_ref[...]
    wr[...] = jnp.concatenate([wr_ref[...], jnp.zeros((128 - wr_ref.shape[0], d_model), BF16)], axis=0)
    pl.semaphore_wait(barrier, 6)

    for h in halves:
        for dz in range(3):
            rs[h][dz].start()
    for copy in to_ids:
        copy.start()
    for h in halves:
        for dz in range(3):
            rs[h][dz].wait_recv()
        got = pl.ds(h * PIECE, PIECE)
        total = part_ref[at(z, h), :].astype(F32) + rs_recv[0, got].astype(F32) + rs_recv[1, got].astype(F32) + rs_recv[2, got].astype(F32)
        row = (hid_ref[at(z, h), :].astype(F32) + total + bout).astype(BF16)
        x1[got, :] = row.astype(F32)
        h2[at(z, h), :] = normalize(row.astype(F32), scale, bias)
        for dz in range(3):
            to_z[h][dz].start()
        to_y[h][0].start()
        to_p[h][0].start()

    def relay(h, k):
        to_y[h][k].wait_recv()
        y_to_p[h][k].start()

    for h in halves:
        for dz in range(3):
            to_z[h][dz].wait_recv()
            to_y[h][dz + 1].start()
            to_p[h][dz + 1].start()
        relay(h, 0)

    def masks(shard):
        picks = ids_buf[shard]
        expert = lax.broadcasted_iota(jnp.int32, (128, n_rows), 0)
        hit = jnp.zeros((128, n_rows), F32)
        for k in range(picks.shape[0]):
            hit = jnp.where(expert == picks[k:k + 1, :], 1.0, hit)
        return hit.T

    def toks(shard):
        return h2[shard * n_rows:(shard + 1) * n_rows, :]

    def gates_of(shard):
        logits = lax.dot_general(toks(shard), wr[...], NT, preferred_element_type=F32)
        logits = jnp.where(masks(shard) > 0.5, logits, -jnp.inf)
        shifted = jnp.exp(logits - jnp.max(logits, axis=1, keepdims=True))
        gates = (shifted / jnp.sum(shifted, axis=1, keepdims=True)).astype(BF16).astype(F32)
        return pltpu.roll(gates, lax.rem(128 - ep * n_exp, 128), 1)

    def up(shard, gates, first, last):
        rows = toks(shard)
        for e in range(first, last):
            if shard == 0:
                loads[2 * e].wait()
                loads[2 * e + 1].wait()
            pre = jnp.dot(rows, wgu[e], preferred_element_type=F32)
            gate_pre, up_pre = pre[:, :128], pre[:, 128:]
            hidden = (gate_pre * jax.nn.sigmoid(gate_pre) * up_pre).astype(BF16).astype(F32)
            act[shard * n_rows:(shard + 1) * n_rows, e * 128:(e + 1) * 128] = (hidden * gates[:, e:e + 1]).astype(BF16)

    for copy in to_ids:
        copy.wait_recv()
    up(0, gates_of(0), 0, n_exp)
    for h in halves:
        for copy in to_p[h]:
            copy.wait_recv()
    up(1, gates_of(1), 0, n_exp)
    for h in halves:
        for k in (1, 2, 3):
            relay(h, k)
    up(2, gates_of(2), 0, n_exp)
    for h in halves:
        for copy in y_to_p[h]:
            copy.wait_recv()
    up(3, gates_of(3), 0, n_exp)
    loads[-1].wait()

    def reduce_pair(n):
        to_d[n].wait_recv()
        y_send[n] = (y_p[n] + d1[n].astype(F32)).astype(BF16)
        to_yy[n].start()

    for n in chunks:
        both = jnp.dot(act[128:256, :], wd[:, cols(n)], preferred_element_type=F32)
        y_p[n] = both[0:64]
        hi1[n] = both[64:128].astype(BF16)
        to_d[n].start()
        if n > 0:
            reduce_pair(n - 1)
        both = jnp.dot(act[0:128, :], wd[:, cols(n)], preferred_element_type=F32)
        own_p[n] = both[0:64]
        hi0[n] = both[64:128].astype(BF16)
        to_d0[n].start()
    reduce_pair(COLS - 1)
    for n in chunks:
        to_d0[n].wait_recv()
        to_yy[n].wait_recv()
        t = own_p[n] + d0[n].astype(F32) + y_recv[n].astype(F32)
        t_f[n] = t
        t_b[n] = t.astype(BF16)
        for copy in to_zz[n]:
            copy.start()
    for n in chunks:
        for copy in to_zz[n]:
            copy.wait_recv()
        moe = t_f[n, mine, :] + z_recv[n, 0].astype(F32) + z_recv[n, 1].astype(F32) + z_recv[n, 2].astype(F32)
        o_buf[n, mine, :] = (x1[:, cols(n)] + moe).astype(BF16)
        for copy in to_o[n]:
            copy.start()
    for n in chunks:
        for copy in to_o[n]:
            copy.wait_recv()
        out_ref[:, cols(n)] = o_buf[n]
    for group in rs + to_z + to_p + to_y + y_to_p + [to_ids, to_d0, to_d, to_yy] + to_zz + to_o:
        for copy in group:
            copy.wait_send()


N_SLOTS = (16 // PIECE) * 18 + 3 + 9 * COLS


def solution(mesh):
    token_rows = P(('dp', 'ep'), None)
    token_vec = P(('dp', 'ep'))
    cache_spec = P(('dp', 'ep'), None, 'tp', None)
    expert_in = P('ep', None, 'tp')
    expert_down = P('ep', 'tp', None)
    vm = pl.BlockSpec(memory_space=pltpu.VMEM)
    anyspace = pl.BlockSpec(memory_space=pl.ANY)

    def device_step(hidden, seq_lens, rope_cos, rope_sin, ln1_scale, ln1_bias, w_qkv, b_qkv, w_out, b_out, k_cache, v_cache, ln2_scale, ln2_bias, w_router, expert_ids, w_gate, w_up, w_down):
        n, d = hidden.shape
        _, s_max, groups, head = k_cache.shape
        feat = groups * head
        n_exp = w_gate.shape[0]
        k_in = k_cache.transpose(0, 2, 3, 1).reshape(n, feat, s_max)
        v_in = v_cache.transpose(0, 2, 3, 1).reshape(n, feat, s_max)
        part, k_out, v_out = pl.pallas_call(
            attention_kernel,
            out_shape=(pltpu.VMEM((n, d), BF16), jax.ShapeDtypeStruct(k_in.shape, BF16), jax.ShapeDtypeStruct(v_in.shape, BF16)),
            in_specs=[anyspace] * 11,
            out_specs=(vm, anyspace, anyspace),
            scratch_shapes=[
                pltpu.SMEM((n,), jnp.int32), pltpu.VMEM((n, d), BF16), pltpu.VMEM((32, n), F32), pltpu.VMEM((32, n), F32),
                pltpu.VMEM((d,), BF16), pltpu.VMEM((d,), BF16), pltpu.VMEM(b_qkv.shape, BF16),
                pltpu.VMEM(k_in.shape, BF16), pltpu.VMEM(v_in.shape, BF16), pltpu.VMEM(w_qkv.shape, BF16), pltpu.VMEM(w_out.shape, BF16),
                pltpu.VMEM((n * 8, 128), F32), pltpu.VMEM((n // BB, 128, 128), F32), pltpu.VMEM((n // BB, 128, 128), F32), pltpu.VMEM((n * 8, 128), F32),
                pltpu.SemaphoreType.DMA((7,)), pltpu.SemaphoreType.DMA((W_PARTS,)), pltpu.SemaphoreType.DMA, pltpu.SemaphoreType.DMA((n // BB,)), pltpu.SemaphoreType.DMA((n // BB,)),
                pltpu.SemaphoreType.DMA((n // BB,)), pltpu.SemaphoreType.DMA((n // BB,)),
            ],
            compiler_params=pltpu.CompilerParams(vmem_limit_bytes=VMEM_LIMIT),
            name="attention",
        )(seq_lens, hidden, rope_cos.T, rope_sin.T, ln1_scale, ln1_bias, b_qkv, w_qkv, w_out, k_in, v_in)
        part = pltpu.with_memory_space_constraint(part, pltpu.VMEM)
        in_hbm = lambda w: pltpu.with_memory_space_constraint(w, pltpu.HBM)
        rows = lambda r, t: pltpu.VMEM((r, d), t)
        cut = lambda r, t: pltpu.VMEM((COLS, r, d // COLS), t)
        hidden_out = pl.pallas_call(
            moe_kernel,
            out_shape=pltpu.VMEM((n, d), BF16),
            in_specs=[vm] * 7 + [anyspace] * 3,
            out_specs=vm,
            scratch_shapes=[
                pltpu.VMEM((n_exp, d, 256), BF16), pltpu.VMEM((n_exp * 128, d), BF16), rows(128, BF16),
                pltpu.VMEM((3, 16, d), BF16), rows(16, F32), rows(256, BF16), pltpu.VMEM((4, 8, n), jnp.int32), pltpu.VMEM((256, n_exp * 128), BF16),
                cut(64, F32), cut(64, F32), cut(64, BF16), cut(64, BF16), cut(64, BF16), cut(64, BF16), cut(64, BF16), cut(64, BF16),
                cut(64, F32), cut(64, BF16), pltpu.VMEM((COLS, 3, 16, d // COLS), BF16), cut(64, BF16),
                pltpu.SemaphoreType.DMA((2 * n_exp + 1,)), pltpu.SemaphoreType.DMA((N_SLOTS,)), pltpu.SemaphoreType.DMA((N_SLOTS,)),
            ],
            compiler_params=pltpu.CompilerParams(vmem_limit_bytes=MOE_LIMIT, collective_id=0, has_side_effects=True),
            name="moe",
        )(hidden, part, b_out, ln2_scale, ln2_bias, w_router.T, expert_ids.T, in_hbm(w_gate), in_hbm(w_up), in_hbm(w_down.reshape(n_exp * 128, d)))
        unfold = lambda c: c.reshape(n, groups, head, s_max).transpose(0, 3, 1, 2)
        return hidden_out, unfold(k_out), unfold(v_out)

    in_specs = (token_rows, token_vec, token_rows, token_rows, P(), P(), P(None, 'tp'), P('tp'), P('tp', None), P(), cache_spec, cache_spec, P(), P(), P(), token_rows, expert_in, expert_in, expert_down)
    return jax.shard_map(device_step, mesh=mesh, in_specs=in_specs, out_specs=(token_rows, cache_spec, cache_spec), check_vma=False)
```

```python
import functools

import jax
import jax.numpy as jnp
from jax import lax
from jax.experimental import pallas as pl
from jax.experimental.pallas import tpu as pltpu
from jax.sharding import PartitionSpec as P

EPS = 1e-5
F32 = jnp.float32
BF16 = jnp.bfloat16
MESH = pl.DeviceIdType.MESH
VMEM_LIMIT = 66_400_000
MOE_LIMIT = 40_000_000
NT = (((1,), (1,)), ((), ()))
BB = 8
COLS = 2
PIECE = 16
AHEAD = 3
W_PARTS = 4


def normalize(vals_f32, ln_scale, ln_bias):
    row_mean = jnp.mean(vals_f32, axis=-1, keepdims=True)
    centered = vals_f32 - row_mean
    row_var = jnp.mean(centered * centered, axis=-1, keepdims=True)
    normed = centered * lax.rsqrt(row_var + EPS)
    return (normed * ln_scale + ln_bias).astype(BF16)


def row_of(vec_ref):
    return vec_ref[...].astype(F32)[None, :]


def attention_kernel(lens_hbm, hid_hbm, cos_hbm, sin_hbm, scale_hbm, bias_hbm, bqkv_hbm, wqkv_hbm, wout_hbm, k_hbm, v_hbm,
                     part_ref, ko_hbm, vo_hbm, lens_ref, hid_ref, cos_ref, sin_ref, scale_ref, bias_ref, bqkv_ref,
                     k_buf, v_buf, w_buf, wo_buf, q_buf, kn_buf, vn_buf, c_buf, in_sem, w_sem, wo_sem, k_sem, v_sem, ko_sem, vo_sem):
    n_rows = hid_ref.shape[0]
    n_blocks = n_rows // BB
    s_max = k_buf.shape[2]
    smalls = ((hid_hbm, hid_ref), (scale_hbm, scale_ref), (bias_hbm, bias_ref), (bqkv_hbm, bqkv_ref), (cos_hbm, cos_ref), (sin_hbm, sin_ref),
              (lens_hbm, lens_ref))
    small_copies = [pltpu.make_async_copy(src, dst, in_sem.at[i]) for i, (src, dst) in enumerate(smalls)]
    w_rows = w_buf.shape[0] // W_PARTS
    w_copies = [pltpu.make_async_copy(wqkv_hbm.at[pl.ds(i * w_rows, w_rows)], w_buf.at[pl.ds(i * w_rows, w_rows)], w_sem.at[i]) for i in range(W_PARTS)]
    wo_copy = pltpu.make_async_copy(wout_hbm, wo_buf, wo_sem)
    for copy in small_copies[:3] + w_copies + small_copies[3:]:
        copy.start()

    def fetch(i):
        rows = pl.ds(i * BB, BB)
        return (pltpu.make_async_copy(k_hbm.at[rows], k_buf.at[rows], k_sem.at[i]),
                pltpu.make_async_copy(v_hbm.at[rows], v_buf.at[rows], v_sem.at[i]))

    def flush(i):
        rows = pl.ds(i * BB, BB)
        return (pltpu.make_async_copy(k_buf.at[rows], ko_hbm.at[rows], ko_sem.at[i]),
                pltpu.make_async_copy(v_buf.at[rows], vo_hbm.at[rows], vo_sem.at[i]))

    def fetch_start(i):
        for copy in fetch(i):
            copy.start()

    for i in range(AHEAD):
        fetch_start(i)

    for copy in small_copies:
        copy.wait()
    normed = normalize(hid_ref[...].astype(F32), row_of(scale_ref), row_of(bias_ref))
    for copy in w_copies:
        copy.wait()
    fetch_start(AHEAD)
    qkv = jnp.dot(normed, w_buf[...], preferred_element_type=F32) + row_of(bqkv_ref)
    qkv = qkv.astype(BF16).astype(F32)
    qkv = jnp.concatenate([qkv, jnp.zeros((128 - n_rows, qkv.shape[1]), F32)], axis=0)
    feats = qkv.T
    cos_t = jnp.concatenate([cos_ref[...], jnp.zeros((32, 128 - n_rows), F32)], axis=1)
    sin_t = jnp.concatenate([sin_ref[...], jnp.zeros((32, 128 - n_rows), F32)], axis=1)

    def rotate(base):
        u, w = feats[base:base + 32], feats[base + 32:base + 64]
        return jnp.concatenate([u * cos_t - w * sin_t, w * cos_t + u * sin_t], axis=0).astype(BF16).astype(F32)

    zeros = jnp.zeros((64, 128), F32)
    for g in range(2):
        for j in range(3):
            q_rot = rotate(g * 320 + j * 64)
            both = jnp.concatenate([q_rot, zeros] if g == 0 else [zeros, q_rot], axis=0)
            q_buf[pl.ds(g * 3 + j, n_rows, stride=8), :] = both.T[:n_rows]
    for r in (6, 7):
        q_buf[pl.ds(r, n_rows, stride=8), :] = jnp.zeros((n_rows, 128), F32)
    k_new = jnp.concatenate([rotate(192), rotate(320 + 192)], axis=0)
    v_new = jnp.concatenate([feats[256:320], feats[320 + 256:320 + 320]], axis=0)
    for i in range(n_blocks):
        kn_buf[i] = k_new if i == 0 else pltpu.roll(k_new, 128 - i * BB, 1)
        vn_buf[i] = v_new if i == 0 else pltpu.roll(v_new, 128 - i * BB, 1)

    def block(i, carry):
        for copy in fetch(i):
            copy.wait()

        @pl.when(i + AHEAD + 1 < n_blocks)
        def _():
            fetch_start(i + AHEAD + 1)

        @pl.when(i == n_blocks - AHEAD - 1)
        def _():
            wo_copy.start()

        k_cols, v_cols = kn_buf[i], vn_buf[i]
        lane = lax.broadcasted_iota(jnp.int32, (128, 128), 1)
        position = lax.broadcasted_iota(jnp.int32, (8, s_max), 1)
        scores = []
        for j in range(BB):
            b = i * BB + j
            pos = lens_ref[b]
            first = pl.multiple_of((pos // 128) * 128, 128)
            hit = lane == pos - first
            window = pl.ds(first, 128)
            k_buf[b, :, window] = jnp.where(hit, k_cols[:, j:j + 1], k_buf[b, :, window].astype(F32)).astype(BF16)
            v_buf[b, :, window] = jnp.where(hit, v_cols[:, j:j + 1], v_buf[b, :, window].astype(F32)).astype(BF16)
            rows = pl.ds(pl.multiple_of(b * 8, 8), 8)
            one = jnp.dot(q_buf[rows, :].astype(BF16), k_buf[b], preferred_element_type=F32) * 0.125
            scores.append(jnp.where(position <= pos, one, -jnp.inf))
        scores = jnp.concatenate(scores, axis=0)
        top = jnp.max(scores, axis=1, keepdims=True)
        weights = jnp.exp(scores - top)
        probs = weights * (1.0 / jnp.sum(weights, axis=1, keepdims=True))
        for j in range(BB):
            b = i * BB + j
            rows = pl.ds(pl.multiple_of(b * 8, 8), 8)
            c_buf[rows, :] = lax.dot_general(probs[j * 8:j * 8 + 8].astype(BF16), v_buf[b], NT, preferred_element_type=F32)
        for copy in flush(i):
            copy.start()
        return carry

    lax.fori_loop(0, n_blocks, block, 0)
    heads = [c_buf[pl.ds(r, n_rows, stride=8), :] for r in range(6)]
    low = lax.broadcasted_iota(jnp.int32, (n_rows, 128), 1) < 64
    ctx = jnp.concatenate([
        jnp.where(low, heads[0], pltpu.roll(heads[1], 64, 1)),
        jnp.where(low, heads[2], heads[3]),
        jnp.where(low, pltpu.roll(heads[4], 64, 1), heads[5]),
    ], axis=1).astype(BF16)
    wo_copy.wait()
    part_ref[...] = jnp.dot(ctx, wo_buf[...], preferred_element_type=F32).astype(BF16)
    for i in range(n_blocks):
        for copy in flush(i):
            copy.wait()


def moe_kernel(hid_ref, part_ref, bout_ref, scale_ref, bias_ref, wr_ref, ids_ref, wg_hbm, wu_hbm, wd_hbm, out_ref,
               wgu, wd, wr, rs_recv, x1, h2, ids_buf, act, own_p, y_p, hi0, hi1, d0, d1, y_send, y_recv,
               t_f, t_b, z_recv, o_buf, wsem, ssem, rsem):
    z, ep = lax.axis_index("tp"), lax.axis_index("ep")
    n_rows, d_model = hid_ref.shape
    n_exp = wgu.shape[0]
    width = d_model // COLS
    z_peers = [lax.rem(z + dz, 4) for dz in (1, 2, 3)]
    y_peer = lax.rem(ep + 2, 4)
    partner = ep + 1 - 2 * lax.rem(ep, 2)
    diagonal = 3 - ep
    barrier = pltpu.get_barrier_semaphore()
    for peer in z_peers:
        pl.semaphore_signal(barrier, inc=1, device_id={"tp": peer}, device_id_type=MESH)
    for peer in (y_peer, partner, diagonal):
        pl.semaphore_signal(barrier, inc=1, device_id={"ep": peer}, device_id_type=MESH)

    loads = []
    for e in range(n_exp):
        loads.append(pltpu.make_async_copy(wg_hbm.at[e], wgu.at[e, :, 0:128], wsem.at[2 * e]))
        loads.append(pltpu.make_async_copy(wu_hbm.at[e], wgu.at[e, :, 128:256], wsem.at[2 * e + 1]))
    loads.append(pltpu.make_async_copy(wd_hbm, wd, wsem.at[2 * n_exp]))
    for load in loads:
        load.start()

    count = [0]

    def remote(src, dst, device):
        slot = count[0]
        count[0] += 1
        return pltpu.make_async_remote_copy(src_ref=src, dst_ref=dst, send_sem=ssem.at[slot], recv_sem=rsem.at[slot],
                                            device_id=device, device_id_type=MESH)

    def at(index, h, shard=0):
        return pl.ds(pl.multiple_of(shard * n_rows + index * 16 + h * PIECE, PIECE), PIECE)

    def rows_at(index):
        return pl.ds(pl.multiple_of(index * 16, 16), 16)

    def cols(n):
        return pl.ds(n * width, width)

    halves = range(16 // PIECE)
    z_order = [z] + [lax.rem(z + 4 - dz, 4) for dz in (1, 2, 3)]
    rs = [[remote(part_ref.at[at(z_peers[dz], h)], rs_recv.at[dz, pl.ds(h * PIECE, PIECE)], {"tp": z_peers[dz]}) for dz in range(3)] for h in halves]
    to_z = [[remote(h2.at[at(z, h)], h2.at[at(z, h)], {"tp": z_peers[dz]}) for dz in range(3)] for h in halves]
    to_p = [[remote(h2.at[at(z_order[k], h)], h2.at[at(z_order[k], h, 1)], {"ep": partner}) for k in range(4)] for h in halves]
    to_y = [[remote(h2.at[at(z_order[k], h)], h2.at[at(z_order[k], h, 2)], {"ep": y_peer}) for k in range(4)] for h in halves]
    y_to_p = [[remote(h2.at[at(z_order[k], h, 2)], h2.at[at(z_order[k], h, 3)], {"ep": partner}) for k in range(4)] for h in halves]
    mine = rows_at(z)
    to_ids = [remote(ids_ref, ids_buf.at[i + 1], {"ep": peer}) for i, peer in enumerate((partner, y_peer, diagonal))]
    chunks = range(COLS)
    to_d0 = [remote(hi0.at[n], d0.at[n], {"ep": partner}) for n in chunks]
    to_d = [remote(hi1.at[n], d1.at[n], {"ep": partner}) for n in chunks]
    to_yy = [remote(y_send.at[n], y_recv.at[n], {"ep": y_peer}) for n in chunks]
    to_zz = [[remote(t_b.at[n, rows_at(z_peers[dz])], z_recv.at[n, dz], {"tp": z_peers[dz]}) for dz in range(3)] for n in chunks]
    to_o = [[remote(o_buf.at[n, mine], o_buf.at[n, mine], {"tp": z_peers[dz]}) for dz in range(3)] for n in chunks]

    scale, bias, bout = row_of(scale_ref), row_of(bias_ref), row_of(bout_ref)
    ids_buf[0] = ids_ref[...]
    wr[...] = jnp.concatenate([wr_ref[...], jnp.zeros((128 - wr_ref.shape[0], d_model), BF16)], axis=0)
    pl.semaphore_wait(barrier, 6)

    for h in halves:
        for dz in range(3):
            rs[h][dz].start()
    for copy in to_ids:
        copy.start()
    for h in halves:
        for dz in range(3):
            rs[h][dz].wait_recv()
        got = pl.ds(h * PIECE, PIECE)
        total = part_ref[at(z, h), :].astype(F32) + rs_recv[0, got].astype(F32) + rs_recv[1, got].astype(F32) + rs_recv[2, got].astype(F32)
        row = (hid_ref[at(z, h), :].astype(F32) + total + bout).astype(BF16)
        x1[got, :] = row.astype(F32)
        h2[at(z, h), :] = normalize(row.astype(F32), scale, bias)
        for dz in range(3):
            to_z[h][dz].start()
        to_y[h][0].start()
        to_p[h][0].start()

    def relay(h, k):
        to_y[h][k].wait_recv()
        y_to_p[h][k].start()

    for h in halves:
        for dz in range(3):
            to_z[h][dz].wait_recv()
            to_y[h][dz + 1].start()
            to_p[h][dz + 1].start()
        relay(h, 0)

    def masks(shard):
        picks = ids_buf[shard]
        expert = lax.broadcasted_iota(jnp.int32, (128, n_rows), 0)
        hit = jnp.zeros((128, n_rows), F32)
        for k in range(picks.shape[0]):
            hit = jnp.where(expert == picks[k:k + 1, :], 1.0, hit)
        return hit.T

    def toks(shard):
        return h2[shard * n_rows:(shard + 1) * n_rows, :]

    def gates_of(shard):
        logits = lax.dot_general(toks(shard), wr[...], NT, preferred_element_type=F32)
        logits = jnp.where(masks(shard) > 0.5, logits, -jnp.inf)
        shifted = jnp.exp(logits - jnp.max(logits, axis=1, keepdims=True))
        gates = (shifted / jnp.sum(shifted, axis=1, keepdims=True)).astype(BF16).astype(F32)
        return pltpu.roll(gates, lax.rem(128 - ep * n_exp, 128), 1)

    def up(shard, gates, first, last):
        rows = toks(shard)
        for e in range(first, last):
            if shard == 0:
                loads[2 * e].wait()
                loads[2 * e + 1].wait()
            pre = jnp.dot(rows, wgu[e], preferred_element_type=F32)
            gate_pre, up_pre = pre[:, :128], pre[:, 128:]
            hidden = (gate_pre * jax.nn.sigmoid(gate_pre) * up_pre).astype(BF16).astype(F32)
            act[shard * n_rows:(shard + 1) * n_rows, e * 128:(e + 1) * 128] = (hidden * gates[:, e:e + 1]).astype(BF16)

    for copy in to_ids:
        copy.wait_recv()
    up(0, gates_of(0), 0, n_exp)
    for h in halves:
        for copy in to_p[h]:
            copy.wait_recv()
    up(1, gates_of(1), 0, n_exp)
    for h in halves:
        for k in (1, 2, 3):
            relay(h, k)
    up(2, gates_of(2), 0, n_exp)
    for h in halves:
        for copy in y_to_p[h]:
            copy.wait_recv()
    up(3, gates_of(3), 0, n_exp)
    loads[-1].wait()

    def reduce_pair(n):
        to_d[n].wait_recv()
        y_send[n] = (y_p[n] + d1[n].astype(F32)).astype(BF16)
        to_yy[n].start()

    for n in chunks:
        both = jnp.dot(act[128:256, :], wd[:, cols(n)], preferred_element_type=F32)
        y_p[n] = both[0:64]
        hi1[n] = both[64:128].astype(BF16)
        to_d[n].start()
        if n > 0:
            reduce_pair(n - 1)
        both = jnp.dot(act[0:128, :], wd[:, cols(n)], preferred_element_type=F32)
        own_p[n] = both[0:64]
        hi0[n] = both[64:128].astype(BF16)
        to_d0[n].start()
    reduce_pair(COLS - 1)
    for n in chunks:
        to_d0[n].wait_recv()
        to_yy[n].wait_recv()
        t = own_p[n] + d0[n].astype(F32) + y_recv[n].astype(F32)
        t_f[n] = t
        t_b[n] = t.astype(BF16)
        for copy in to_zz[n]:
            copy.start()
    for n in chunks:
        for copy in to_zz[n]:
            copy.wait_recv()
        moe = t_f[n, mine, :] + z_recv[n, 0].astype(F32) + z_recv[n, 1].astype(F32) + z_recv[n, 2].astype(F32)
        o_buf[n, mine, :] = (x1[:, cols(n)] + moe).astype(BF16)
        for copy in to_o[n]:
            copy.start()
    for n in chunks:
        for copy in to_o[n]:
            copy.wait_recv()
        out_ref[:, cols(n)] = o_buf[n]
    for group in rs + to_z + to_p + to_y + y_to_p + [to_ids, to_d0, to_d, to_yy] + to_zz + to_o:
        for copy in group:
            copy.wait_send()


N_SLOTS = (16 // PIECE) * 18 + 3 + 9 * COLS


def solution(mesh):
    token_rows = P(('dp', 'ep'), None)
    token_vec = P(('dp', 'ep'))
    cache_spec = P(('dp', 'ep'), None, 'tp', None)
    expert_in = P('ep', None, 'tp')
    expert_down = P('ep', 'tp', None)
    vm = pl.BlockSpec(memory_space=pltpu.VMEM)
    anyspace = pl.BlockSpec(memory_space=pl.ANY)

    def device_step(hidden, seq_lens, rope_cos, rope_sin, ln1_scale, ln1_bias, w_qkv, b_qkv, w_out, b_out, k_cache, v_cache, ln2_scale, ln2_bias, w_router, expert_ids, w_gate, w_up, w_down):
        n, d = hidden.shape
        _, s_max, groups, head = k_cache.shape
        feat = groups * head
        n_exp = w_gate.shape[0]
        k_in = k_cache.transpose(0, 2, 3, 1).reshape(n, feat, s_max)
        v_in = v_cache.transpose(0, 2, 3, 1).reshape(n, feat, s_max)
        part, k_out, v_out = pl.pallas_call(
            attention_kernel,
            out_shape=(pltpu.VMEM((n, d), BF16), jax.ShapeDtypeStruct(k_in.shape, BF16), jax.ShapeDtypeStruct(v_in.shape, BF16)),
            in_specs=[anyspace] * 11,
            out_specs=(vm, anyspace, anyspace),
            scratch_shapes=[
                pltpu.SMEM((n,), jnp.int32), pltpu.VMEM((n, d), BF16), pltpu.VMEM((32, n), F32), pltpu.VMEM((32, n), F32),
                pltpu.VMEM((d,), BF16), pltpu.VMEM((d,), BF16), pltpu.VMEM(b_qkv.shape, BF16),
                pltpu.VMEM(k_in.shape, BF16), pltpu.VMEM(v_in.shape, BF16), pltpu.VMEM(w_qkv.shape, BF16), pltpu.VMEM(w_out.shape, BF16),
                pltpu.VMEM((n * 8, 128), F32), pltpu.VMEM((n // BB, 128, 128), F32), pltpu.VMEM((n // BB, 128, 128), F32), pltpu.VMEM((n * 8, 128), F32),
                pltpu.SemaphoreType.DMA((7,)), pltpu.SemaphoreType.DMA((W_PARTS,)), pltpu.SemaphoreType.DMA, pltpu.SemaphoreType.DMA((n // BB,)), pltpu.SemaphoreType.DMA((n // BB,)),
                pltpu.SemaphoreType.DMA((n // BB,)), pltpu.SemaphoreType.DMA((n // BB,)),
            ],
            compiler_params=pltpu.CompilerParams(vmem_limit_bytes=VMEM_LIMIT),
            name="attention",
        )(seq_lens, hidden, rope_cos.T, rope_sin.T, ln1_scale, ln1_bias, b_qkv, w_qkv, w_out, k_in, v_in)
        part = pltpu.with_memory_space_constraint(part, pltpu.VMEM)
        in_hbm = lambda w: pltpu.with_memory_space_constraint(w, pltpu.HBM)
        rows = lambda r, t: pltpu.VMEM((r, d), t)
        cut = lambda r, t: pltpu.VMEM((COLS, r, d // COLS), t)
        hidden_out = pl.pallas_call(
            moe_kernel,
            out_shape=pltpu.VMEM((n, d), BF16),
            in_specs=[vm] * 7 + [anyspace] * 3,
            out_specs=vm,
            scratch_shapes=[
                pltpu.VMEM((n_exp, d, 256), BF16), pltpu.VMEM((n_exp * 128, d), BF16), rows(128, BF16),
                pltpu.VMEM((3, 16, d), BF16), rows(16, F32), rows(256, BF16), pltpu.VMEM((4, 8, n), jnp.int32), pltpu.VMEM((256, n_exp * 128), BF16),
                cut(64, F32), cut(64, F32), cut(64, BF16), cut(64, BF16), cut(64, BF16), cut(64, BF16), cut(64, BF16), cut(64, BF16),
                cut(64, F32), cut(64, BF16), pltpu.VMEM((COLS, 3, 16, d // COLS), BF16), cut(64, BF16),
                pltpu.SemaphoreType.DMA((2 * n_exp + 1,)), pltpu.SemaphoreType.DMA((N_SLOTS,)), pltpu.SemaphoreType.DMA((N_SLOTS,)),
            ],
            compiler_params=pltpu.CompilerParams(vmem_limit_bytes=MOE_LIMIT, collective_id=0, has_side_effects=True),
            name="moe",
        )(hidden, part, b_out, ln2_scale, ln2_bias, w_router.T, expert_ids.T, in_hbm(w_gate), in_hbm(w_up), in_hbm(w_down.reshape(n_exp * 128, d)))
        unfold = lambda c: c.reshape(n, groups, head, s_max).transpose(0, 3, 1, 2)
        return hidden_out, unfold(k_out), unfold(v_out)

    in_specs = (token_rows, token_vec, token_rows, token_rows, P(), P(), P(None, 'tp'), P('tp'), P('tp', None), P(), cache_spec, cache_spec, P(), P(), P(), token_rows, expert_in, expert_in, expert_down)
    return jax.shard_map(device_step, mesh=mesh, in_specs=in_specs, out_specs=(token_rows, cache_spec, cache_spec), check_vma=False)
```

```python
import functools

import jax
import jax.numpy as jnp
from jax import lax
from jax.experimental import pallas as pl
from jax.experimental.pallas import tpu as pltpu
from jax.sharding import PartitionSpec as P

EPS = 1e-5
F32 = jnp.float32
BF16 = jnp.bfloat16
MESH = pl.DeviceIdType.MESH
VMEM_LIMIT = 66_400_000
MOE_LIMIT = 40_000_000
NT = (((1,), (1,)), ((), ()))
BB = 8
COLS = 3
PIECE = 16
AHEAD = 4
W_PARTS = 4


def normalize(vals_f32, ln_scale, ln_bias):
    row_mean = jnp.mean(vals_f32, axis=-1, keepdims=True)
    centered = vals_f32 - row_mean
    row_var = jnp.mean(centered * centered, axis=-1, keepdims=True)
    normed = centered * lax.rsqrt(row_var + EPS)
    return (normed * ln_scale + ln_bias).astype(BF16)


def row_of(vec_ref):
    return vec_ref[...].astype(F32)[None, :]


def attention_kernel(lens_hbm, hid_hbm, cos_hbm, sin_hbm, scale_hbm, bias_hbm, bqkv_hbm, wqkv_hbm, wout_hbm, k_hbm, v_hbm,
                     part_ref, ko_hbm, vo_hbm, lens_ref, hid_ref, cos_ref, sin_ref, scale_ref, bias_ref, bqkv_ref,
                     k_buf, v_buf, w_buf, wo_buf, q_buf, kn_buf, vn_buf, c_buf, in_sem, w_sem, wo_sem, k_sem, v_sem, ko_sem, vo_sem):
    n_rows = hid_ref.shape[0]
    n_blocks = n_rows // BB
    s_max = k_buf.shape[2]
    smalls = ((hid_hbm, hid_ref), (scale_hbm, scale_ref), (bias_hbm, bias_ref), (bqkv_hbm, bqkv_ref), (cos_hbm, cos_ref), (sin_hbm, sin_ref),
              (lens_hbm, lens_ref))
    small_copies = [pltpu.make_async_copy(src, dst, in_sem.at[i]) for i, (src, dst) in enumerate(smalls)]
    w_rows = w_buf.shape[0] // W_PARTS
    w_copies = [pltpu.make_async_copy(wqkv_hbm.at[pl.ds(i * w_rows, w_rows)], w_buf.at[pl.ds(i * w_rows, w_rows)], w_sem.at[i]) for i in range(W_PARTS)]
    wo_copy = pltpu.make_async_copy(wout_hbm, wo_buf, wo_sem)
    for copy in small_copies[:3] + w_copies + small_copies[3:]:
        copy.start()

    def fetch(i):
        rows = pl.ds(i * BB, BB)
        return (pltpu.make_async_copy(k_hbm.at[rows], k_buf.at[rows], k_sem.at[i]),
                pltpu.make_async_copy(v_hbm.at[rows], v_buf.at[rows], v_sem.at[i]))

    def flush(i):
        rows = pl.ds(i * BB, BB)
        return (pltpu.make_async_copy(k_buf.at[rows], ko_hbm.at[rows], ko_sem.at[i]),
                pltpu.make_async_copy(v_buf.at[rows], vo_hbm.at[rows], vo_sem.at[i]))

    def fetch_start(i):
        for copy in fetch(i):
            copy.start()

    for i in range(AHEAD):
        fetch_start(i)

    for copy in small_copies:
        copy.wait()
    normed = normalize(hid_ref[...].astype(F32), row_of(scale_ref), row_of(bias_ref))
    for copy in w_copies:
        copy.wait()
    fetch_start(AHEAD)
    qkv = jnp.dot(normed, w_buf[...], preferred_element_type=F32) + row_of(bqkv_ref)
    qkv = qkv.astype(BF16).astype(F32)
    qkv = jnp.concatenate([qkv, jnp.zeros((128 - n_rows, qkv.shape[1]), F32)], axis=0)
    feats = qkv.T
    cos_t = jnp.concatenate([cos_ref[...], jnp.zeros((32, 128 - n_rows), F32)], axis=1)
    sin_t = jnp.concatenate([sin_ref[...], jnp.zeros((32, 128 - n_rows), F32)], axis=1)

    def rotate(base):
        u, w = feats[base:base + 32], feats[base + 32:base + 64]
        return jnp.concatenate([u * cos_t - w * sin_t, w * cos_t + u * sin_t], axis=0).astype(BF16).astype(F32)

    zeros = jnp.zeros((64, 128), F32)
    for g in range(2):
        for j in range(3):
            q_rot = rotate(g * 320 + j * 64)
            both = jnp.concatenate([q_rot, zeros] if g == 0 else [zeros, q_rot], axis=0)
            q_buf[pl.ds(g * 3 + j, n_rows, stride=8), :] = both.T[:n_rows]
    for r in (6, 7):
        q_buf[pl.ds(r, n_rows, stride=8), :] = jnp.zeros((n_rows, 128), F32)
    k_new = jnp.concatenate([rotate(192), rotate(320 + 192)], axis=0)
    v_new = jnp.concatenate([feats[256:320], feats[320 + 256:320 + 320]], axis=0)
    for i in range(n_blocks):
        kn_buf[i] = k_new if i == 0 else pltpu.roll(k_new, 128 - i * BB, 1)
        vn_buf[i] = v_new if i == 0 else pltpu.roll(v_new, 128 - i * BB, 1)

    def block(i, carry):
        for copy in fetch(i):
            copy.wait()

        @pl.when(i + AHEAD + 1 < n_blocks)
        def _():
            fetch_start(i + AHEAD + 1)

        @pl.when(i == n_blocks - AHEAD - 1)
        def _():
            wo_copy.start()

        k_cols, v_cols = kn_buf[i], vn_buf[i]
        lane = lax.broadcasted_iota(jnp.int32, (128, 128), 1)
        position = lax.broadcasted_iota(jnp.int32, (8, s_max), 1)
        scores = []
        for j in range(BB):
            b = i * BB + j
            pos = lens_ref[b]
            first = pl.multiple_of((pos // 128) * 128, 128)
            hit = lane == pos - first
            window = pl.ds(first, 128)
            k_buf[b, :, window] = jnp.where(hit, k_cols[:, j:j + 1], k_buf[b, :, window].astype(F32)).astype(BF16)
            v_buf[b, :, window] = jnp.where(hit, v_cols[:, j:j + 1], v_buf[b, :, window].astype(F32)).astype(BF16)
            rows = pl.ds(pl.multiple_of(b * 8, 8), 8)
            one = jnp.dot(q_buf[rows, :].astype(BF16), k_buf[b], preferred_element_type=F32) * 0.125
            scores.append(jnp.where(position <= pos, one, -jnp.inf))
        scores = jnp.concatenate(scores, axis=0)
        top = jnp.max(scores, axis=1, keepdims=True)
        weights = jnp.exp(scores - top)
        probs = weights * (1.0 / jnp.sum(weights, axis=1, keepdims=True))
        for j in range(BB):
            b = i * BB + j
            rows = pl.ds(pl.multiple_of(b * 8, 8), 8)
            c_buf[rows, :] = lax.dot_general(probs[j * 8:j * 8 + 8].astype(BF16), v_buf[b], NT, preferred_element_type=F32)
        for copy in flush(i):
            copy.start()
        return carry

    lax.fori_loop(0, n_blocks, block, 0)
    heads = [c_buf[pl.ds(r, n_rows, stride=8), :] for r in range(6)]
    low = lax.broadcasted_iota(jnp.int32, (n_rows, 128), 1) < 64
    ctx = jnp.concatenate([
        jnp.where(low, heads[0], pltpu.roll(heads[1], 64, 1)),
        jnp.where(low, heads[2], heads[3]),
        jnp.where(low, pltpu.roll(heads[4], 64, 1), heads[5]),
    ], axis=1).astype(BF16)
    wo_copy.wait()
    part_ref[...] = jnp.dot(ctx, wo_buf[...], preferred_element_type=F32).astype(BF16)
    for i in range(n_blocks):
        for copy in flush(i):
            copy.wait()


def moe_kernel(hid_ref, part_ref, bout_ref, scale_ref, bias_ref, wr_ref, ids_ref, wg_hbm, wu_hbm, wd_hbm, out_ref,
               wgu, wd, wr, rs_recv, x1, h2, ids_buf, act, own_p, y_p, hi0, hi1, d0, d1, y_send, y_recv,
               t_f, t_b, z_recv, o_buf, wsem, ssem, rsem):
    z, ep = lax.axis_index("tp"), lax.axis_index("ep")
    n_rows, d_model = hid_ref.shape
    n_exp = wgu.shape[0]
    width = d_model // COLS
    z_peers = [lax.rem(z + dz, 4) for dz in (1, 2, 3)]
    y_peer = lax.rem(ep + 2, 4)
    partner = ep + 1 - 2 * lax.rem(ep, 2)
    diagonal = 3 - ep
    barrier = pltpu.get_barrier_semaphore()
    for peer in z_peers:
        pl.semaphore_signal(barrier, inc=1, device_id={"tp": peer}, device_id_type=MESH)
    for peer in (y_peer, partner, diagonal):
        pl.semaphore_signal(barrier, inc=1, device_id={"ep": peer}, device_id_type=MESH)

    loads = []
    for e in range(n_exp):
        loads.append(pltpu.make_async_copy(wg_hbm.at[e], wgu.at[e, :, 0:128], wsem.at[2 * e]))
        loads.append(pltpu.make_async_copy(wu_hbm.at[e], wgu.at[e, :, 128:256], wsem.at[2 * e + 1]))
    loads.append(pltpu.make_async_copy(wd_hbm, wd, wsem.at[2 * n_exp]))
    for load in loads:
        load.start()

    count = [0]

    def remote(src, dst, device):
        slot = count[0]
        count[0] += 1
        return pltpu.make_async_remote_copy(src_ref=src, dst_ref=dst, send_sem=ssem.at[slot], recv_sem=rsem.at[slot],
                                            device_id=device, device_id_type=MESH)

    def at(index, h, shard=0):
        return pl.ds(pl.multiple_of(shard * n_rows + index * 16 + h * PIECE, PIECE), PIECE)

    def rows_at(index):
        return pl.ds(pl.multiple_of(index * 16, 16), 16)

    def cols(n):
        return pl.ds(n * width, width)

    halves = range(16 // PIECE)
    z_order = [z] + [lax.rem(z + 4 - dz, 4) for dz in (1, 2, 3)]
    rs = [[remote(part_ref.at[at(z_peers[dz], h)], rs_recv.at[dz, pl.ds(h * PIECE, PIECE)], {"tp": z_peers[dz]}) for dz in range(3)] for h in halves]
    to_z = [[remote(h2.at[at(z, h)], h2.at[at(z, h)], {"tp": z_peers[dz]}) for dz in range(3)] for h in halves]
    to_p = [[remote(h2.at[at(z_order[k], h)], h2.at[at(z_order[k], h, 1)], {"ep": partner}) for k in range(4)] for h in halves]
    to_y = [[remote(h2.at[at(z_order[k], h)], h2.at[at(z_order[k], h, 2)], {"ep": y_peer}) for k in range(4)] for h in halves]
    y_to_p = [[remote(h2.at[at(z_order[k], h, 2)], h2.at[at(z_order[k], h, 3)], {"ep": partner}) for k in range(4)] for h in halves]
    mine = rows_at(z)
    to_ids = [remote(ids_ref, ids_buf.at[i + 1], {"ep": peer}) for i, peer in enumerate((partner, y_peer, diagonal))]
    chunks = range(COLS)
    to_d0 = [remote(hi0.at[n], d0.at[n], {"ep": partner}) for n in chunks]
    to_d = [remote(hi1.at[n], d1.at[n], {"ep": partner}) for n in chunks]
    to_yy = [remote(y_send.at[n], y_recv.at[n], {"ep": y_peer}) for n in chunks]
    to_zz = [[remote(t_b.at[n, rows_at(z_peers[dz])], z_recv.at[n, dz], {"tp": z_peers[dz]}) for dz in range(3)] for n in chunks]
    to_o = [[remote(o_buf.at[n, mine], o_buf.at[n, mine], {"tp": z_peers[dz]}) for dz in range(3)] for n in chunks]

    scale, bias, bout = row_of(scale_ref), row_of(bias_ref), row_of(bout_ref)
    ids_buf[0] = ids_ref[...]
    wr[...] = jnp.concatenate([wr_ref[...], jnp.zeros((128 - wr_ref.shape[0], d_model), BF16)], axis=0)
    pl.semaphore_wait(barrier, 6)

    for h in halves:
        for dz in range(3):
            rs[h][dz].start()
    for copy in to_ids:
        copy.start()
    for h in halves:
        for dz in range(3):
            rs[h][dz].wait_recv()
        got = pl.ds(h * PIECE, PIECE)
        total = part_ref[at(z, h), :].astype(F32) + rs_recv[0, got].astype(F32) + rs_recv[1, got].astype(F32) + rs_recv[2, got].astype(F32)
        row = (hid_ref[at(z, h), :].astype(F32) + total + bout).astype(BF16)
        x1[got, :] = row.astype(F32)
        h2[at(z, h), :] = normalize(row.astype(F32), scale, bias)
        for dz in range(3):
            to_z[h][dz].start()
        to_y[h][0].start()
        to_p[h][0].start()

    def relay(h, k):
        to_y[h][k].wait_recv()
        y_to_p[h][k].start()

    for h in halves:
        for dz in range(3):
            to_z[h][dz].wait_recv()
            to_y[h][dz + 1].start()
            to_p[h][dz + 1].start()
        relay(h, 0)

    def masks(shard):
        picks = ids_buf[shard]
        expert = lax.broadcasted_iota(jnp.int32, (128, n_rows), 0)
        hit = jnp.zeros((128, n_rows), F32)
        for k in range(picks.shape[0]):
            hit = jnp.where(expert == picks[k:k + 1, :], 1.0, hit)
        return hit.T

    def toks(shard):
        return h2[shard * n_rows:(shard + 1) * n_rows, :]

    def gates_of(shard):
        logits = lax.dot_general(toks(shard), wr[...], NT, preferred_element_type=F32)
        logits = jnp.where(masks(shard) > 0.5, logits, -jnp.inf)
        shifted = jnp.exp(logits - jnp.max(logits, axis=1, keepdims=True))
        gates = (shifted / jnp.sum(shifted, axis=1, keepdims=True)).astype(BF16).astype(F32)
        return pltpu.roll(gates, lax.rem(128 - ep * n_exp, 128), 1)

    def up(shard, gates, first, last):
        rows = toks(shard)
        for e in range(first, last):
            if shard == 0:
                loads[2 * e].wait()
                loads[2 * e + 1].wait()
            pre = jnp.dot(rows, wgu[e], preferred_element_type=F32)
            gate_pre, up_pre = pre[:, :128], pre[:, 128:]
            hidden = (gate_pre * jax.nn.sigmoid(gate_pre) * up_pre).astype(BF16).astype(F32)
            act[shard * n_rows:(shard + 1) * n_rows, e * 128:(e + 1) * 128] = (hidden * gates[:, e:e + 1]).astype(BF16)

    for copy in to_ids:
        copy.wait_recv()
    up(0, gates_of(0), 0, n_exp)
    for h in halves:
        for copy in to_p[h]:
            copy.wait_recv()
    up(1, gates_of(1), 0, n_exp)
    for h in halves:
        for k in (1, 2, 3):
            relay(h, k)
    up(2, gates_of(2), 0, n_exp)
    for h in halves:
        for copy in y_to_p[h]:
            copy.wait_recv()
    up(3, gates_of(3), 0, n_exp)
    loads[-1].wait()

    def reduce_pair(n):
        to_d[n].wait_recv()
        y_send[n] = (y_p[n] + d1[n].astype(F32)).astype(BF16)
        to_yy[n].start()

    for n in chunks:
        both = jnp.dot(act[128:256, :], wd[:, cols(n)], preferred_element_type=F32)
        y_p[n] = both[0:64]
        hi1[n] = both[64:128].astype(BF16)
        to_d[n].start()
        if n > 0:
            reduce_pair(n - 1)
        both = jnp.dot(act[0:128, :], wd[:, cols(n)], preferred_element_type=F32)
        own_p[n] = both[0:64]
        hi0[n] = both[64:128].astype(BF16)
        to_d0[n].start()
    reduce_pair(COLS - 1)
    for n in chunks:
        to_d0[n].wait_recv()
        to_yy[n].wait_recv()
        t = own_p[n] + d0[n].astype(F32) + y_recv[n].astype(F32)
        t_f[n] = t
        t_b[n] = t.astype(BF16)
        for copy in to_zz[n]:
            copy.start()
    for n in chunks:
        for copy in to_zz[n]:
            copy.wait_recv()
        moe = t_f[n, mine, :] + z_recv[n, 0].astype(F32) + z_recv[n, 1].astype(F32) + z_recv[n, 2].astype(F32)
        o_buf[n, mine, :] = (x1[:, cols(n)] + moe).astype(BF16)
        for copy in to_o[n]:
            copy.start()
    for n in chunks:
        for copy in to_o[n]:
            copy.wait_recv()
        out_ref[:, cols(n)] = o_buf[n]
    for group in rs + to_z + to_p + to_y + y_to_p + [to_ids, to_d0, to_d, to_yy] + to_zz + to_o:
        for copy in group:
            copy.wait_send()


N_SLOTS = (16 // PIECE) * 18 + 3 + 9 * COLS


def solution(mesh):
    token_rows = P(('dp', 'ep'), None)
    token_vec = P(('dp', 'ep'))
    cache_spec = P(('dp', 'ep'), None, 'tp', None)
    expert_in = P('ep', None, 'tp')
    expert_down = P('ep', 'tp', None)
    vm = pl.BlockSpec(memory_space=pltpu.VMEM)
    anyspace = pl.BlockSpec(memory_space=pl.ANY)

    def device_step(hidden, seq_lens, rope_cos, rope_sin, ln1_scale, ln1_bias, w_qkv, b_qkv, w_out, b_out, k_cache, v_cache, ln2_scale, ln2_bias, w_router, expert_ids, w_gate, w_up, w_down):
        n, d = hidden.shape
        _, s_max, groups, head = k_cache.shape
        feat = groups * head
        n_exp = w_gate.shape[0]
        k_in = k_cache.transpose(0, 2, 3, 1).reshape(n, feat, s_max)
        v_in = v_cache.transpose(0, 2, 3, 1).reshape(n, feat, s_max)
        part, k_out, v_out = pl.pallas_call(
            attention_kernel,
            out_shape=(pltpu.VMEM((n, d), BF16), jax.ShapeDtypeStruct(k_in.shape, BF16), jax.ShapeDtypeStruct(v_in.shape, BF16)),
            in_specs=[anyspace] * 11,
            out_specs=(vm, anyspace, anyspace),
            scratch_shapes=[
                pltpu.SMEM((n,), jnp.int32), pltpu.VMEM((n, d), BF16), pltpu.VMEM((32, n), F32), pltpu.VMEM((32, n), F32),
                pltpu.VMEM((d,), BF16), pltpu.VMEM((d,), BF16), pltpu.VMEM(b_qkv.shape, BF16),
                pltpu.VMEM(k_in.shape, BF16), pltpu.VMEM(v_in.shape, BF16), pltpu.VMEM(w_qkv.shape, BF16), pltpu.VMEM(w_out.shape, BF16),
                pltpu.VMEM((n * 8, 128), F32), pltpu.VMEM((n // BB, 128, 128), F32), pltpu.VMEM((n // BB, 128, 128), F32), pltpu.VMEM((n * 8, 128), F32),
                pltpu.SemaphoreType.DMA((7,)), pltpu.SemaphoreType.DMA((W_PARTS,)), pltpu.SemaphoreType.DMA, pltpu.SemaphoreType.DMA((n // BB,)), pltpu.SemaphoreType.DMA((n // BB,)),
                pltpu.SemaphoreType.DMA((n // BB,)), pltpu.SemaphoreType.DMA((n // BB,)),
            ],
            compiler_params=pltpu.CompilerParams(vmem_limit_bytes=VMEM_LIMIT),
            name="attention",
        )(seq_lens, hidden, rope_cos.T, rope_sin.T, ln1_scale, ln1_bias, b_qkv, w_qkv, w_out, k_in, v_in)
        part = pltpu.with_memory_space_constraint(part, pltpu.VMEM)
        in_hbm = lambda w: pltpu.with_memory_space_constraint(w, pltpu.HBM)
        rows = lambda r, t: pltpu.VMEM((r, d), t)
        cut = lambda r, t: pltpu.VMEM((COLS, r, d // COLS), t)
        hidden_out = pl.pallas_call(
            moe_kernel,
            out_shape=pltpu.VMEM((n, d), BF16),
            in_specs=[vm] * 7 + [anyspace] * 3,
            out_specs=vm,
            scratch_shapes=[
                pltpu.VMEM((n_exp, d, 256), BF16), pltpu.VMEM((n_exp * 128, d), BF16), rows(128, BF16),
                pltpu.VMEM((3, 16, d), BF16), rows(16, F32), rows(256, BF16), pltpu.VMEM((4, 8, n), jnp.int32), pltpu.VMEM((256, n_exp * 128), BF16),
                cut(64, F32), cut(64, F32), cut(64, BF16), cut(64, BF16), cut(64, BF16), cut(64, BF16), cut(64, BF16), cut(64, BF16),
                cut(64, F32), cut(64, BF16), pltpu.VMEM((COLS, 3, 16, d // COLS), BF16), cut(64, BF16),
                pltpu.SemaphoreType.DMA((2 * n_exp + 1,)), pltpu.SemaphoreType.DMA((N_SLOTS,)), pltpu.SemaphoreType.DMA((N_SLOTS,)),
            ],
            compiler_params=pltpu.CompilerParams(vmem_limit_bytes=MOE_LIMIT, collective_id=0, has_side_effects=True),
            name="moe",
        )(hidden, part, b_out, ln2_scale, ln2_bias, w_router.T, expert_ids.T, in_hbm(w_gate), in_hbm(w_up), in_hbm(w_down.reshape(n_exp * 128, d)))
        unfold = lambda c: c.reshape(n, groups, head, s_max).transpose(0, 3, 1, 2)
        return hidden_out, unfold(k_out), unfold(v_out)

    in_specs = (token_rows, token_vec, token_rows, token_rows, P(), P(), P(None, 'tp'), P('tp'), P('tp', None), P(), cache_spec, cache_spec, P(), P(), P(), token_rows, expert_in, expert_in, expert_down)
    return jax.shard_map(device_step, mesh=mesh, in_specs=in_specs, out_specs=(token_rows, cache_spec, cache_spec), check_vma=False)
```

```python
import functools

import jax
import jax.numpy as jnp
from jax import lax
from jax.experimental import pallas as pl
from jax.experimental.pallas import tpu as pltpu
from jax.sharding import PartitionSpec as P

EPS = 1e-5
F32 = jnp.float32
BF16 = jnp.bfloat16
MESH = pl.DeviceIdType.MESH
VMEM_LIMIT = 66_400_000
MOE_LIMIT = 40_000_000
NT = (((1,), (1,)), ((), ()))
BB = 8
COLS = 3
PIECE = 16
AHEAD = 6
W_PARTS = 4


def normalize(vals_f32, ln_scale, ln_bias):
    row_mean = jnp.mean(vals_f32, axis=-1, keepdims=True)
    centered = vals_f32 - row_mean
    row_var = jnp.mean(centered * centered, axis=-1, keepdims=True)
    normed = centered * lax.rsqrt(row_var + EPS)
    return (normed * ln_scale + ln_bias).astype(BF16)


def row_of(vec_ref):
    return vec_ref[...].astype(F32)[None, :]


def attention_kernel(lens_hbm, hid_hbm, cos_hbm, sin_hbm, scale_hbm, bias_hbm, bqkv_hbm, wqkv_hbm, wout_hbm, k_hbm, v_hbm,
                     part_ref, ko_hbm, vo_hbm, lens_ref, hid_ref, cos_ref, sin_ref, scale_ref, bias_ref, bqkv_ref,
                     k_buf, v_buf, w_buf, wo_buf, q_buf, kn_buf, vn_buf, c_buf, in_sem, w_sem, wo_sem, k_sem, v_sem, ko_sem, vo_sem):
    n_rows = hid_ref.shape[0]
    n_blocks = n_rows // BB
    s_max = k_buf.shape[2]
    smalls = ((hid_hbm, hid_ref), (scale_hbm, scale_ref), (bias_hbm, bias_ref), (bqkv_hbm, bqkv_ref), (cos_hbm, cos_ref), (sin_hbm, sin_ref),
              (lens_hbm, lens_ref))
    small_copies = [pltpu.make_async_copy(src, dst, in_sem.at[i]) for i, (src, dst) in enumerate(smalls)]
    w_rows = w_buf.shape[0] // W_PARTS
    w_copies = [pltpu.make_async_copy(wqkv_hbm.at[pl.ds(i * w_rows, w_rows)], w_buf.at[pl.ds(i * w_rows, w_rows)], w_sem.at[i]) for i in range(W_PARTS)]
    wo_copy = pltpu.make_async_copy(wout_hbm, wo_buf, wo_sem)
    for copy in small_copies[:3] + w_copies + small_copies[3:]:
        copy.start()

    def fetch(i):
        rows = pl.ds(i * BB, BB)
        return (pltpu.make_async_copy(k_hbm.at[rows], k_buf.at[rows], k_sem.at[i]),
                pltpu.make_async_copy(v_hbm.at[rows], v_buf.at[rows], v_sem.at[i]))

    def flush(i):
        rows = pl.ds(i * BB, BB)
        return (pltpu.make_async_copy(k_buf.at[rows], ko_hbm.at[rows], ko_sem.at[i]),
                pltpu.make_async_copy(v_buf.at[rows], vo_hbm.at[rows], vo_sem.at[i]))

    def fetch_start(i):
        for copy in fetch(i):
            copy.start()

    for i in range(AHEAD):
        fetch_start(i)

    for copy in small_copies:
        copy.wait()
    normed = normalize(hid_ref[...].astype(F32), row_of(scale_ref), row_of(bias_ref))
    for copy in w_copies:
        copy.wait()
    fetch_start(AHEAD)
    qkv = jnp.dot(normed, w_buf[...], preferred_element_type=F32) + row_of(bqkv_ref)
    qkv = qkv.astype(BF16).astype(F32)
    qkv = jnp.concatenate([qkv, jnp.zeros((128 - n_rows, qkv.shape[1]), F32)], axis=0)
    feats = qkv.T
    cos_t = jnp.concatenate([cos_ref[...], jnp.zeros((32, 128 - n_rows), F32)], axis=1)
    sin_t = jnp.concatenate([sin_ref[...], jnp.zeros((32, 128 - n_rows), F32)], axis=1)

    def rotate(base):
        u, w = feats[base:base + 32], feats[base + 32:base + 64]
        return jnp.concatenate([u * cos_t - w * sin_t, w * cos_t + u * sin_t], axis=0).astype(BF16).astype(F32)

    zeros = jnp.zeros((64, 128), F32)
    for g in range(2):
        for j in range(3):
            q_rot = rotate(g * 320 + j * 64)
            both = jnp.concatenate([q_rot, zeros] if g == 0 else [zeros, q_rot], axis=0)
            q_buf[pl.ds(g * 3 + j, n_rows, stride=8), :] = both.T[:n_rows]
    for r in (6, 7):
        q_buf[pl.ds(r, n_rows, stride=8), :] = jnp.zeros((n_rows, 128), F32)
    k_new = jnp.concatenate([rotate(192), rotate(320 + 192)], axis=0)
    v_new = jnp.concatenate([feats[256:320], feats[320 + 256:320 + 320]], axis=0)
    for i in range(n_blocks):
        kn_buf[i] = k_new if i == 0 else pltpu.roll(k_new, 128 - i * BB, 1)
        vn_buf[i] = v_new if i == 0 else pltpu.roll(v_new, 128 - i * BB, 1)

    def block(i, carry):
        for copy in fetch(i):
            copy.wait()

        @pl.when(i + AHEAD + 1 < n_blocks)
        def _():
            fetch_start(i + AHEAD + 1)

        @pl.when(i == n_blocks - AHEAD - 1)
        def _():
            wo_copy.start()

        k_cols, v_cols = kn_buf[i], vn_buf[i]
        lane = lax.broadcasted_iota(jnp.int32, (128, 128), 1)
        position = lax.broadcasted_iota(jnp.int32, (8, s_max), 1)
        scores = []
        for j in range(BB):
            b = i * BB + j
            pos = lens_ref[b]
            first = pl.multiple_of((pos // 128) * 128, 128)
            hit = lane == pos - first
            window = pl.ds(first, 128)
            k_buf[b, :, window] = jnp.where(hit, k_cols[:, j:j + 1], k_buf[b, :, window].astype(F32)).astype(BF16)
            v_buf[b, :, window] = jnp.where(hit, v_cols[:, j:j + 1], v_buf[b, :, window].astype(F32)).astype(BF16)
            rows = pl.ds(pl.multiple_of(b * 8, 8), 8)
            one = jnp.dot(q_buf[rows, :].astype(BF16), k_buf[b], preferred_element_type=F32) * 0.125
            scores.append(jnp.where(position <= pos, one, -jnp.inf))
        scores = jnp.concatenate(scores, axis=0)
        top = jnp.max(scores, axis=1, keepdims=True)
        weights = jnp.exp(scores - top)
        probs = weights * (1.0 / jnp.sum(weights, axis=1, keepdims=True))
        for j in range(BB):
            b = i * BB + j
            rows = pl.ds(pl.multiple_of(b * 8, 8), 8)
            c_buf[rows, :] = lax.dot_general(probs[j * 8:j * 8 + 8].astype(BF16), v_buf[b], NT, preferred_element_type=F32)
        for copy in flush(i):
            copy.start()
        return carry

    lax.fori_loop(0, n_blocks, block, 0)
    heads = [c_buf[pl.ds(r, n_rows, stride=8), :] for r in range(6)]
    low = lax.broadcasted_iota(jnp.int32, (n_rows, 128), 1) < 64
    ctx = jnp.concatenate([
        jnp.where(low, heads[0], pltpu.roll(heads[1], 64, 1)),
        jnp.where(low, heads[2], heads[3]),
        jnp.where(low, pltpu.roll(heads[4], 64, 1), heads[5]),
    ], axis=1).astype(BF16)
    wo_copy.wait()
    part_ref[...] = jnp.dot(ctx, wo_buf[...], preferred_element_type=F32).astype(BF16)
    for i in range(n_blocks):
        for copy in flush(i):
            copy.wait()


def moe_kernel(hid_ref, part_ref, bout_ref, scale_ref, bias_ref, wr_ref, ids_ref, wg_hbm, wu_hbm, wd_hbm, out_ref,
               wgu, wd, wr, rs_recv, x1, h2, ids_buf, act, own_p, y_p, hi0, hi1, d0, d1, y_send, y_recv,
               t_f, t_b, z_recv, o_buf, wsem, ssem, rsem):
    z, ep = lax.axis_index("tp"), lax.axis_index("ep")
    n_rows, d_model = hid_ref.shape
    n_exp = wgu.shape[0]
    width = d_model // COLS
    z_peers = [lax.rem(z + dz, 4) for dz in (1, 2, 3)]
    y_peer = lax.rem(ep + 2, 4)
    partner = ep + 1 - 2 * lax.rem(ep, 2)
    diagonal = 3 - ep
    barrier = pltpu.get_barrier_semaphore()
    for peer in z_peers:
        pl.semaphore_signal(barrier, inc=1, device_id={"tp": peer}, device_id_type=MESH)
    for peer in (y_peer, partner, diagonal):
        pl.semaphore_signal(barrier, inc=1, device_id={"ep": peer}, device_id_type=MESH)

    loads = []
    for e in range(n_exp):
        loads.append(pltpu.make_async_copy(wg_hbm.at[e], wgu.at[e, :, 0:128], wsem.at[2 * e]))
        loads.append(pltpu.make_async_copy(wu_hbm.at[e], wgu.at[e, :, 128:256], wsem.at[2 * e + 1]))
    loads.append(pltpu.make_async_copy(wd_hbm, wd, wsem.at[2 * n_exp]))
    for load in loads:
        load.start()

    count = [0]

    def remote(src, dst, device):
        slot = count[0]
        count[0] += 1
        return pltpu.make_async_remote_copy(src_ref=src, dst_ref=dst, send_sem=ssem.at[slot], recv_sem=rsem.at[slot],
                                            device_id=device, device_id_type=MESH)

    def at(index, h, shard=0):
        return pl.ds(pl.multiple_of(shard * n_rows + index * 16 + h * PIECE, PIECE), PIECE)

    def rows_at(index):
        return pl.ds(pl.multiple_of(index * 16, 16), 16)

    def cols(n):
        return pl.ds(n * width, width)

    halves = range(16 // PIECE)
    z_order = [z] + [lax.rem(z + 4 - dz, 4) for dz in (1, 2, 3)]
    rs = [[remote(part_ref.at[at(z_peers[dz], h)], rs_recv.at[dz, pl.ds(h * PIECE, PIECE)], {"tp": z_peers[dz]}) for dz in range(3)] for h in halves]
    to_z = [[remote(h2.at[at(z, h)], h2.at[at(z, h)], {"tp": z_peers[dz]}) for dz in range(3)] for h in halves]
    to_p = [[remote(h2.at[at(z_order[k], h)], h2.at[at(z_order[k], h, 1)], {"ep": partner}) for k in range(4)] for h in halves]
    to_y = [[remote(h2.at[at(z_order[k], h)], h2.at[at(z_order[k], h, 2)], {"ep": y_peer}) for k in range(4)] for h in halves]
    y_to_p = [[remote(h2.at[at(z_order[k], h, 2)], h2.at[at(z_order[k], h, 3)], {"ep": partner}) for k in range(4)] for h in halves]
    mine = rows_at(z)
    to_ids = [remote(ids_ref, ids_buf.at[i + 1], {"ep": peer}) for i, peer in enumerate((partner, y_peer, diagonal))]
    chunks = range(COLS)
    to_d0 = [remote(hi0.at[n], d0.at[n], {"ep": partner}) for n in chunks]
    to_d = [remote(hi1.at[n], d1.at[n], {"ep": partner}) for n in chunks]
    to_yy = [remote(y_send.at[n], y_recv.at[n], {"ep": y_peer}) for n in chunks]
    to_zz = [[remote(t_b.at[n, rows_at(z_peers[dz])], z_recv.at[n, dz], {"tp": z_peers[dz]}) for dz in range(3)] for n in chunks]
    to_o = [[remote(o_buf.at[n, mine], o_buf.at[n, mine], {"tp": z_peers[dz]}) for dz in range(3)] for n in chunks]

    scale, bias, bout = row_of(scale_ref), row_of(bias_ref), row_of(bout_ref)
    ids_buf[0] = ids_ref[...]
    wr[...] = jnp.concatenate([wr_ref[...], jnp.zeros((128 - wr_ref.shape[0], d_model), BF16)], axis=0)
    pl.semaphore_wait(barrier, 6)

    for h in halves:
        for dz in range(3):
            rs[h][dz].start()
    for copy in to_ids:
        copy.start()
    for h in halves:
        for dz in range(3):
            rs[h][dz].wait_recv()
        got = pl.ds(h * PIECE, PIECE)
        total = part_ref[at(z, h), :].astype(F32) + rs_recv[0, got].astype(F32) + rs_recv[1, got].astype(F32) + rs_recv[2, got].astype(F32)
        row = (hid_ref[at(z, h), :].astype(F32) + total + bout).astype(BF16)
        x1[got, :] = row.astype(F32)
        h2[at(z, h), :] = normalize(row.astype(F32), scale, bias)
        for dz in range(3):
            to_z[h][dz].start()
        to_y[h][0].start()
        to_p[h][0].start()

    def relay(h, k):
        to_y[h][k].wait_recv()
        y_to_p[h][k].start()

    for h in halves:
        for dz in range(3):
            to_z[h][dz].wait_recv()
            to_y[h][dz + 1].start()
            to_p[h][dz + 1].start()
        relay(h, 0)

    def masks(shard):
        picks = ids_buf[shard]
        expert = lax.broadcasted_iota(jnp.int32, (128, n_rows), 0)
        hit = jnp.zeros((128, n_rows), F32)
        for k in range(picks.shape[0]):
            hit = jnp.where(expert == picks[k:k + 1, :], 1.0, hit)
        return hit.T

    def toks(shard):
        return h2[shard * n_rows:(shard + 1) * n_rows, :]

    def gates_of(shard):
        logits = lax.dot_general(toks(shard), wr[...], NT, preferred_element_type=F32)
        logits = jnp.where(masks(shard) > 0.5, logits, -jnp.inf)
        shifted = jnp.exp(logits - jnp.max(logits, axis=1, keepdims=True))
        gates = (shifted / jnp.sum(shifted, axis=1, keepdims=True)).astype(BF16).astype(F32)
        return pltpu.roll(gates, lax.rem(128 - ep * n_exp, 128), 1)

    def up(shard, gates, first, last):
        rows = toks(shard)
        for e in range(first, last):
            if shard == 0:
                loads[2 * e].wait()
                loads[2 * e + 1].wait()
            pre = jnp.dot(rows, wgu[e], preferred_element_type=F32)
            gate_pre, up_pre = pre[:, :128], pre[:, 128:]
            hidden = (gate_pre * jax.nn.sigmoid(gate_pre) * up_pre).astype(BF16).astype(F32)
            act[shard * n_rows:(shard + 1) * n_rows, e * 128:(e + 1) * 128] = (hidden * gates[:, e:e + 1]).astype(BF16)

    for copy in to_ids:
        copy.wait_recv()
    up(0, gates_of(0), 0, n_exp)
    for h in halves:
        for copy in to_p[h]:
            copy.wait_recv()
    up(1, gates_of(1), 0, n_exp)
    for h in halves:
        for k in (1, 2, 3):
            relay(h, k)
    up(2, gates_of(2), 0, n_exp)
    for h in halves:
        for copy in y_to_p[h]:
            copy.wait_recv()
    up(3, gates_of(3), 0, n_exp)
    loads[-1].wait()

    def reduce_pair(n):
        to_d[n].wait_recv()
        y_send[n] = (y_p[n] + d1[n].astype(F32)).astype(BF16)
        to_yy[n].start()

    for n in chunks:
        both = jnp.dot(act[128:256, :], wd[:, cols(n)], preferred_element_type=F32)
        y_p[n] = both[0:64]
        hi1[n] = both[64:128].astype(BF16)
        to_d[n].start()
        if n > 0:
            reduce_pair(n - 1)
        both = jnp.dot(act[0:128, :], wd[:, cols(n)], preferred_element_type=F32)
        own_p[n] = both[0:64]
        hi0[n] = both[64:128].astype(BF16)
        to_d0[n].start()
    reduce_pair(COLS - 1)
    for n in chunks:
        to_d0[n].wait_recv()
        to_yy[n].wait_recv()
        t = own_p[n] + d0[n].astype(F32) + y_recv[n].astype(F32)
        t_f[n] = t
        t_b[n] = t.astype(BF16)
        for copy in to_zz[n]:
            copy.start()
    for n in chunks:
        for copy in to_zz[n]:
            copy.wait_recv()
        moe = t_f[n, mine, :] + z_recv[n, 0].astype(F32) + z_recv[n, 1].astype(F32) + z_recv[n, 2].astype(F32)
        o_buf[n, mine, :] = (x1[:, cols(n)] + moe).astype(BF16)
        for copy in to_o[n]:
            copy.start()
    for n in chunks:
        for copy in to_o[n]:
            copy.wait_recv()
        out_ref[:, cols(n)] = o_buf[n]
    for group in rs + to_z + to_p + to_y + y_to_p + [to_ids, to_d0, to_d, to_yy] + to_zz + to_o:
        for copy in group:
            copy.wait_send()


N_SLOTS = (16 // PIECE) * 18 + 3 + 9 * COLS


def solution(mesh):
    token_rows = P(('dp', 'ep'), None)
    token_vec = P(('dp', 'ep'))
    cache_spec = P(('dp', 'ep'), None, 'tp', None)
    expert_in = P('ep', None, 'tp')
    expert_down = P('ep', 'tp', None)
    vm = pl.BlockSpec(memory_space=pltpu.VMEM)
    anyspace = pl.BlockSpec(memory_space=pl.ANY)

    def device_step(hidden, seq_lens, rope_cos, rope_sin, ln1_scale, ln1_bias, w_qkv, b_qkv, w_out, b_out, k_cache, v_cache, ln2_scale, ln2_bias, w_router, expert_ids, w_gate, w_up, w_down):
        n, d = hidden.shape
        _, s_max, groups, head = k_cache.shape
        feat = groups * head
        n_exp = w_gate.shape[0]
        k_in = k_cache.transpose(0, 2, 3, 1).reshape(n, feat, s_max)
        v_in = v_cache.transpose(0, 2, 3, 1).reshape(n, feat, s_max)
        part, k_out, v_out = pl.pallas_call(
            attention_kernel,
            out_shape=(pltpu.VMEM((n, d), BF16), jax.ShapeDtypeStruct(k_in.shape, BF16), jax.ShapeDtypeStruct(v_in.shape, BF16)),
            in_specs=[anyspace] * 11,
            out_specs=(vm, anyspace, anyspace),
            scratch_shapes=[
                pltpu.SMEM((n,), jnp.int32), pltpu.VMEM((n, d), BF16), pltpu.VMEM((32, n), F32), pltpu.VMEM((32, n), F32),
                pltpu.VMEM((d,), BF16), pltpu.VMEM((d,), BF16), pltpu.VMEM(b_qkv.shape, BF16),
                pltpu.VMEM(k_in.shape, BF16), pltpu.VMEM(v_in.shape, BF16), pltpu.VMEM(w_qkv.shape, BF16), pltpu.VMEM(w_out.shape, BF16),
                pltpu.VMEM((n * 8, 128), F32), pltpu.VMEM((n // BB, 128, 128), F32), pltpu.VMEM((n // BB, 128, 128), F32), pltpu.VMEM((n * 8, 128), F32),
                pltpu.SemaphoreType.DMA((7,)), pltpu.SemaphoreType.DMA((W_PARTS,)), pltpu.SemaphoreType.DMA, pltpu.SemaphoreType.DMA((n // BB,)), pltpu.SemaphoreType.DMA((n // BB,)),
                pltpu.SemaphoreType.DMA((n // BB,)), pltpu.SemaphoreType.DMA((n // BB,)),
            ],
            compiler_params=pltpu.CompilerParams(vmem_limit_bytes=VMEM_LIMIT),
            name="attention",
        )(seq_lens, hidden, rope_cos.T, rope_sin.T, ln1_scale, ln1_bias, b_qkv, w_qkv, w_out, k_in, v_in)
        part = pltpu.with_memory_space_constraint(part, pltpu.VMEM)
        in_hbm = lambda w: pltpu.with_memory_space_constraint(w, pltpu.HBM)
        rows = lambda r, t: pltpu.VMEM((r, d), t)
        cut = lambda r, t: pltpu.VMEM((COLS, r, d // COLS), t)
        hidden_out = pl.pallas_call(
            moe_kernel,
            out_shape=pltpu.VMEM((n, d), BF16),
            in_specs=[vm] * 7 + [anyspace] * 3,
            out_specs=vm,
            scratch_shapes=[
                pltpu.VMEM((n_exp, d, 256), BF16), pltpu.VMEM((n_exp * 128, d), BF16), rows(128, BF16),
                pltpu.VMEM((3, 16, d), BF16), rows(16, F32), rows(256, BF16), pltpu.VMEM((4, 8, n), jnp.int32), pltpu.VMEM((256, n_exp * 128), BF16),
                cut(64, F32), cut(64, F32), cut(64, BF16), cut(64, BF16), cut(64, BF16), cut(64, BF16), cut(64, BF16), cut(64, BF16),
                cut(64, F32), cut(64, BF16), pltpu.VMEM((COLS, 3, 16, d // COLS), BF16), cut(64, BF16),
                pltpu.SemaphoreType.DMA((2 * n_exp + 1,)), pltpu.SemaphoreType.DMA((N_SLOTS,)), pltpu.SemaphoreType.DMA((N_SLOTS,)),
            ],
            compiler_params=pltpu.CompilerParams(vmem_limit_bytes=MOE_LIMIT, collective_id=0, has_side_effects=True),
            name="moe",
        )(hidden, part, b_out, ln2_scale, ln2_bias, w_router.T, expert_ids.T, in_hbm(w_gate), in_hbm(w_up), in_hbm(w_down.reshape(n_exp * 128, d)))
        unfold = lambda c: c.reshape(n, groups, head, s_max).transpose(0, 3, 1, 2)
        return hidden_out, unfold(k_out), unfold(v_out)

    in_specs = (token_rows, token_vec, token_rows, token_rows, P(), P(), P(None, 'tp'), P('tp'), P('tp', None), P(), cache_spec, cache_spec, P(), P(), P(), token_rows, expert_in, expert_in, expert_down)
    return jax.shard_map(device_step, mesh=mesh, in_specs=in_specs, out_specs=(token_rows, cache_spec, cache_spec), check_vma=False)
```

```python
import functools

import jax
import jax.numpy as jnp
from jax import lax
from jax.experimental import pallas as pl
from jax.experimental.pallas import tpu as pltpu
from jax.sharding import PartitionSpec as P

EPS = 1e-5
F32 = jnp.float32
BF16 = jnp.bfloat16
MESH = pl.DeviceIdType.MESH
VMEM_LIMIT = 66_400_000
MOE_LIMIT = 40_000_000
NT = (((1,), (1,)), ((), ()))
BB = 8
COLS = 3
PIECE = 16
AHEAD = 4
W_PARTS = 4


def normalize(vals_f32, ln_scale, ln_bias):
    row_mean = jnp.mean(vals_f32, axis=-1, keepdims=True)
    centered = vals_f32 - row_mean
    row_var = jnp.mean(centered * centered, axis=-1, keepdims=True)
    normed = centered * lax.rsqrt(row_var + EPS)
    return (normed * ln_scale + ln_bias).astype(BF16)


def row_of(vec_ref):
    return vec_ref[...].astype(F32)[None, :]


def attention_kernel(lens_hbm, hid_hbm, cos_hbm, sin_hbm, scale_hbm, bias_hbm, bqkv_hbm, wqkv_hbm, k_hbm, v_hbm,
                     ctx_ref, ko_hbm, vo_hbm, lens_ref, hid_ref, cos_ref, sin_ref, scale_ref, bias_ref, bqkv_ref,
                     k_buf, v_buf, w_buf, q_buf, kn_buf, vn_buf, c_buf, in_sem, w_sem, k_sem, v_sem, ko_sem, vo_sem):
    n_rows = hid_ref.shape[0]
    n_blocks = n_rows // BB
    s_max = k_buf.shape[2]
    smalls = ((hid_hbm, hid_ref), (scale_hbm, scale_ref), (bias_hbm, bias_ref), (bqkv_hbm, bqkv_ref), (cos_hbm, cos_ref), (sin_hbm, sin_ref),
              (lens_hbm, lens_ref))
    small_copies = [pltpu.make_async_copy(src, dst, in_sem.at[i]) for i, (src, dst) in enumerate(smalls)]
    w_rows = w_buf.shape[0] // W_PARTS
    w_copies = [pltpu.make_async_copy(wqkv_hbm.at[pl.ds(i * w_rows, w_rows)], w_buf.at[pl.ds(i * w_rows, w_rows)], w_sem.at[i]) for i in range(W_PARTS)]
    for copy in small_copies[:3] + w_copies + small_copies[3:]:
        copy.start()

    def fetch(i):
        rows = pl.ds(i * BB, BB)
        return (pltpu.make_async_copy(k_hbm.at[rows], k_buf.at[rows], k_sem.at[i]),
                pltpu.make_async_copy(v_hbm.at[rows], v_buf.at[rows], v_sem.at[i]))

    def flush(i):
        rows = pl.ds(i * BB, BB)
        return (pltpu.make_async_copy(k_buf.at[rows], ko_hbm.at[rows], ko_sem.at[i]),
                pltpu.make_async_copy(v_buf.at[rows], vo_hbm.at[rows], vo_sem.at[i]))

    def fetch_start(i):
        for copy in fetch(i):
            copy.start()

    for i in range(AHEAD):
        fetch_start(i)

    for copy in small_copies:
        copy.wait()
    normed = normalize(hid_ref[...].astype(F32), row_of(scale_ref), row_of(bias_ref))
    for copy in w_copies:
        copy.wait()
    fetch_start(AHEAD)
    qkv = jnp.dot(normed, w_buf[...], preferred_element_type=F32) + row_of(bqkv_ref)
    qkv = qkv.astype(BF16).astype(F32)
    qkv = jnp.concatenate([qkv, jnp.zeros((128 - n_rows, qkv.shape[1]), F32)], axis=0)
    feats = qkv.T
    cos_t = jnp.concatenate([cos_ref[...], jnp.zeros((32, 128 - n_rows), F32)], axis=1)
    sin_t = jnp.concatenate([sin_ref[...], jnp.zeros((32, 128 - n_rows), F32)], axis=1)

    def rotate(base):
        u, w = feats[base:base + 32], feats[base + 32:base + 64]
        return jnp.concatenate([u * cos_t - w * sin_t, w * cos_t + u * sin_t], axis=0).astype(BF16).astype(F32)

    zeros = jnp.zeros((64, 128), F32)
    for g in range(2):
        for j in range(3):
            q_rot = rotate(g * 320 + j * 64)
            both = jnp.concatenate([q_rot, zeros] if g == 0 else [zeros, q_rot], axis=0)
            q_buf[pl.ds(g * 3 + j, n_rows, stride=8), :] = both.T[:n_rows]
    for r in (6, 7):
        q_buf[pl.ds(r, n_rows, stride=8), :] = jnp.zeros((n_rows, 128), F32)
    k_new = jnp.concatenate([rotate(192), rotate(320 + 192)], axis=0)
    v_new = jnp.concatenate([feats[256:320], feats[320 + 256:320 + 320]], axis=0)
    for i in range(n_blocks):
        kn_buf[i] = k_new if i == 0 else pltpu.roll(k_new, 128 - i * BB, 1)
        vn_buf[i] = v_new if i == 0 else pltpu.roll(v_new, 128 - i * BB, 1)

    def block(i, carry):
        for copy in fetch(i):
            copy.wait()

        @pl.when(i + AHEAD + 1 < n_blocks)
        def _():
            fetch_start(i + AHEAD + 1)

        k_cols, v_cols = kn_buf[i], vn_buf[i]
        lane = lax.broadcasted_iota(jnp.int32, (128, 128), 1)
        position = lax.broadcasted_iota(jnp.int32, (8, s_max), 1)
        scores = []
        for j in range(BB):
            b = i * BB + j
            pos = lens_ref[b]
            first = pl.multiple_of((pos // 128) * 128, 128)
            hit = lane == pos - first
            window = pl.ds(first, 128)
            k_buf[b, :, window] = jnp.where(hit, k_cols[:, j:j + 1], k_buf[b, :, window].astype(F32)).astype(BF16)
            v_buf[b, :, window] = jnp.where(hit, v_cols[:, j:j + 1], v_buf[b, :, window].astype(F32)).astype(BF16)
            rows = pl.ds(pl.multiple_of(b * 8, 8), 8)
            one = jnp.dot(q_buf[rows, :].astype(BF16), k_buf[b], preferred_element_type=F32) * 0.125
            scores.append(jnp.where(position <= pos, one, -jnp.inf))
        scores = jnp.concatenate(scores, axis=0)
        top = jnp.max(scores, axis=1, keepdims=True)
        weights = jnp.exp(scores - top)
        probs = weights * (1.0 / jnp.sum(weights, axis=1, keepdims=True))
        for j in range(BB):
            b = i * BB + j
            rows = pl.ds(pl.multiple_of(b * 8, 8), 8)
            c_buf[rows, :] = lax.dot_general(probs[j * 8:j * 8 + 8].astype(BF16), v_buf[b], NT, preferred_element_type=F32)
        for copy in flush(i):
            copy.start()
        return carry

    lax.fori_loop(0, n_blocks, block, 0)
    heads = [c_buf[pl.ds(r, n_rows, stride=8), :] for r in range(6)]
    low = lax.broadcasted_iota(jnp.int32, (n_rows, 128), 1) < 64
    ctx_ref[...] = jnp.concatenate([
        jnp.where(low, heads[0], pltpu.roll(heads[1], 64, 1)),
        jnp.where(low, heads[2], heads[3]),
        jnp.where(low, pltpu.roll(heads[4], 64, 1), heads[5]),
    ], axis=1).astype(BF16)
    for i in range(n_blocks):
        for copy in flush(i):
            copy.wait()


def moe_kernel(hid_ref, ctx_ref, bout_ref, scale_ref, bias_ref, wr_ref, ids_ref, wout_hbm, wg_hbm, wu_hbm, wd_hbm, out_ref,
               wout, part_ref, wgu, wd, wr, rs_recv, x1, h2, ids_buf, act, own_p, y_p, hi0, hi1, d0, d1, y_send, y_recv,
               t_f, t_b, z_recv, o_buf, wsem, ssem, rsem):
    z, ep = lax.axis_index("tp"), lax.axis_index("ep")
    n_rows, d_model = hid_ref.shape
    n_exp = wgu.shape[0]
    width = d_model // COLS
    z_peers = [lax.rem(z + dz, 4) for dz in (1, 2, 3)]
    y_peer = lax.rem(ep + 2, 4)
    partner = ep + 1 - 2 * lax.rem(ep, 2)
    diagonal = 3 - ep
    barrier = pltpu.get_barrier_semaphore()
    for peer in z_peers:
        pl.semaphore_signal(barrier, inc=1, device_id={"tp": peer}, device_id_type=MESH)
    for peer in (y_peer, partner, diagonal):
        pl.semaphore_signal(barrier, inc=1, device_id={"ep": peer}, device_id_type=MESH)

    wout_copy = pltpu.make_async_copy(wout_hbm, wout, wsem.at[2 * n_exp + 1])
    wout_copy.start()
    loads = []
    for e in range(n_exp):
        loads.append(pltpu.make_async_copy(wg_hbm.at[e], wgu.at[e, :, 0:128], wsem.at[2 * e]))
        loads.append(pltpu.make_async_copy(wu_hbm.at[e], wgu.at[e, :, 128:256], wsem.at[2 * e + 1]))
    loads.append(pltpu.make_async_copy(wd_hbm, wd, wsem.at[2 * n_exp]))
    wout_copy.wait()
    for load in loads:
        load.start()
    part_ref[...] = jnp.dot(ctx_ref[...], wout[...], preferred_element_type=F32).astype(BF16)

    count = [0]

    def remote(src, dst, device):
        slot = count[0]
        count[0] += 1
        return pltpu.make_async_remote_copy(src_ref=src, dst_ref=dst, send_sem=ssem.at[slot], recv_sem=rsem.at[slot],
                                            device_id=device, device_id_type=MESH)

    def at(index, h, shard=0):
        return pl.ds(pl.multiple_of(shard * n_rows + index * 16 + h * PIECE, PIECE), PIECE)

    def rows_at(index):
        return pl.ds(pl.multiple_of(index * 16, 16), 16)

    def cols(n):
        return pl.ds(n * width, width)

    halves = range(16 // PIECE)
    z_order = [z] + [lax.rem(z + 4 - dz, 4) for dz in (1, 2, 3)]
    rs = [[remote(part_ref.at[at(z_peers[dz], h)], rs_recv.at[dz, pl.ds(h * PIECE, PIECE)], {"tp": z_peers[dz]}) for dz in range(3)] for h in halves]
    to_z = [[remote(h2.at[at(z, h)], h2.at[at(z, h)], {"tp": z_peers[dz]}) for dz in range(3)] for h in halves]
    to_p = [[remote(h2.at[at(z_order[k], h)], h2.at[at(z_order[k], h, 1)], {"ep": partner}) for k in range(4)] for h in halves]
    to_y = [[remote(h2.at[at(z_order[k], h)], h2.at[at(z_order[k], h, 2)], {"ep": y_peer}) for k in range(4)] for h in halves]
    y_to_p = [[remote(h2.at[at(z_order[k], h, 2)], h2.at[at(z_order[k], h, 3)], {"ep": partner}) for k in range(4)] for h in halves]
    mine = rows_at(z)
    to_ids = [remote(ids_ref, ids_buf.at[i + 1], {"ep": peer}) for i, peer in enumerate((partner, y_peer, diagonal))]
    chunks = range(COLS)
    to_d0 = [remote(hi0.at[n], d0.at[n], {"ep": partner}) for n in chunks]
    to_d = [remote(hi1.at[n], d1.at[n], {"ep": partner}) for n in chunks]
    to_yy = [remote(y_send.at[n], y_recv.at[n], {"ep": y_peer}) for n in chunks]
    to_zz = [[remote(t_b.at[n, rows_at(z_peers[dz])], z_recv.at[n, dz], {"tp": z_peers[dz]}) for dz in range(3)] for n in chunks]
    to_o = [[remote(o_buf.at[n, mine], o_buf.at[n, mine], {"tp": z_peers[dz]}) for dz in range(3)] for n in chunks]

    scale, bias, bout = row_of(scale_ref), row_of(bias_ref), row_of(bout_ref)
    ids_buf[0] = ids_ref[...]
    wr[...] = jnp.concatenate([wr_ref[...], jnp.zeros((128 - wr_ref.shape[0], d_model), BF16)], axis=0)
    pl.semaphore_wait(barrier, 6)

    for h in halves:
        for dz in range(3):
            rs[h][dz].start()
    for copy in to_ids:
        copy.start()
    for h in halves:
        for dz in range(3):
            rs[h][dz].wait_recv()
        got = pl.ds(h * PIECE, PIECE)
        total = part_ref[at(z, h), :].astype(F32) + rs_recv[0, got].astype(F32) + rs_recv[1, got].astype(F32) + rs_recv[2, got].astype(F32)
        row = (hid_ref[at(z, h), :].astype(F32) + total + bout).astype(BF16)
        x1[got, :] = row.astype(F32)
        h2[at(z, h), :] = normalize(row.astype(F32), scale, bias)
        for dz in range(3):
            to_z[h][dz].start()
        to_y[h][0].start()
        to_p[h][0].start()

    def relay(h, k):
        to_y[h][k].wait_recv()
        y_to_p[h][k].start()

    for h in halves:
        for dz in range(3):
            to_z[h][dz].wait_recv()
            to_y[h][dz + 1].start()
            to_p[h][dz + 1].start()
        relay(h, 0)

    def masks(shard):
        picks = ids_buf[shard]
        expert = lax.broadcasted_iota(jnp.int32, (128, n_rows), 0)
        hit = jnp.zeros((128, n_rows), F32)
        for k in range(picks.shape[0]):
            hit = jnp.where(expert == picks[k:k + 1, :], 1.0, hit)
        return hit.T

    def toks(shard):
        return h2[shard * n_rows:(shard + 1) * n_rows, :]

    def gates_of(shard):
        logits = lax.dot_general(toks(shard), wr[...], NT, preferred_element_type=F32)
        logits = jnp.where(masks(shard) > 0.5, logits, -jnp.inf)
        shifted = jnp.exp(logits - jnp.max(logits, axis=1, keepdims=True))
        gates = (shifted / jnp.sum(shifted, axis=1, keepdims=True)).astype(BF16).astype(F32)
        return pltpu.roll(gates, lax.rem(128 - ep * n_exp, 128), 1)

    def up(shard, gates, first, last):
        rows = toks(shard)
        for e in range(first, last):
            if shard == 0:
                loads[2 * e].wait()
                loads[2 * e + 1].wait()
            pre = jnp.dot(rows, wgu[e], preferred_element_type=F32)
            gate_pre, up_pre = pre[:, :128], pre[:, 128:]
            hidden = (gate_pre * jax.nn.sigmoid(gate_pre) * up_pre).astype(BF16).astype(F32)
            act[shard * n_rows:(shard + 1) * n_rows, e * 128:(e + 1) * 128] = (hidden * gates[:, e:e + 1]).astype(BF16)

    for copy in to_ids:
        copy.wait_recv()
    up(0, gates_of(0), 0, n_exp)
    for h in halves:
        for copy in to_p[h]:
            copy.wait_recv()
    up(1, gates_of(1), 0, n_exp)
    for h in halves:
        for k in (1, 2, 3):
            relay(h, k)
    up(2, gates_of(2), 0, n_exp)
    for h in halves:
        for copy in y_to_p[h]:
            copy.wait_recv()
    up(3, gates_of(3), 0, n_exp)
    loads[-1].wait()

    def reduce_pair(n):
        to_d[n].wait_recv()
        y_send[n] = (y_p[n] + d1[n].astype(F32)).astype(BF16)
        to_yy[n].start()

    for n in chunks:
        both = jnp.dot(act[128:256, :], wd[:, cols(n)], preferred_element_type=F32)
        y_p[n] = both[0:64]
        hi1[n] = both[64:128].astype(BF16)
        to_d[n].start()
        if n > 0:
            reduce_pair(n - 1)
        both = jnp.dot(act[0:128, :], wd[:, cols(n)], preferred_element_type=F32)
        own_p[n] = both[0:64]
        hi0[n] = both[64:128].astype(BF16)
        to_d0[n].start()
    reduce_pair(COLS - 1)
    for n in chunks:
        to_d0[n].wait_recv()
        to_yy[n].wait_recv()
        t = own_p[n] + d0[n].astype(F32) + y_recv[n].astype(F32)
        t_f[n] = t
        t_b[n] = t.astype(BF16)
        for copy in to_zz[n]:
            copy.start()
    for n in chunks:
        for copy in to_zz[n]:
            copy.wait_recv()
        moe = t_f[n, mine, :] + z_recv[n, 0].astype(F32) + z_recv[n, 1].astype(F32) + z_recv[n, 2].astype(F32)
        o_buf[n, mine, :] = (x1[:, cols(n)] + moe).astype(BF16)
        for copy in to_o[n]:
            copy.start()
    for n in chunks:
        for copy in to_o[n]:
            copy.wait_recv()
        out_ref[:, cols(n)] = o_buf[n]
    for group in rs + to_z + to_p + to_y + y_to_p + [to_ids, to_d0, to_d, to_yy] + to_zz + to_o:
        for copy in group:
            copy.wait_send()


N_SLOTS = (16 // PIECE) * 18 + 3 + 9 * COLS


def solution(mesh):
    token_rows = P(('dp', 'ep'), None)
    token_vec = P(('dp', 'ep'))
    cache_spec = P(('dp', 'ep'), None, 'tp', None)
    expert_in = P('ep', None, 'tp')
    expert_down = P('ep', 'tp', None)
    vm = pl.BlockSpec(memory_space=pltpu.VMEM)
    anyspace = pl.BlockSpec(memory_space=pl.ANY)

    def device_step(hidden, seq_lens, rope_cos, rope_sin, ln1_scale, ln1_bias, w_qkv, b_qkv, w_out, b_out, k_cache, v_cache, ln2_scale, ln2_bias, w_router, expert_ids, w_gate, w_up, w_down):
        n, d = hidden.shape
        _, s_max, groups, head = k_cache.shape
        feat = groups * head
        n_exp = w_gate.shape[0]
        k_in = k_cache.transpose(0, 2, 3, 1).reshape(n, feat, s_max)
        v_in = v_cache.transpose(0, 2, 3, 1).reshape(n, feat, s_max)
        ctx, k_out, v_out = pl.pallas_call(
            attention_kernel,
            out_shape=(pltpu.VMEM((n, 384), BF16), jax.ShapeDtypeStruct(k_in.shape, BF16), jax.ShapeDtypeStruct(v_in.shape, BF16)),
            in_specs=[anyspace] * 10,
            out_specs=(vm, anyspace, anyspace),
            scratch_shapes=[
                pltpu.SMEM((n,), jnp.int32), pltpu.VMEM((n, d), BF16), pltpu.VMEM((32, n), F32), pltpu.VMEM((32, n), F32),
                pltpu.VMEM((d,), BF16), pltpu.VMEM((d,), BF16), pltpu.VMEM(b_qkv.shape, BF16),
                pltpu.VMEM(k_in.shape, BF16), pltpu.VMEM(v_in.shape, BF16), pltpu.VMEM(w_qkv.shape, BF16),
                pltpu.VMEM((n * 8, 128), F32), pltpu.VMEM((n // BB, 128, 128), F32), pltpu.VMEM((n // BB, 128, 128), F32), pltpu.VMEM((n * 8, 128), F32),
                pltpu.SemaphoreType.DMA((7,)), pltpu.SemaphoreType.DMA((W_PARTS,)), pltpu.SemaphoreType.DMA((n // BB,)), pltpu.SemaphoreType.DMA((n // BB,)),
                pltpu.SemaphoreType.DMA((n // BB,)), pltpu.SemaphoreType.DMA((n // BB,)),
            ],
            compiler_params=pltpu.CompilerParams(vmem_limit_bytes=VMEM_LIMIT),
            name="attention",
        )(seq_lens, hidden, rope_cos.T, rope_sin.T, ln1_scale, ln1_bias, b_qkv, w_qkv, k_in, v_in)
        ctx = pltpu.with_memory_space_constraint(ctx, pltpu.VMEM)
        in_hbm = lambda w: pltpu.with_memory_space_constraint(w, pltpu.HBM)
        rows = lambda r, t: pltpu.VMEM((r, d), t)
        cut = lambda r, t: pltpu.VMEM((COLS, r, d // COLS), t)
        hidden_out = pl.pallas_call(
            moe_kernel,
            out_shape=pltpu.VMEM((n, d), BF16),
            in_specs=[vm] * 7 + [anyspace] * 4,
            out_specs=vm,
            scratch_shapes=[
                pltpu.VMEM(w_out.shape, BF16), rows(64, BF16), pltpu.VMEM((n_exp, d, 256), BF16), pltpu.VMEM((n_exp * 128, d), BF16), rows(128, BF16),
                pltpu.VMEM((3, 16, d), BF16), rows(16, F32), rows(256, BF16), pltpu.VMEM((4, 8, n), jnp.int32), pltpu.VMEM((256, n_exp * 128), BF16),
                cut(64, F32), cut(64, F32), cut(64, BF16), cut(64, BF16), cut(64, BF16), cut(64, BF16), cut(64, BF16), cut(64, BF16),
                cut(64, F32), cut(64, BF16), pltpu.VMEM((COLS, 3, 16, d // COLS), BF16), cut(64, BF16),
                pltpu.SemaphoreType.DMA((2 * n_exp + 2,)), pltpu.SemaphoreType.DMA((N_SLOTS,)), pltpu.SemaphoreType.DMA((N_SLOTS,)),
            ],
            compiler_params=pltpu.CompilerParams(vmem_limit_bytes=MOE_LIMIT, collective_id=0, has_side_effects=True),
            name="moe",
        )(hidden, ctx, b_out, ln2_scale, ln2_bias, w_router.T, expert_ids.T, in_hbm(w_out), in_hbm(w_gate), in_hbm(w_up), in_hbm(w_down.reshape(n_exp * 128, d)))
        unfold = lambda c: c.reshape(n, groups, head, s_max).transpose(0, 3, 1, 2)
        return hidden_out, unfold(k_out), unfold(v_out)

    in_specs = (token_rows, token_vec, token_rows, token_rows, P(), P(), P(None, 'tp'), P('tp'), P('tp', None), P(), cache_spec, cache_spec, P(), P(), P(), token_rows, expert_in, expert_in, expert_down)
    return jax.shard_map(device_step, mesh=mesh, in_specs=in_specs, out_specs=(token_rows, cache_spec, cache_spec), check_vma=False)
```

```python
import functools

import jax
import jax.numpy as jnp
from jax import lax
from jax.experimental import pallas as pl
from jax.experimental.pallas import tpu as pltpu
from jax.sharding import PartitionSpec as P

EPS = 1e-5
F32 = jnp.float32
BF16 = jnp.bfloat16
MESH = pl.DeviceIdType.MESH
VMEM_LIMIT = 66_400_000
MOE_LIMIT = 40_000_000
NT = (((1,), (1,)), ((), ()))
BB = 8
COLS = 3
PIECE = 16
AHEAD = 5
W_PARTS = 4


def normalize(vals_f32, ln_scale, ln_bias):
    row_mean = jnp.mean(vals_f32, axis=-1, keepdims=True)
    centered = vals_f32 - row_mean
    row_var = jnp.mean(centered * centered, axis=-1, keepdims=True)
    normed = centered * lax.rsqrt(row_var + EPS)
    return (normed * ln_scale + ln_bias).astype(BF16)


def row_of(vec_ref):
    return vec_ref[...].astype(F32)[None, :]


def attention_kernel(lens_hbm, hid_hbm, cos_hbm, sin_hbm, scale_hbm, bias_hbm, bqkv_hbm, wqkv_hbm, wout_hbm, k_hbm, v_hbm,
                     part_ref, ko_hbm, vo_hbm, lens_ref, hid_ref, cos_ref, sin_ref, scale_ref, bias_ref, bqkv_ref,
                     k_buf, v_buf, w_buf, wo_buf, q_buf, kn_buf, vn_buf, c_buf, in_sem, w_sem, wo_sem, k_sem, v_sem, ko_sem, vo_sem):
    n_rows = hid_ref.shape[0]
    n_blocks = n_rows // BB
    s_max = k_buf.shape[2]
    smalls = ((hid_hbm, hid_ref), (scale_hbm, scale_ref), (bias_hbm, bias_ref), (bqkv_hbm, bqkv_ref), (cos_hbm, cos_ref), (sin_hbm, sin_ref),
              (lens_hbm, lens_ref))
    small_copies = [pltpu.make_async_copy(src, dst, in_sem.at[i]) for i, (src, dst) in enumerate(smalls)]
    w_rows = w_buf.shape[0] // W_PARTS
    w_copies = [pltpu.make_async_copy(wqkv_hbm.at[pl.ds(i * w_rows, w_rows)], w_buf.at[pl.ds(i * w_rows, w_rows)], w_sem.at[i]) for i in range(W_PARTS)]
    wo_copy = pltpu.make_async_copy(wout_hbm, wo_buf, wo_sem)
    for copy in small_copies[:3] + w_copies + small_copies[3:]:
        copy.start()

    def fetch(i):
        rows = pl.ds(i * BB, BB)
        return (pltpu.make_async_copy(k_hbm.at[rows], k_buf.at[rows], k_sem.at[i]),
                pltpu.make_async_copy(v_hbm.at[rows], v_buf.at[rows], v_sem.at[i]))

    def flush(i):
        rows = pl.ds(i * BB, BB)
        return (pltpu.make_async_copy(k_buf.at[rows], ko_hbm.at[rows], ko_sem.at[i]),
                pltpu.make_async_copy(v_buf.at[rows], vo_hbm.at[rows], vo_sem.at[i]))

    def fetch_start(i):
        for copy in fetch(i):
            copy.start()

    for i in range(AHEAD):
        fetch_start(i)

    for copy in small_copies:
        copy.wait()
    normed = normalize(hid_ref[...].astype(F32), row_of(scale_ref), row_of(bias_ref))
    for copy in w_copies:
        copy.wait()
    fetch_start(AHEAD)
    qkv = jnp.dot(normed, w_buf[...], preferred_element_type=F32) + row_of(bqkv_ref)
    qkv = qkv.astype(BF16).astype(F32)
    qkv = jnp.concatenate([qkv, jnp.zeros((128 - n_rows, qkv.shape[1]), F32)], axis=0)
    feats = qkv.T
    cos_t = jnp.concatenate([cos_ref[...], jnp.zeros((32, 128 - n_rows), F32)], axis=1)
    sin_t = jnp.concatenate([sin_ref[...], jnp.zeros((32, 128 - n_rows), F32)], axis=1)

    def rotate(base):
        u, w = feats[base:base + 32], feats[base + 32:base + 64]
        return jnp.concatenate([u * cos_t - w * sin_t, w * cos_t + u * sin_t], axis=0).astype(BF16).astype(F32)

    zeros = jnp.zeros((64, 128), F32)
    for g in range(2):
        for j in range(3):
            q_rot = rotate(g * 320 + j * 64)
            both = jnp.concatenate([q_rot, zeros] if g == 0 else [zeros, q_rot], axis=0)
            q_buf[pl.ds(g * 3 + j, n_rows, stride=8), :] = both.T[:n_rows]
    for r in (6, 7):
        q_buf[pl.ds(r, n_rows, stride=8), :] = jnp.zeros((n_rows, 128), F32)
    k_new = jnp.concatenate([rotate(192), rotate(320 + 192)], axis=0)
    v_new = jnp.concatenate([feats[256:320], feats[320 + 256:320 + 320]], axis=0)
    for i in range(n_blocks):
        kn_buf[i] = k_new if i == 0 else pltpu.roll(k_new, 128 - i * BB, 1)
        vn_buf[i] = v_new if i == 0 else pltpu.roll(v_new, 128 - i * BB, 1)

    def block(i, carry):
        for copy in fetch(i):
            copy.wait()

        @pl.when(i + AHEAD + 1 < n_blocks)
        def _():
            fetch_start(i + AHEAD + 1)

        @pl.when(i == n_blocks - AHEAD - 1)
        def _():
            wo_copy.start()

        k_cols, v_cols = kn_buf[i], vn_buf[i]
        lane = lax.broadcasted_iota(jnp.int32, (128, 128), 1)
        position = lax.broadcasted_iota(jnp.int32, (8, s_max), 1)
        scores = []
        for j in range(BB):
            b = i * BB + j
            pos = lens_ref[b]
            first = pl.multiple_of((pos // 128) * 128, 128)
            hit = lane == pos - first
            window = pl.ds(first, 128)
            k_buf[b, :, window] = jnp.where(hit, k_cols[:, j:j + 1], k_buf[b, :, window].astype(F32)).astype(BF16)
            v_buf[b, :, window] = jnp.where(hit, v_cols[:, j:j + 1], v_buf[b, :, window].astype(F32)).astype(BF16)
            rows = pl.ds(pl.multiple_of(b * 8, 8), 8)
            one = jnp.dot(q_buf[rows, :].astype(BF16), k_buf[b], preferred_element_type=F32) * 0.125
            scores.append(jnp.where(position <= pos, one, -jnp.inf))
        scores = jnp.concatenate(scores, axis=0)
        top = jnp.max(scores, axis=1, keepdims=True)
        weights = jnp.exp(scores - top)
        probs = weights * (1.0 / jnp.sum(weights, axis=1, keepdims=True))
        for j in range(BB):
            b = i * BB + j
            rows = pl.ds(pl.multiple_of(b * 8, 8), 8)
            c_buf[rows, :] = lax.dot_general(probs[j * 8:j * 8 + 8].astype(BF16), v_buf[b], NT, preferred_element_type=F32)
        for copy in flush(i):
            copy.start()
        return carry

    lax.fori_loop(0, n_blocks, block, 0)
    heads = [c_buf[pl.ds(r, n_rows, stride=8), :] for r in range(6)]
    low = lax.broadcasted_iota(jnp.int32, (n_rows, 128), 1) < 64
    ctx = jnp.concatenate([
        jnp.where(low, heads[0], pltpu.roll(heads[1], 64, 1)),
        jnp.where(low, heads[2], heads[3]),
        jnp.where(low, pltpu.roll(heads[4], 64, 1), heads[5]),
    ], axis=1).astype(BF16)
    wo_copy.wait()
    part_ref[...] = jnp.dot(ctx, wo_buf[...], preferred_element_type=F32).astype(BF16)
    for i in range(n_blocks):
        for copy in flush(i):
            copy.wait()


def moe_kernel(hid_ref, part_ref, bout_ref, scale_ref, bias_ref, wr_ref, ids_ref, wg_hbm, wu_hbm, wd_hbm, out_ref,
               wgu, wd, wr, rs_recv, x1, h2, ids_buf, act, own_p, y_p, hi0, hi1, d0, d1, y_send, y_recv,
               t_f, t_b, z_recv, o_buf, wsem, ssem, rsem):
    z, ep = lax.axis_index("tp"), lax.axis_index("ep")
    n_rows, d_model = hid_ref.shape
    n_exp = wgu.shape[0]
    width = d_model // COLS
    z_peers = [lax.rem(z + dz, 4) for dz in (1, 2, 3)]
    y_peer = lax.rem(ep + 2, 4)
    partner = ep + 1 - 2 * lax.rem(ep, 2)
    diagonal = 3 - ep
    barrier = pltpu.get_barrier_semaphore()
    for peer in z_peers:
        pl.semaphore_signal(barrier, inc=1, device_id={"tp": peer}, device_id_type=MESH)
    for peer in (y_peer, partner, diagonal):
        pl.semaphore_signal(barrier, inc=1, device_id={"ep": peer}, device_id_type=MESH)

    loads = []
    for e in range(n_exp):
        loads.append(pltpu.make_async_copy(wg_hbm.at[e], wgu.at[e, :, 0:128], wsem.at[2 * e]))
        loads.append(pltpu.make_async_copy(wu_hbm.at[e], wgu.at[e, :, 128:256], wsem.at[2 * e + 1]))
    loads.append(pltpu.make_async_copy(wd_hbm, wd, wsem.at[2 * n_exp]))
    for load in loads:
        load.start()

    count = [0]

    def remote(src, dst, device):
        slot = count[0]
        count[0] += 1
        return pltpu.make_async_remote_copy(src_ref=src, dst_ref=dst, send_sem=ssem.at[slot], recv_sem=rsem.at[slot],
                                            device_id=device, device_id_type=MESH)

    def at(index, h, shard=0):
        return pl.ds(pl.multiple_of(shard * n_rows + index * 16 + h * PIECE, PIECE), PIECE)

    def rows_at(index):
        return pl.ds(pl.multiple_of(index * 16, 16), 16)

    def cols(n):
        return pl.ds(n * width, width)

    halves = range(16 // PIECE)
    z_order = [z] + [lax.rem(z + 4 - dz, 4) for dz in (1, 2, 3)]
    rs = [[remote(part_ref.at[at(z_peers[dz], h)], rs_recv.at[dz, pl.ds(h * PIECE, PIECE)], {"tp": z_peers[dz]}) for dz in range(3)] for h in halves]
    to_z = [[remote(h2.at[at(z, h)], h2.at[at(z, h)], {"tp": z_peers[dz]}) for dz in range(3)] for h in halves]
    to_p = [[remote(h2.at[at(z_order[k], h)], h2.at[at(z_order[k], h, 1)], {"ep": partner}) for k in range(4)] for h in halves]
    to_y = [[remote(h2.at[at(z_order[k], h)], h2.at[at(z_order[k], h, 2)], {"ep": y_peer}) for k in range(4)] for h in halves]
    y_to_p = [[remote(h2.at[at(z_order[k], h, 2)], h2.at[at(z_order[k], h, 3)], {"ep": partner}) for k in range(4)] for h in halves]
    mine = rows_at(z)
    to_ids = [remote(ids_ref, ids_buf.at[i + 1], {"ep": peer}) for i, peer in enumerate((partner, y_peer, diagonal))]
    chunks = range(COLS)
    to_d0 = [remote(hi0.at[n], d0.at[n], {"ep": partner}) for n in chunks]
    to_d = [remote(hi1.at[n], d1.at[n], {"ep": partner}) for n in chunks]
    to_yy = [remote(y_send.at[n], y_recv.at[n], {"ep": y_peer}) for n in chunks]
    to_zz = [[remote(t_b.at[n, rows_at(z_peers[dz])], z_recv.at[n, dz], {"tp": z_peers[dz]}) for dz in range(3)] for n in chunks]
    to_o = [[remote(o_buf.at[n, mine], o_buf.at[n, mine], {"tp": z_peers[dz]}) for dz in range(3)] for n in chunks]

    scale, bias, bout = row_of(scale_ref), row_of(bias_ref), row_of(bout_ref)
    ids_buf[0] = ids_ref[...]
    wr[...] = jnp.concatenate([wr_ref[...], jnp.zeros((128 - wr_ref.shape[0], d_model), BF16)], axis=0)
    pl.semaphore_wait(barrier, 6)

    for h in halves:
        for dz in range(3):
            rs[h][dz].start()
    for copy in to_ids:
        copy.start()
    for h in halves:
        for dz in range(3):
            rs[h][dz].wait_recv()
        got = pl.ds(h * PIECE, PIECE)
        total = part_ref[at(z, h), :].astype(F32) + rs_recv[0, got].astype(F32) + rs_recv[1, got].astype(F32) + rs_recv[2, got].astype(F32)
        row = (hid_ref[at(z, h), :].astype(F32) + total + bout).astype(BF16)
        x1[got, :] = row.astype(F32)
        h2[at(z, h), :] = normalize(row.astype(F32), scale, bias)
        for dz in range(3):
            to_z[h][dz].start()
        to_y[h][0].start()
        to_p[h][0].start()

    def relay(h, k):
        to_y[h][k].wait_recv()
        y_to_p[h][k].start()

    for h in halves:
        for dz in range(3):
            to_z[h][dz].wait_recv()
            to_y[h][dz + 1].start()
            to_p[h][dz + 1].start()
        relay(h, 0)

    def masks(shard):
        picks = ids_buf[shard]
        expert = lax.broadcasted_iota(jnp.int32, (128, n_rows), 0)
        hit = jnp.zeros((128, n_rows), F32)
        for k in range(picks.shape[0]):
            hit = jnp.where(expert == picks[k:k + 1, :], 1.0, hit)
        return hit.T

    def toks(shard):
        return h2[shard * n_rows:(shard + 1) * n_rows, :]

    def gates_of(shard):
        logits = lax.dot_general(toks(shard), wr[...], NT, preferred_element_type=F32)
        logits = jnp.where(masks(shard) > 0.5, logits, -jnp.inf)
        shifted = jnp.exp(logits - jnp.max(logits, axis=1, keepdims=True))
        gates = (shifted / jnp.sum(shifted, axis=1, keepdims=True)).astype(BF16).astype(F32)
        return pltpu.roll(gates, lax.rem(128 - ep * n_exp, 128), 1)

    def up(shard, gates, first, last):
        rows = toks(shard)
        for e in range(first, last):
            if shard == 0:
                loads[2 * e].wait()
                loads[2 * e + 1].wait()
            pre = jnp.dot(rows, wgu[e], preferred_element_type=F32)
            gate_pre, up_pre = pre[:, :128], pre[:, 128:]
            hidden = (gate_pre * jax.nn.sigmoid(gate_pre) * up_pre).astype(BF16).astype(F32)
            act[shard * n_rows:(shard + 1) * n_rows, e * 128:(e + 1) * 128] = (hidden * gates[:, e:e + 1]).astype(BF16)

    for copy in to_ids:
        copy.wait_recv()
    up(0, gates_of(0), 0, n_exp)
    for h in halves:
        for copy in to_p[h]:
            copy.wait_recv()
    up(1, gates_of(1), 0, n_exp)
    for h in halves:
        for k in (1, 2, 3):
            relay(h, k)
    up(2, gates_of(2), 0, n_exp)
    for h in halves:
        for copy in y_to_p[h]:
            copy.wait_recv()
    up(3, gates_of(3), 0, n_exp)
    loads[-1].wait()

    def reduce_pair(n):
        to_d[n].wait_recv()
        y_send[n] = (y_p[n] + d1[n].astype(F32)).astype(BF16)
        to_yy[n].start()

    for n in chunks:
        both = jnp.dot(act[128:256, :], wd[:, cols(n)], preferred_element_type=F32)
        y_p[n] = both[0:64]
        hi1[n] = both[64:128].astype(BF16)
        to_d[n].start()
        if n > 0:
            reduce_pair(n - 1)
        both = jnp.dot(act[0:128, :], wd[:, cols(n)], preferred_element_type=F32)
        own_p[n] = both[0:64]
        hi0[n] = both[64:128].astype(BF16)
        to_d0[n].start()
    reduce_pair(COLS - 1)
    for n in chunks:
        to_d0[n].wait_recv()
        to_yy[n].wait_recv()
        t = own_p[n] + d0[n].astype(F32) + y_recv[n].astype(F32)
        t_f[n] = t
        t_b[n] = t.astype(BF16)
        for copy in to_zz[n]:
            copy.start()
    for n in chunks:
        for copy in to_zz[n]:
            copy.wait_recv()
        moe = t_f[n, mine, :] + z_recv[n, 0].astype(F32) + z_recv[n, 1].astype(F32) + z_recv[n, 2].astype(F32)
        o_buf[n, mine, :] = (x1[:, cols(n)] + moe).astype(BF16)
        for copy in to_o[n]:
            copy.start()
    for n in chunks:
        for copy in to_o[n]:
            copy.wait_recv()
        out_ref[:, cols(n)] = o_buf[n]
    for group in rs + to_z + to_p + to_y + y_to_p + [to_ids, to_d0, to_d, to_yy] + to_zz + to_o:
        for copy in group:
            copy.wait_send()


N_SLOTS = (16 // PIECE) * 18 + 3 + 9 * COLS


def solution(mesh):
    token_rows = P(('dp', 'ep'), None)
    token_vec = P(('dp', 'ep'))
    cache_spec = P(('dp', 'ep'), None, 'tp', None)
    expert_in = P('ep', None, 'tp')
    expert_down = P('ep', 'tp', None)
    vm = pl.BlockSpec(memory_space=pltpu.VMEM)
    anyspace = pl.BlockSpec(memory_space=pl.ANY)

    def device_step(hidden, seq_lens, rope_cos, rope_sin, ln1_scale, ln1_bias, w_qkv, b_qkv, w_out, b_out, k_cache, v_cache, ln2_scale, ln2_bias, w_router, expert_ids, w_gate, w_up, w_down):
        n, d = hidden.shape
        _, s_max, groups, head = k_cache.shape
        feat = groups * head
        n_exp = w_gate.shape[0]
        k_in = k_cache.transpose(0, 2, 3, 1).reshape(n, feat, s_max)
        v_in = v_cache.transpose(0, 2, 3, 1).reshape(n, feat, s_max)
        part, k_out, v_out = pl.pallas_call(
            attention_kernel,
            out_shape=(pltpu.VMEM((n, d), BF16), jax.ShapeDtypeStruct(k_in.shape, BF16), jax.ShapeDtypeStruct(v_in.shape, BF16)),
            in_specs=[anyspace] * 11,
            out_specs=(vm, anyspace, anyspace),
            scratch_shapes=[
                pltpu.SMEM((n,), jnp.int32), pltpu.VMEM((n, d), BF16), pltpu.VMEM((32, n), F32), pltpu.VMEM((32, n), F32),
                pltpu.VMEM((d,), BF16), pltpu.VMEM((d,), BF16), pltpu.VMEM(b_qkv.shape, BF16),
                pltpu.VMEM(k_in.shape, BF16), pltpu.VMEM(v_in.shape, BF16), pltpu.VMEM(w_qkv.shape, BF16), pltpu.VMEM(w_out.shape, BF16),
                pltpu.VMEM((n * 8, 128), F32), pltpu.VMEM((n // BB, 128, 128), F32), pltpu.VMEM((n // BB, 128, 128), F32), pltpu.VMEM((n * 8, 128), F32),
                pltpu.SemaphoreType.DMA((7,)), pltpu.SemaphoreType.DMA((W_PARTS,)), pltpu.SemaphoreType.DMA, pltpu.SemaphoreType.DMA((n // BB,)), pltpu.SemaphoreType.DMA((n // BB,)),
                pltpu.SemaphoreType.DMA((n // BB,)), pltpu.SemaphoreType.DMA((n // BB,)),
            ],
            compiler_params=pltpu.CompilerParams(vmem_limit_bytes=VMEM_LIMIT),
            name="attention",
        )(seq_lens, hidden, rope_cos.T, rope_sin.T, ln1_scale, ln1_bias, b_qkv, w_qkv, w_out, k_in, v_in)
        part = pltpu.with_memory_space_constraint(part, pltpu.VMEM)
        in_hbm = lambda w: pltpu.with_memory_space_constraint(w, pltpu.HBM)
        rows = lambda r, t: pltpu.VMEM((r, d), t)
        cut = lambda r, t: pltpu.VMEM((COLS, r, d // COLS), t)
        hidden_out = pl.pallas_call(
            moe_kernel,
            out_shape=pltpu.VMEM((n, d), BF16),
            in_specs=[vm] * 7 + [anyspace] * 3,
            out_specs=vm,
            scratch_shapes=[
                pltpu.VMEM((n_exp, d, 256), BF16), pltpu.VMEM((n_exp * 128, d), BF16), rows(128, BF16),
                pltpu.VMEM((3, 16, d), BF16), rows(16, F32), rows(256, BF16), pltpu.VMEM((4, 8, n), jnp.int32), pltpu.VMEM((256, n_exp * 128), BF16),
                cut(64, F32), cut(64, F32), cut(64, BF16), cut(64, BF16), cut(64, BF16), cut(64, BF16), cut(64, BF16), cut(64, BF16),
                cut(64, F32), cut(64, BF16), pltpu.VMEM((COLS, 3, 16, d // COLS), BF16), cut(64, BF16),
                pltpu.SemaphoreType.DMA((2 * n_exp + 1,)), pltpu.SemaphoreType.DMA((N_SLOTS,)), pltpu.SemaphoreType.DMA((N_SLOTS,)),
            ],
            compiler_params=pltpu.CompilerParams(vmem_limit_bytes=MOE_LIMIT, collective_id=0, has_side_effects=True),
            name="moe",
        )(hidden, part, b_out, ln2_scale, ln2_bias, w_router.T, expert_ids.T, in_hbm(w_gate), in_hbm(w_up), in_hbm(w_down.reshape(n_exp * 128, d)))
        unfold = lambda c: c.reshape(n, groups, head, s_max).transpose(0, 3, 1, 2)
        return hidden_out, unfold(k_out), unfold(v_out)

    in_specs = (token_rows, token_vec, token_rows, token_rows, P(), P(), P(None, 'tp'), P('tp'), P('tp', None), P(), cache_spec, cache_spec, P(), P(), P(), token_rows, expert_in, expert_in, expert_down)
    return jax.shard_map(device_step, mesh=mesh, in_specs=in_specs, out_specs=(token_rows, cache_spec, cache_spec), check_vma=False)
```
